32 devices in a mesh: dpy: 4 (over z), dpx: 2 (over y), tp: 4 (over x, core).
Axes of the slice: x: 2, y: 2, z: 4, core: 2. Of those that a mesh axis runs over, the one named last changes fastest.
Arguments:
- x_saved: bfloat16 [2, 16, 1024, 1536], P(None, ('dpy', 'dpx'))
- y_saved: bfloat16 [2, 16, 1024, 1536], P(None, ('dpy', 'dpx'))
- d_out: bfloat16 [16, 1024, 1536], P(('dpy', 'dpx'))
- w_qkv: bfloat16 [2, 1536, 3, 12, 128], P(None, None, None, 'tp')
- w_out: bfloat16 [2, 12, 128, 1536], P(None, 'tp')
- w_up: bfloat16 [2, 1536, 6144], P(None, None, 'tp')
- w_down: bfloat16 [2, 6144, 1536], P(None, 'tp')
Outputs:
- output 1: bfloat16 [16, 1024, 1536], P(('dpy', 'dpx'))
- output 2: float32 [2, 1536, 3, 12, 128], P(None, None, None, 'tp')
- output 3: float32 [2, 12, 128, 1536], P(None, 'tp')
- output 4: float32 [2, 1536, 6144], P(None, None, 'tp')
- output 5: float32 [2, 6144, 1536], P(None, 'tp')
All inputs are finite; a program needn't handle non-finite values.
Results may differ from the reference program's by a relative error of at most 0.02.
Values are sent between devices in bfloat16 or wider.
A program may use at most 1 GiB of HBM per device.

```python
import jax
import jax.numpy as jnp
from jax import lax

WIDTH = 1536
FFN = 6144
HEADS = 12
BATCH = 2
SEQ = 1024
REPLICAS = 8
LAYERS = 2
HEAD_DIM = WIDTH // HEADS
SEQ_TOTAL = REPLICAS * BATCH


def setup_inputs(seed: int = 0) -> dict:
    root_key = jax.random.key(seed)
    sub_keys = jax.random.split(root_key, 7)
    act_shape = (LAYERS, SEQ_TOTAL, SEQ, WIDTH)
    x_saved = jax.random.normal(sub_keys[0], act_shape, jnp.float32).astype(jnp.bfloat16)
    y_saved = jax.random.normal(sub_keys[1], act_shape, jnp.float32).astype(jnp.bfloat16)
    d_out = jax.random.normal(sub_keys[2], (SEQ_TOTAL, SEQ, WIDTH), jnp.float32).astype(jnp.bfloat16)
    w_qkv = (jax.random.normal(sub_keys[3], (LAYERS, WIDTH, 3, HEADS, HEAD_DIM), jnp.float32) * WIDTH ** -0.5).astype(jnp.bfloat16)
    w_out = (jax.random.normal(sub_keys[4], (LAYERS, HEADS, HEAD_DIM, WIDTH), jnp.float32) * (4.0 * WIDTH ** -0.5)).astype(jnp.bfloat16)
    w_up = (jax.random.normal(sub_keys[5], (LAYERS, WIDTH, FFN), jnp.float32) * WIDTH ** -0.5).astype(jnp.bfloat16)
    w_down = (jax.random.normal(sub_keys[6], (LAYERS, FFN, WIDTH), jnp.float32) * (2.0 * FFN ** -0.5)).astype(jnp.bfloat16)
    return {'x_saved': x_saved, 'y_saved': y_saved, 'd_out': d_out, 'w_qkv': w_qkv, 'w_out': w_out, 'w_up': w_up, 'w_down': w_down}


def attention_backward(qkv_seq, d_att):
    queries = qkv_seq[:, 0].astype(jnp.float32)
    keys_all = qkv_seq[:, 1].astype(jnp.float32)
    values = qkv_seq[:, 2].astype(jnp.float32)
    datt_f32 = d_att.astype(jnp.float32)
    scale_factor = HEAD_DIM ** -0.5
    scores = jnp.einsum('qnd,knd->nqk', queries, keys_all) * scale_factor
    probs_f = jax.nn.softmax(scores, axis=-1)
    probs_b = probs_f.astype(jnp.bfloat16).astype(jnp.float32)
    att_out = jnp.einsum('nqk,knd->qnd', probs_b, values).astype(jnp.bfloat16)
    d_probs = jnp.einsum('qnd,knd->nqk', datt_f32, values)
    d_values = jnp.einsum('nqk,qnd->knd', probs_b, datt_f32).astype(jnp.bfloat16)
    row_dot = jnp.sum(d_probs * probs_f, axis=-1, keepdims=True)
    d_scores = (probs_f * (d_probs - row_dot) * scale_factor).astype(jnp.bfloat16).astype(jnp.float32)
    d_queries = jnp.einsum('nqk,knd->qnd', d_scores, keys_all).astype(jnp.bfloat16)
    d_keys = jnp.einsum('nqk,qnd->knd', d_scores, queries).astype(jnp.bfloat16)
    return att_out, jnp.stack([d_queries, d_keys, d_values], axis=1)


def layer_backward(x_in, y_mid, grad_out, wqkv_l, wout_l, wup_l, wdown_l):
    mid_f32 = y_mid.astype(jnp.float32)
    gout_f32 = grad_out.astype(jnp.float32)
    wup_f32 = wup_l.astype(jnp.float32)
    hidden = jnp.einsum('bsh,hf->bsf', mid_f32, wup_f32)
    act_f32, gelu_pull = jax.vjp(jax.nn.gelu, hidden)
    act_b = act_f32.astype(jnp.bfloat16).astype(jnp.float32)
    g_down = jnp.einsum('bsf,bsh->fh', act_b, gout_f32)
    d_act = jnp.einsum('bsh,fh->bsf', gout_f32, wdown_l.astype(jnp.float32))
    d_hidden = gelu_pull(d_act)[0].astype(jnp.bfloat16).astype(jnp.float32)
    g_up = jnp.einsum('bsh,bsf->hf', mid_f32, d_hidden)
    d_mid = (gout_f32 + jnp.einsum('bsf,hf->bsh', d_hidden, wup_f32)).astype(jnp.bfloat16)
    in_f32 = x_in.astype(jnp.float32)
    wqkv_f32 = wqkv_l.astype(jnp.float32)
    qkv = jnp.einsum('bsh,hcnd->bscnd', in_f32, wqkv_f32).astype(jnp.bfloat16)
    dmid_f32 = d_mid.astype(jnp.float32)
    d_att = jnp.einsum('bsh,ndh->bsnd', dmid_f32, wout_l.astype(jnp.float32)).astype(jnp.bfloat16)
    att_out, d_qkv = lax.map(lambda seq_pair: attention_backward(seq_pair[0], seq_pair[1]), (qkv, d_att))
    g_out = jnp.einsum('bsnd,bsh->ndh', att_out.astype(jnp.float32), dmid_f32)
    dqkv_f32 = d_qkv.astype(jnp.float32)
    g_qkv = jnp.einsum('bsh,bscnd->hcnd', in_f32, dqkv_f32)
    d_in = (dmid_f32 + jnp.einsum('bscnd,hcnd->bsh', dqkv_f32, wqkv_f32)).astype(jnp.bfloat16)
    return d_in, (g_qkv, g_out, g_up, g_down)


def reference(x_saved, y_saved, d_out, w_qkv, w_out, w_up, w_down):
    def replica_step(grad_sums, rep_idx):
        row_start = rep_idx * BATCH
        grad_cur = lax.dynamic_slice_in_dim(d_out, row_start, BATCH, axis=0)
        layer_grads = [None] * LAYERS
        for layer_idx in reversed(range(LAYERS)):
            x_in = lax.dynamic_slice_in_dim(x_saved[layer_idx], row_start, BATCH, axis=0)
            y_mid = lax.dynamic_slice_in_dim(y_saved[layer_idx], row_start, BATCH, axis=0)
            grad_cur, layer_grads[layer_idx] = layer_backward(x_in, y_mid, grad_cur, w_qkv[layer_idx], w_out[layer_idx], w_up[layer_idx], w_down[layer_idx])
        new_sums = tuple(sum_prev + jnp.stack([grad_set[slot_idx] for grad_set in layer_grads]) for slot_idx, sum_prev in enumerate(grad_sums))
        return new_sums, grad_cur

    init_sums = tuple(jnp.zeros(weight.shape, jnp.float32) for weight in (w_qkv, w_out, w_up, w_down))
    grad_sums, d_inputs = lax.scan(replica_step, init_sums, jnp.arange(REPLICAS))
    d_input = d_inputs.reshape(SEQ_TOTAL, SEQ, WIDTH)
    g_qkv, g_out, g_up, g_down = (sum_all / REPLICAS for sum_all in grad_sums)
    return d_input, g_qkv, g_out, g_up, g_down
```

```python
import functools

import jax
import jax.numpy as jnp
from jax import lax
from jax.experimental import pallas as pl
from jax.experimental.pallas import tpu as pltpu
from jax.sharding import PartitionSpec as P

F32, BF16 = jnp.float32, jnp.bfloat16
PLAIN = (((1,), (0,)), ((), ()))
LANES = (((1,), (1,)), ((), ()))
ROWS = (((0,), (0,)), ((), ()))
ANY = pl.BlockSpec(memory_space=pl.ANY)
TANH_1 = 0.7978845608028654
TANH_3 = 0.044715 * TANH_1


def dot(a, b, dims=PLAIN):
    return lax.dot_general(a, b, dims, preferred_element_type=F32)


def attention_kernel(scale, heads, q_ref, k_ref, v_ref, mid_ref, wo_ref, wq_ref, *refs):
    o_ref, dqkv_ref, part_ref, p_ref, ds_ref, do_ref = refs[-6:]
    n = pl.program_id(0)
    rows, d = q_ref.shape
    blk, cols = 256, 512
    do_ref[...] = dot(mid_ref[...], wo_ref[...], LANES).astype(BF16)
    keys, vals = k_ref[...], v_ref[...]
    keys_t, vals_t = keys.T, vals.T
    place = lambda c: pl.ds(pl.multiple_of((c * heads + n) * d, d), d)
    for i in range(rows // blk):
        sl = slice(i * blk, (i + 1) * blk)
        q, do = q_ref[sl, :], do_ref[sl, :]
        s = dot(keys, q, LANES)
        top = jnp.max(s, axis=0, keepdims=True)
        e = jnp.exp((s - top) * scale)
        p = e * (1.0 / jnp.sum(e, axis=0, keepdims=True))
        pb = p.astype(BF16)
        p_ref[:, sl] = pb
        o_ref[sl, :] = dot(vals_t, pb).T.astype(BF16)
        dp = dot(vals, do, LANES)
        row_dot = jnp.sum(dp * p, axis=0, keepdims=True)
        ds = (p * (dp - row_dot) * scale).astype(BF16)
        ds_ref[:, sl] = ds
        dqkv_ref[sl, place(0)] = dot(keys_t, ds).T.astype(BF16)
    dqkv_ref[:, place(1)] = dot(ds_ref[...], q_ref[...]).astype(BF16)
    dqkv_ref[:, place(2)] = dot(p_ref[...], do_ref[...]).astype(BF16)

    @pl.when(n == heads - 1)
    def _():
        for c in range(part_ref.shape[1] // cols):
            sl = slice(c * cols, (c + 1) * cols)
            part_ref[:, sl] = dot(dqkv_ref[...], wq_ref[sl, :], LANES).astype(BF16)


def attention(qkv, mid, w_out, wq, held, l, m, mbs):
    s, width = mid.shape[0] // mbs, mid.shape[1]
    heads, d = w_out.shape[1:3]
    hd = heads * d
    col = lambda c: pl.BlockSpec((s, d), lambda n: (m, c * heads + n))
    held = tuple(held)
    return pl.pallas_call(
        functools.partial(attention_kernel, d ** -0.5, heads),
        grid=(heads,),
        in_specs=[
            col(0),
            col(1),
            col(2),
            pl.BlockSpec((s, width), lambda n: (m, 0)),
            pl.BlockSpec((None, None, d, width), lambda n: (l, n, 0, 0)),
            pl.BlockSpec((width, 3 * hd), lambda n: (0, 0)),
        ]
        + [ANY] * len(held),
        out_specs=[col(0), pl.BlockSpec((s, 3 * hd), lambda n: (m, 0)), pl.BlockSpec((s, width), lambda n: (0, 0))],
        out_shape=[
            jax.ShapeDtypeStruct((mbs * s, hd), BF16),
            jax.ShapeDtypeStruct((mbs * s, 3 * hd), BF16),
            jax.ShapeDtypeStruct((s, width), BF16),
        ],
        scratch_shapes=[pltpu.VMEM((s, s), BF16), pltpu.VMEM((s, s), BF16), pltpu.VMEM((s, d), BF16)],
        input_output_aliases={6 + i: i for i in range(len(held))},
        compiler_params=pltpu.CompilerParams(dimension_semantics=("arbitrary",)),
        cost_estimate=pl.CostEstimate(
            flops=24 * hd * s * s + 8 * s * hd * width, bytes_accessed=20 * s * hd + 4 * s * width + 8 * hd * width, transcendentals=heads * s * s
        ),
        name="attention_backward",
    )(qkv, qkv, qkv, mid, w_out, wq, *held)


def mlp_kernel(y_ref, g_ref, wu_ref, wd_ref, *refs):
    a_ref, dh_ref, p_ref = refs[-3:]
    cols = 512
    y, g = y_ref[...], g_ref[...]
    for c in range(wu_ref.shape[1] // cols):
        sl = slice(c * cols, (c + 1) * cols)
        h = dot(y, wu_ref[:, sl])
        da = dot(g, wd_ref[sl, :], LANES)
        h2 = h * h
        t = jnp.tanh(h * (TANH_1 + TANH_3 * h2))
        cdf = 0.5 * t + 0.5
        slope = cdf + (0.5 * h) * (1.0 - t * t) * (TANH_1 + (3.0 * TANH_3) * h2)
        a_ref[:, sl] = (h * cdf).astype(BF16)
        dh_ref[:, sl] = (da * slope).astype(BF16)
    dh = dh_ref[...]
    for c in range(p_ref.shape[1] // cols):
        sl = slice(c * cols, (c + 1) * cols)
        p_ref[:, sl] = dot(dh, wu_ref[sl, :], LANES).astype(BF16)


def mlp(y, g, w_up, w_down, held, l, m):
    mbs, s, h = g.shape
    f = w_up.shape[2]
    blk = 256
    steps = s // blk
    put = pl.BlockSpec((blk, f), lambda i: (m * steps + i, 0))
    big = jax.ShapeDtypeStruct((mbs * s, f), BF16)
    held = tuple(held)
    return pl.pallas_call(
        mlp_kernel,
        grid=(steps,),
        in_specs=[
            pl.BlockSpec((None, None, blk, h), lambda i: (l, m, i, 0)),
            pl.BlockSpec((None, blk, h), lambda i: (m, i, 0)),
            pl.BlockSpec((None, h, f), lambda i: (l, 0, 0)),
            pl.BlockSpec((None, f, h), lambda i: (l, 0, 0)),
        ]
        + [ANY] * len(held),
        out_specs=[put, put, pl.BlockSpec((blk, h), lambda i: (i, 0))],
        out_shape=[big, big, jax.ShapeDtypeStruct((s, h), BF16)],
        input_output_aliases={4 + i: i for i in range(len(held))},
        compiler_params=pltpu.CompilerParams(dimension_semantics=("arbitrary",)),
        cost_estimate=pl.CostEstimate(flops=6 * s * h * f, bytes_accessed=2 * (3 * s * h + 2 * s * f + 2 * h * f), transcendentals=s * f),
        name="mlp_backward",
    )(y, g, w_up, w_down, *held)


def solution(mesh):
    nz, ny, ntp = mesh.shape['dpy'], mesh.shape['dpx'], mesh.shape['tp']
    replicas = nz * ny
    data_axes = ('dpy', 'dpx')
    act_spec = P(None, data_axes, None, None)
    tok_spec = P(data_axes, None, None)
    qkv_spec = P(None, None, None, 'tp', None)
    wout_spec = P(None, 'tp', None, None)
    up_spec = P(None, None, 'tp')
    down_spec = P(None, 'tp', None)

    core_swap = [(i, i ^ 1) for i in range(ntp)]
    chip_swap = [(i, i ^ 2) for i in range(ntp)]
    y_swap = [(0, 1), (1, 0)]
    z_fold = [(0, 1), (3, 2)]
    z_mid = [(1, 2), (2, 1)]
    z_cast = [(1, 0), (2, 3)]

    def tp_sum(part, base):
        half = part.shape[0] // 2
        core = lax.axis_index('tp') % 2
        mine, other = core * half, (1 - core) * half
        cut = lambda a, at: lax.dynamic_slice_in_dim(a, at, half, axis=0)
        got = lax.ppermute(cut(part, other), 'tp', core_swap)
        pair = (cut(part, mine).astype(F32) + got.astype(F32)).astype(BF16)
        got = lax.ppermute(pair, 'tp', chip_swap)
        own = (cut(base, mine).astype(F32) + (pair.astype(F32) + got.astype(F32))).astype(BF16)
        return mine, own, other, lax.ppermute(own, 'tp', core_swap)

    def put_rows(buf, m, s, mine, own, other, got):
        buf = lax.dynamic_update_slice_in_dim(buf, own, m * s + mine, axis=0)
        return lax.dynamic_update_slice_in_dim(buf, got, m * s + other, axis=0)

    def replica_sum(grad, axis, y_rows):
        iy, iz = lax.axis_index('dpx'), lax.axis_index('dpy')
        inner = (iz == 1) | (iz == 2)
        cut = lambda a, at, n: lax.dynamic_slice_in_dim(a, at, n, axis=axis)
        wide = lambda a: a.astype(F32)
        total = grad.shape[axis]
        h = y_rows // 2
        mine, other = iy * h, (1 - iy) * h
        r0 = lax.ppermute(cut(grad, other, h).astype(BF16), 'dpx', y_swap)
        acc = cut(grad, mine, h) + wide(r0)
        r1 = lax.ppermute(acc.astype(BF16), 'dpy', z_fold)
        acc = (acc + wide(r1)).astype(BF16)
        r2 = lax.ppermute(acc, 'dpy', z_mid)
        full = ((wide(acc) + wide(r2)) / replicas).astype(BF16)
        r3 = lax.ppermute(full, 'dpy', z_cast)
        full = jnp.where(inner, full, r3)
        r4 = lax.ppermute(full, 'dpx', y_swap)
        pieces = [jnp.where(iy == 0, full, r4), jnp.where(iy == 0, r4, full)]
        n = total - y_rows
        if n:
            h = n // 2
            tail = lax.slice_in_dim(grad, y_rows, total, axis=axis)
            r0 = lax.ppermute(tail.astype(BF16), 'dpy', z_fold)
            late = (iz > 1).astype(jnp.int32)
            mine, other = late * h, (1 - late) * h
            pick = lambda at: cut(grad, y_rows + at, h) + wide(cut(r0, at, h))
            r1 = lax.ppermute(pick(other).astype(BF16), 'dpy', z_mid)
            acc = (pick(mine) + wide(r1)).astype(BF16)
            r2 = lax.ppermute(acc, ('dpy', 'dpx'), [(ny * z + y, ny * z + 1 - y) for z in (1, 2) for y in range(ny)])
            acc = ((wide(acc) + wide(r2)) / replicas).astype(BF16)
            r3 = lax.ppermute(acc, 'dpy', z_mid)
            full = jnp.concatenate([jnp.where(late == 0, acc, r3), jnp.where(late == 0, r3, acc)], axis=axis)
            r4 = lax.ppermute(full, 'dpy', z_cast)
            pieces.append(jnp.where(inner, full, r4))
        return jnp.concatenate(pieces, axis=axis).astype(F32)

    def device_backward(x_saved, y_saved, d_out, w_qkv, w_out, w_up, w_down):
        layers, mbs, s, width = x_saved.shape
        heads, d = w_qkv.shape[3:]
        rows = mbs * s
        grad = d_out
        sums = [None] * layers
        take = lambda a, m: lax.slice_in_dim(a, m * s, (m + 1) * s, axis=0)
        for l in reversed(range(layers)):
            x, y = x_saved[l].reshape(rows, width), y_saved[l].reshape(rows, width)
            wq = w_qkv[l].reshape(width, 3 * heads * d)
            qkv = dot(x, wq).astype(BF16)
            held, mid = (), jnp.zeros((rows, width), BF16)
            parts = []
            for m in range(mbs):
                *held, part = mlp(y_saved, grad, w_up, w_down, held, l, m)
                parts.append(part)
            a, dh = held
            for m in range(mbs):
                mid = put_rows(mid, m, s, *tp_sum(parts[m], grad[m]))
            g_down = dot(a, grad.reshape(rows, width), ROWS)
            g_up = dot(y, dh, ROWS)
            sums[l] = [None, None, replica_sum(g_up, 0, width // 2), replica_sum(g_down, 0, width // 2)]
            low = jnp.zeros((rows, width), BF16)
            held = ()
            for m in range(mbs):
                *held, part = attention(qkv, mid, w_out, wq, held, l, m, mbs)
                low = put_rows(low, m, s, *tp_sum(part, take(mid, m)))
            o, dqkv = held
            g_out = dot(o, mid, ROWS)
            g_qkv = dot(x, dqkv, ROWS)
            sums[l][0] = replica_sum(g_qkv, 0, width // 2).reshape(width, 3, heads, d)
            sums[l][1] = replica_sum(g_out, 0, heads * d).reshape(heads, d, width)
            grad = low.reshape(mbs, s, width)
        grads = tuple(jnp.stack([sums[l][i] for l in range(layers)]) for i in range(4))
        return (grad,) + grads

    return jax.shard_map(device_backward, mesh=mesh, in_specs=(act_spec, act_spec, tok_spec, qkv_spec, wout_spec, up_spec, down_spec), out_specs=(tok_spec, qkv_spec, wout_spec, up_spec, down_spec), check_vma=False)
```

```python
import functools

import jax
import jax.numpy as jnp
from jax import lax
from jax.experimental import pallas as pl
from jax.experimental.pallas import tpu as pltpu
from jax.sharding import PartitionSpec as P

F32, BF16 = jnp.float32, jnp.bfloat16
PLAIN = (((1,), (0,)), ((), ()))
LANES = (((1,), (1,)), ((), ()))
ROWS = (((0,), (0,)), ((), ()))
ANY = pl.BlockSpec(memory_space=pl.ANY)
MESH = pl.DeviceIdType.MESH
TANH_1 = 0.7978845608028654
TANH_3 = 0.044715 * TANH_1


def dot(a, b, dims=PLAIN):
    return lax.dot_general(a, b, dims, preferred_element_type=F32)


def attention_kernel(scale, heads, q_ref, k_ref, v_ref, mid_ref, wo_ref, wq_ref, *refs):
    o_ref, dqkv_ref, part_ref, p_ref, ds_ref, do_ref = refs[-6:]
    n = pl.program_id(0)
    rows, d = q_ref.shape
    blk, cols = 256, 512
    do_ref[...] = dot(mid_ref[...], wo_ref[...], LANES).astype(BF16)
    keys, vals = k_ref[...], v_ref[...]
    keys_t, vals_t = keys.T, vals.T
    place = lambda c: pl.ds(pl.multiple_of((c * heads + n) * d, d), d)
    for i in range(rows // blk):
        sl = slice(i * blk, (i + 1) * blk)
        q, do = q_ref[sl, :], do_ref[sl, :]
        s = dot(keys, q, LANES)
        top = jnp.max(s, axis=0, keepdims=True)
        e = jnp.exp((s - top) * scale)
        p = e * (1.0 / jnp.sum(e, axis=0, keepdims=True))
        pb = p.astype(BF16)
        p_ref[:, sl] = pb
        o_ref[sl, :] = dot(vals_t, pb).T.astype(BF16)
        dp = dot(vals, do, LANES)
        row_dot = jnp.sum(dp * p, axis=0, keepdims=True)
        ds = (p * (dp - row_dot) * scale).astype(BF16)
        ds_ref[:, sl] = ds
        dqkv_ref[sl, place(0)] = dot(keys_t, ds).T.astype(BF16)
    dqkv_ref[:, place(1)] = dot(ds_ref[...], q_ref[...]).astype(BF16)
    dqkv_ref[:, place(2)] = dot(p_ref[...], do_ref[...]).astype(BF16)

    @pl.when(n == heads - 1)
    def _():
        for c in range(part_ref.shape[1] // cols):
            sl = slice(c * cols, (c + 1) * cols)
            part_ref[:, sl] = dot(dqkv_ref[...], wq_ref[sl, :], LANES).astype(BF16)


def attention(qkv, mid, w_out, wq, held, l, m, mbs):
    s, width = mid.shape[0] // mbs, mid.shape[1]
    heads, d = w_out.shape[1:3]
    hd = heads * d
    col = lambda c: pl.BlockSpec((s, d), lambda n: (m, c * heads + n))
    held = tuple(held)
    return pl.pallas_call(
        functools.partial(attention_kernel, d ** -0.5, heads),
        grid=(heads,),
        in_specs=[
            col(0),
            col(1),
            col(2),
            pl.BlockSpec((s, width), lambda n: (m, 0)),
            pl.BlockSpec((None, None, d, width), lambda n: (l, n, 0, 0)),
            pl.BlockSpec((width, 3 * hd), lambda n: (0, 0)),
        ]
        + [ANY] * len(held),
        out_specs=[col(0), pl.BlockSpec((s, 3 * hd), lambda n: (m, 0)), pl.BlockSpec((s, width), lambda n: (0, 0))],
        out_shape=[
            jax.ShapeDtypeStruct((mbs * s, hd), BF16),
            jax.ShapeDtypeStruct((mbs * s, 3 * hd), BF16),
            jax.ShapeDtypeStruct((s, width), BF16),
        ],
        scratch_shapes=[pltpu.VMEM((s, s), BF16), pltpu.VMEM((s, s), BF16), pltpu.VMEM((s, d), BF16)],
        input_output_aliases={6 + i: i for i in range(len(held))},
        compiler_params=pltpu.CompilerParams(dimension_semantics=("arbitrary",)),
        cost_estimate=pl.CostEstimate(
            flops=24 * hd * s * s + 8 * s * hd * width, bytes_accessed=20 * s * hd + 4 * s * width + 8 * hd * width, transcendentals=heads * s * s
        ),
        name="attention_backward",
    )(qkv, qkv, qkv, mid, w_out, wq, *held)


def mlp_kernel(y_ref, g_ref, wu_ref, wd_ref, *refs):
    a_ref, dh_ref, p_ref = refs[-3:]
    cols = 512
    y, g = y_ref[...], g_ref[...]
    for c in range(wu_ref.shape[1] // cols):
        sl = slice(c * cols, (c + 1) * cols)
        h = dot(y, wu_ref[:, sl])
        da = dot(g, wd_ref[sl, :], LANES)
        h2 = h * h
        t = jnp.tanh(h * (TANH_1 + TANH_3 * h2))
        cdf = 0.5 * t + 0.5
        slope = cdf + (0.5 * h) * (1.0 - t * t) * (TANH_1 + (3.0 * TANH_3) * h2)
        a_ref[:, sl] = (h * cdf).astype(BF16)
        dh_ref[:, sl] = (da * slope).astype(BF16)
    dh = dh_ref[...]
    for c in range(p_ref.shape[1] // cols):
        sl = slice(c * cols, (c + 1) * cols)
        p_ref[:, sl] = dot(dh, wu_ref[sl, :], LANES).astype(BF16)


def mlp(y, g, w_up, w_down, held, l, m):
    mbs, s, h = g.shape
    f = w_up.shape[2]
    blk = 256
    steps = s // blk
    put = pl.BlockSpec((blk, f), lambda i: (m * steps + i, 0))
    big = jax.ShapeDtypeStruct((mbs * s, f), BF16)
    held = tuple(held)
    return pl.pallas_call(
        mlp_kernel,
        grid=(steps,),
        in_specs=[
            pl.BlockSpec((None, None, blk, h), lambda i: (l, m, i, 0)),
            pl.BlockSpec((None, blk, h), lambda i: (m, i, 0)),
            pl.BlockSpec((None, h, f), lambda i: (l, 0, 0)),
            pl.BlockSpec((None, f, h), lambda i: (l, 0, 0)),
        ]
        + [ANY] * len(held),
        out_specs=[put, put, pl.BlockSpec((blk, h), lambda i: (i, 0))],
        out_shape=[big, big, jax.ShapeDtypeStruct((s, h), BF16)],
        input_output_aliases={4 + i: i for i in range(len(held))},
        compiler_params=pltpu.CompilerParams(dimension_semantics=("arbitrary",)),
        cost_estimate=pl.CostEstimate(flops=6 * s * h * f, bytes_accessed=2 * (3 * s * h + 2 * s * f + 2 * h * f), transcendentals=s * f),
        name="mlp_backward",
    )(y, g, w_up, w_down, *held)


class Place:
    def __init__(self):
        self.iz, self.iy = lax.axis_index("dpy"), lax.axis_index("dpx")
        self.inner = (self.iz == 1) | (self.iz == 2)
        self.outer = jnp.logical_not(self.inner)
        self.late = self.iz // 2
        self.fold = self.iz + 1 - 2 * (self.iz % 2)
        self.mid = 3 - self.iz


def entry_barrier(at):
    sem = pltpu.get_barrier_semaphore()
    here = lambda axis, i: pl.semaphore_signal(sem, inc=1, device_id={axis: i}, device_id_type=MESH)
    here("dpx", 1 - at.iy)
    here("dpy", at.fold)

    @pl.when(at.inner)
    def _():
        here("dpy", at.mid)

    pl.semaphore_wait(sem, 2 + (at.iz + 1) // 2 - 2 * (at.iz // 3))


def combine(fn, ins, out):
    rows, cols = out.shape
    blk = next(b for b in (128, 96, 64, 48, 32, 16) if rows % b == 0)
    spec = pl.BlockSpec((blk, cols), lambda i: (i, 0))

    def body(*refs):
        refs[-1][...] = fn(*(r[...].astype(F32) for r in refs[:-1])).astype(refs[-1].dtype)

    pltpu.emit_pipeline(body, grid=(rows // blk,), in_specs=[spec] * len(ins), out_specs=[spec])(*ins, out)


class Mean:
    steps = 6

    def __init__(self, at, replicas, first, g16, g32, fin, a_bufs, b_bufs, send, recv):
        self.at, self.scale = at, 1.0 / replicas
        self.g16, self.g32, self.fin = g16, g32, fin
        self.h, self.h2 = first // 2, (fin.shape[0] - first) // 2
        self.first = first
        self.r0, self.r1, self.r2, self.s1 = a_bufs
        if self.h2:
            self.b0, self.b1, self.b2, self.t1, self.t2 = b_bufs
        self.send, self.recv = send, recv

    def rows(self, ref, start, n):
        return ref.at[pl.ds(pl.multiple_of(start, 16), n), :]

    def a(self, ref, own):
        return self.rows(ref, (self.at.iy if own else 1 - self.at.iy) * self.h, self.h)

    def b(self, ref, own, base):
        return self.rows(ref, base + (self.at.late if own else 1 - self.at.late) * self.h2, self.h2)

    def copy(self, k, src, dst, axis, to):
        return pltpu.make_async_remote_copy(
            src_ref=src, dst_ref=dst, send_sem=self.send.at[k], recv_sem=self.recv.at[k], device_id={axis: to}, device_id_type=MESH
        )

    def line(self, k):
        at, fin = self.at, self.fin
        if k == 0:
            return self.copy(k, self.a(self.g16, False), self.r0, "dpx", 1 - at.iy)
        if k == 1:
            return self.copy(k, self.s1, self.r1, "dpy", at.fold)
        if k == 2:
            return self.copy(k, self.s1, self.r2, "dpy", at.mid)
        if k == 3:
            return self.copy(k, self.a(fin, True), self.a(fin, True), "dpy", at.fold)
        if k == 4:
            return self.copy(k, self.a(fin, True), self.a(fin, True), "dpx", 1 - at.iy)
        if k in (5, 6):
            return self.copy(k, self.b(self.g16, k == 6, self.first), self.b(self.b0, k == 6, 0), "dpy", at.fold)
        if k == 7:
            return self.copy(k, self.t1, self.b1, "dpy", at.mid)
        if k == 8:
            return self.copy(k, self.t2, self.b2, "dpx", 1 - at.iy)
        if k == 9:
            return self.copy(k, self.b(fin, True, self.first), self.b(fin, True, self.first), "dpy", at.mid)
        own = k == 10
        return self.copy(k, self.b(fin, own, self.first), self.b(fin, own, self.first), "dpy", at.fold)

    def landed(self, k):
        self.line(k).wait_recv()

    def step(self, n):
        at, two = self.at, bool(self.h2)
        wide = lambda f: f
        if n == 0:
            self.line(0).start()
            if two:

                @pl.when(at.outer)
                def _():
                    self.line(5).start()
                    self.line(6).start()

        elif n == 1:
            self.landed(0)

            @pl.when(at.outer)
            def _():
                combine(lambda g, r: g + r, [self.a(self.g32, True), self.r0], self.s1)
                self.line(1).start()

            if two:

                @pl.when(at.inner)
                def _():
                    self.landed(5)
                    combine(lambda g, r: g + r, [self.b(self.g32, False, self.first), self.b(self.b0, False, 0)], self.t1)
                    self.line(7).start()

        elif n == 2:

            @pl.when(at.inner)
            def _():
                self.landed(1)
                combine(lambda g, r, q: g + r + q, [self.a(self.g32, True), self.r0, self.r1], self.s1)
                self.line(2).start()
                if two:
                    self.landed(6)
                    self.landed(7)
                    own = [self.b(self.g32, True, self.first), self.b(self.b0, True, 0), self.b1]
                    combine(lambda g, r, q: g + r + q, own, self.t2)
                    self.line(8).start()

        elif n == 3:

            @pl.when(at.inner)
            def _():
                self.landed(2)
                combine(lambda s, r: (s + r) * self.scale, [self.s1, self.r2], self.a(self.fin, True))
                self.line(3).start()
                self.line(4).start()
                if two:
                    self.landed(8)
                    combine(lambda s, r: (s + r) * self.scale, [self.t2, self.b2], self.b(self.fin, True, self.first))
                    self.line(9).start()
                    self.line(10).start()

        elif n == 4:

            @pl.when(at.outer)
            def _():
                self.landed(3)
                self.line(4).start()

            if two:

                @pl.when(at.inner)
                def _():
                    self.landed(9)
                    self.line(11).start()

        else:
            self.landed(4)
            self.line(0).wait_send()
            self.line(4).wait_send()

            @pl.when(at.outer)
            def _():
                self.line(1).wait_send()
                if two:
                    self.landed(10)
                    self.landed(11)
                    self.line(5).wait_send()
                    self.line(6).wait_send()

            @pl.when(at.inner)
            def _():
                self.line(2).wait_send()
                self.line(3).wait_send()
                if two:
                    for k in (7, 8, 9, 10, 11):
                        self.line(k).wait_send()


def means_kernel(replicas, firsts, *refs):
    n = len(firsts)
    at = Place()
    entry_barrier(at)
    g16, g32, fin = refs[:n], refs[n : 2 * n], refs[2 * n : 3 * n]
    rest = list(refs[3 * n : -2])
    send, recv = refs[-2:]
    means = []
    for i in range(n):
        a = [rest.pop(0) for _ in range(4)]
        b = [rest.pop(0) for _ in range(5)] if fin[i].shape[0] > firsts[i] else None
        means.append(Mean(at, replicas, firsts[i], g16[i], g32[i], fin[i], a, b, send.at[i], recv.at[i]))
    for slot in range(n + Mean.steps - 1):
        for i in range(n):
            if 0 <= slot - i < Mean.steps:
                means[i].step(slot - i)


def replica_means(grads, firsts, replicas, collective_id):
    n = len(grads)
    shape = lambda r, c: jax.ShapeDtypeStruct((r, c), BF16)
    outs = [shape(*g.shape) for g in grads]
    for g, first in zip(grads, firsts):
        r, c = g.shape
        outs += [shape(first // 2, c)] * 4
        if r > first:
            h2 = (r - first) // 2
            outs += [shape(2 * h2, c)] + [shape(h2, c)] * 4
    return pl.pallas_call(
        functools.partial(means_kernel, replicas, firsts),
        in_specs=[ANY] * (2 * n),
        out_specs=[ANY] * len(outs),
        out_shape=outs,
        scratch_shapes=[pltpu.SemaphoreType.DMA((n, 12)), pltpu.SemaphoreType.DMA((n, 12))],
        compiler_params=pltpu.CompilerParams(collective_id=collective_id, has_side_effects=True),
        name="replica_means",
    )(*[g.astype(BF16) for g in grads], *grads)[:n]


def solution(mesh):
    nz, ny, ntp = mesh.shape['dpy'], mesh.shape['dpx'], mesh.shape['tp']
    replicas = nz * ny
    data_axes = ('dpy', 'dpx')
    act_spec = P(None, data_axes, None, None)
    tok_spec = P(data_axes, None, None)
    qkv_spec = P(None, None, None, 'tp', None)
    wout_spec = P(None, 'tp', None, None)
    up_spec = P(None, None, 'tp')
    down_spec = P(None, 'tp', None)

    core_swap = [(i, i ^ 1) for i in range(ntp)]
    chip_swap = [(i, i ^ 2) for i in range(ntp)]

    def tp_sum(part, base):
        half = part.shape[0] // 2
        core = lax.axis_index('tp') % 2
        mine, other = core * half, (1 - core) * half
        cut = lambda a, at: lax.dynamic_slice_in_dim(a, at, half, axis=0)
        got = lax.ppermute(cut(part, other), 'tp', core_swap)
        pair = (cut(part, mine).astype(F32) + got.astype(F32)).astype(BF16)
        got = lax.ppermute(pair, 'tp', chip_swap)
        own = (cut(base, mine).astype(F32) + (pair.astype(F32) + got.astype(F32))).astype(BF16)
        return mine, own, other, lax.ppermute(own, 'tp', core_swap)

    def put_rows(buf, m, s, mine, own, other, got):
        buf = lax.dynamic_update_slice_in_dim(buf, own, m * s + mine, axis=0)
        return lax.dynamic_update_slice_in_dim(buf, got, m * s + other, axis=0)

    def device_backward(x_saved, y_saved, d_out, w_qkv, w_out, w_up, w_down):
        layers, mbs, s, width = x_saved.shape
        heads, d = w_qkv.shape[3:]
        rows = mbs * s
        grad = d_out
        sums = [None] * layers
        take = lambda a, m: lax.slice_in_dim(a, m * s, (m + 1) * s, axis=0)
        for l in reversed(range(layers)):
            x, y = x_saved[l].reshape(rows, width), y_saved[l].reshape(rows, width)
            wq = w_qkv[l].reshape(width, 3 * heads * d)
            qkv = dot(x, wq).astype(BF16)
            held, mid = (), jnp.zeros((rows, width), BF16)
            parts = []
            for m in range(mbs):
                *held, part = mlp(y_saved, grad, w_up, w_down, held, l, m)
                parts.append(part)
            a, dh = held
            for m in range(mbs):
                mid = put_rows(mid, m, s, *tp_sum(parts[m], grad[m]))
            g_down = dot(a, grad.reshape(rows, width), ROWS)
            g_up = dot(y, dh, ROWS)
            low = jnp.zeros((rows, width), BF16)
            held = ()
            for m in range(mbs):
                *held, part = attention(qkv, mid, w_out, wq, held, l, m, mbs)
                low = put_rows(low, m, s, *tp_sum(part, take(mid, m)))
            o, dqkv = held
            g_out = dot(o, mid, ROWS)
            g_qkv = dot(x, dqkv, ROWS)
            sums[l] = (g_down, g_up, g_qkv, g_out)
            grad = low.reshape(mbs, s, width)
        flat = [g for l in reversed(range(layers)) for g in sums[l]]
        firsts = [width // 2, width // 2, width // 2, heads * d] * layers
        flat = replica_means(flat, firsts, replicas, 0)
        final = [flat[4 * (layers - 1 - l) : 4 * (layers - l)] for l in range(layers)]
        stack = lambda i: jnp.stack([final[l][i] for l in range(layers)]).astype(F32)
        grads = (stack(2).reshape(w_qkv.shape), stack(3).reshape(w_out.shape), stack(1), stack(0))
        return (grad,) + grads

    return jax.shard_map(device_backward, mesh=mesh, in_specs=(act_spec, act_spec, tok_spec, qkv_spec, wout_spec, up_spec, down_spec), out_specs=(tok_spec, qkv_spec, wout_spec, up_spec, down_spec), check_vma=False)
```

```python
import functools

import jax
import jax.numpy as jnp
from jax import lax
from jax.experimental import pallas as pl
from jax.experimental.pallas import tpu as pltpu
from jax.sharding import PartitionSpec as P

F32, BF16 = jnp.float32, jnp.bfloat16
PLAIN = (((1,), (0,)), ((), ()))
BLOCK = 192
LANES = (((1,), (1,)), ((), ()))
ROWS = (((0,), (0,)), ((), ()))
ANY = pl.BlockSpec(memory_space=pl.ANY)
MESH = pl.DeviceIdType.MESH
TANH_1 = 0.7978845608028654
TANH_3 = 0.044715 * TANH_1
KINDS = DOWN, UP, QKV, OUT = range(4)
(
    START,
    LOAD_MLP,
    WAIT_MLP,
    LOAD_ATTN,
    WAIT_ATTN,
    LOAD_HEAD,
    ACT,
    MLP,
    PROJECT,
    HEAD,
    PART,
    SEND,
    PAIR,
    TOTAL,
    DONE,
    FREE,
    GRAD,
    MEAN,
    FINISH,
) = range(19)


def dot(a, b, dims=PLAIN):
    return lax.dot_general(a, b, dims, preferred_element_type=F32)


def aligned(i, n=16):
    return pl.multiple_of(i, n)


class Place:
    def __init__(self):
        self.iz, self.iy, self.tp = lax.axis_index("dpy"), lax.axis_index("dpx"), lax.axis_index("tp")
        self.core = self.tp % 2
        self.other_core = self.tp + 1 - 2 * self.core
        self.other_chip = self.tp + 2 - 4 * (self.tp // 2)
        self.inner = (self.iz == 1) | (self.iz == 2)
        self.outer = jnp.logical_not(self.inner)
        self.late = self.iz // 2
        self.fold = self.iz + 1 - 2 * (self.iz % 2)
        self.mid = 3 - self.iz


def signal(sem, axis, i):
    pl.semaphore_signal(sem, inc=1, device_id={axis: i}, device_id_type=MESH)


def entry_barrier(at):
    sem = pltpu.get_barrier_semaphore()
    signal(sem, "dpx", 1 - at.iy)
    signal(sem, "dpy", at.fold)
    signal(sem, "tp", at.other_core)
    signal(sem, "tp", at.other_chip)

    @pl.when(at.inner)
    def _():
        signal(sem, "dpy", at.mid)

    pl.semaphore_wait(sem, 4 + (at.iz + 1) // 2 - 2 * (at.iz // 3))


def in_place(rows, fn):
    n = next(b for b in (32, 16) if rows % b == 0)

    @pl.loop(0, rows // n)
    def _(i):
        fn(aligned(i * n, n), n)


class Combine:
    def __init__(self, wide, narrow, sem):
        self.wide, self.narrow, self.sem = wide, narrow, sem
        self.rows = wide.shape[0]

    def __call__(self, fn, ins, out):
        rows, cols = out.shape
        for lo in range(0, rows, self.rows):
            n = min(self.rows, rows - lo)
            part = lambda ref: ref.at[pl.ds(lo, n), :]
            narrow = [self.narrow.at[k, 0:n, 0:cols] for k in range(3)]
            mine = narrow.pop()
            bufs = [self.wide.at[0:n, 0:cols] if r.dtype == F32 else narrow.pop() for r in ins]
            loads = [pltpu.make_async_copy(part(r), b, self.sem.at[k]) for k, (r, b) in enumerate(zip(ins, bufs))]
            for c in loads:
                c.start()
            for c in loads:
                c.wait()

            def block(i, k):
                at = pl.ds(i, k)
                mine[at, :] = fn(*(b[at, :].astype(F32) for b in bufs)).astype(BF16)

            in_place(n, block)
            store = pltpu.make_async_copy(mine, part(out), self.sem.at[3])
            store.start()
            store.wait()


class Mean:
    steps = 6

    def __init__(self, at, combine, replicas, base, rows, first, g16, g32, fin, a_bufs, b_bufs, send, recv):
        self.at, self.combine, self.scale = at, combine, 1.0 / replicas
        self.g16, self.g32, self.fin = g16, g32, fin
        self.h, self.h2 = first // 2, (rows - first) // 2
        self.base, self.first = base, base + first
        self.r0, self.r1, self.r2, self.s1 = a_bufs
        if self.h2:
            self.b0, self.b1, self.b2, self.t1, self.t2 = b_bufs
        self.send, self.recv = send, recv

    def a(self, ref, own):
        start = self.base + (self.at.iy if own else 1 - self.at.iy) * self.h
        return ref.at[pl.ds(aligned(start), self.h), :]

    def b(self, ref, own, base):
        start = base + (self.at.late if own else 1 - self.at.late) * self.h2
        return ref.at[pl.ds(aligned(start), self.h2), :]

    def copy(self, k, src, dst, axis, to):
        return pltpu.make_async_remote_copy(
            src_ref=src, dst_ref=dst, send_sem=self.send.at[k], recv_sem=self.recv.at[k], device_id={axis: to}, device_id_type=MESH
        )

    def line(self, k):
        at, fin = self.at, self.fin
        if k == 0:
            return self.copy(k, self.a(self.g16, False), self.r0, "dpx", 1 - at.iy)
        if k == 1:
            return self.copy(k, self.s1, self.r1, "dpy", at.fold)
        if k == 2:
            return self.copy(k, self.s1, self.r2, "dpy", at.mid)
        if k == 3:
            return self.copy(k, self.a(fin, True), self.a(fin, True), "dpy", at.fold)
        if k == 4:
            return self.copy(k, self.a(fin, True), self.a(fin, True), "dpx", 1 - at.iy)
        if k in (5, 6):
            return self.copy(k, self.b(self.g16, k == 6, self.first), self.b(self.b0, k == 6, 0), "dpy", at.fold)
        if k == 7:
            return self.copy(k, self.t1, self.b1, "dpy", at.mid)
        if k == 8:
            return self.copy(k, self.t2, self.b2, "dpx", 1 - at.iy)
        if k == 9:
            return self.copy(k, self.b(fin, True, self.first), self.b(fin, True, self.first), "dpy", at.mid)
        own = k == 10
        return self.copy(k, self.b(fin, own, self.first), self.b(fin, own, self.first), "dpy", at.fold)

    def landed(self, k):
        self.line(k).wait_recv()

    def step(self, n):
        at, two = self.at, bool(self.h2)
        if n == 0:
            self.line(0).start()
            if two:

                @pl.when(at.outer)
                def _():
                    self.line(5).start()
                    self.line(6).start()

        elif n == 1:
            self.landed(0)

            @pl.when(at.outer)
            def _():
                self.combine(lambda g, r: g + r, [self.a(self.g32, True), self.r0], self.s1)
                self.line(1).start()

            if two:

                @pl.when(at.inner)
                def _():
                    self.landed(5)
                    self.combine(lambda g, r: g + r, [self.b(self.g32, False, self.first), self.b(self.b0, False, 0)], self.t1)
                    self.line(7).start()

        elif n == 2:

            @pl.when(at.inner)
            def _():
                self.landed(1)
                self.combine(lambda g, r, q: g + r + q, [self.a(self.g32, True), self.r0, self.r1], self.s1)
                self.line(2).start()
                if two:
                    self.landed(6)
                    self.landed(7)
                    own = [self.b(self.g32, True, self.first), self.b(self.b0, True, 0), self.b1]
                    self.combine(lambda g, r, q: g + r + q, own, self.t2)
                    self.line(8).start()

        elif n == 3:

            @pl.when(at.inner)
            def _():
                self.landed(2)
                self.combine(lambda s, r: (s + r) * self.scale, [self.s1, self.r2], self.a(self.fin, True))
                self.line(3).start()
                self.line(4).start()
                if two:
                    self.landed(8)
                    self.combine(lambda s, r: (s + r) * self.scale, [self.t2, self.b2], self.b(self.fin, True, self.first))
                    self.line(9).start()
                    self.line(10).start()

        elif n == 4:

            @pl.when(at.outer)
            def _():
                self.landed(3)
                self.line(4).start()

            if two:

                @pl.when(at.inner)
                def _():
                    self.landed(9)
                    self.line(11).start()

        else:
            self.landed(4)
            self.line(0).wait_send()
            self.line(4).wait_send()

            @pl.when(at.outer)
            def _():
                self.line(1).wait_send()
                if two:
                    self.landed(10)
                    self.landed(11)
                    self.line(5).wait_send()
                    self.line(6).wait_send()

            @pl.when(at.inner)
            def _():
                self.line(2).wait_send()
                self.line(3).wait_send()
                if two:
                    for k in (7, 8, 9, 10, 11):
                        self.line(k).wait_send()


class Backward:
    def __init__(self, dims, refs):
        self.__dict__.update(dims)
        self.at = Place()
        refs = list(refs)
        for name in self.names[0]:
            setattr(self, name, refs.pop(0))
        self.fins = [refs.pop(0) for _ in KINDS]
        self.tensors = [refs.pop(0) for _ in range(self.count)]
        for name, ref in zip(self.names[1], refs, strict=True):
            setattr(self, name, ref)
        self.half = self.s // 2
        self.blk = min(256, self.half)
        self.means, self.grads = {}, {}
        tensors, i = list(self.tensors), 0
        combine = Combine(self.wide, self.narrow, self.combine_sem)
        for l in range(self.layers):
            for kind in KINDS:
                parts, first = self.cuts[kind, l]
                g16, g32, a = tensors.pop(0), tensors.pop(0), tensors.pop(0)
                rows = g16.shape[0] // parts
                b0, b = (tensors.pop(0), tensors.pop(0)) if rows > first else (None, None)
                self.grads[kind, l] = g16, g32, rows
                for p in range(parts):
                    a_bufs = [a.at[p, j] for j in range(4)]
                    b_bufs = [b0.at[p]] + [b.at[p, j] for j in range(4)] if rows > first else None
                    sems = self.dp_send.at[i], self.dp_recv.at[i]
                    self.means[kind, l, p] = Mean(self.at, combine, self.replicas, p * rows, rows, first, g16, g32, self.fins[kind].at[l], a_bufs, b_bufs, *sems)
                    i += 1

    def local(self, k, src, dst):
        return pltpu.make_async_copy(src, dst, self.local_sem.at[k])

    def mlp_weights(self, l):
        return [self.local(0, self.w_up.at[l], self.wu_v), self.local(1, self.w_down.at[l], self.wd_v)]

    def attn_weights(self, l):
        d, heads = self.hd // self.heads, self.heads
        cols = [self.local(4 + c * heads + n, self.w_qkv.at[l, c, n], self.wq_v.at[:, pl.ds((c * heads + n) * d, d)]) for c in range(3) for n in range(heads)]
        rows = [self.local(4 + 3 * heads + n, self.w_out.at[l, n], self.wo_v.at[pl.ds(n * d, d), :]) for n in range(heads)]
        return cols + rows

    def top_grad(self, m):
        return self.local(2 + m, self.d_out.at[m], self.res.at[pl.ds(m * self.s, self.s), :])

    def mlp(self, l, m, own):
        half, blk, cols = self.half, self.blk, min(512, self.f)
        start = (self.at.core if own else 1 - self.at.core) * half
        part = (self.own if own else self.part).at[m]

        def body(step, y_ref, a_ref):
            i = step.index[0]
            rows = pl.ds(aligned(m * self.s + start + i * blk, blk), blk)
            y, g = y_ref[...], self.res[rows, :]
            for c in range(self.f // cols):
                sl = slice(c * cols, (c + 1) * cols)
                h = dot(y, self.wu_v[:, sl])
                da = dot(g, self.wd_v[sl, :], LANES)
                h2 = h * h
                t = jnp.tanh(h * (TANH_1 + TANH_3 * h2))
                cdf = 0.5 * t + 0.5
                slope = cdf + (0.5 * h) * (1.0 - t * t) * (TANH_1 + (3.0 * TANH_3) * h2)
                a_ref[:, sl] = (h * cdf).astype(BF16)
                self.dh_v[rows, sl] = (da * slope).astype(BF16)
            dh = self.dh_v[rows, :]
            wcols = min(512, self.w)
            for c in range(self.w // wcols):
                sl = slice(c * wcols, (c + 1) * wcols)
                part[pl.ds(aligned(i * blk, blk), blk), sl] = dot(dh, self.wu_v[sl, :], LANES).astype(BF16)

        row = lambda width: pl.BlockSpec((blk, width), lambda i: (i, 0))
        pltpu.emit_pipeline(body, grid=(half // blk,), in_specs=[row(self.w)], out_specs=[row(self.f)], _explicit_indices=True)(
            self.y_saved.at[l, m, pl.ds(aligned(start, blk), half), :], self.act.at[pl.ds(aligned(m * self.s + start, blk), half), :]
        )

    def qkv(self, l, m):
        blk, cols = self.blk, min(384, 3 * self.hd)

        def body(x_ref, out_ref):
            x = x_ref[...]
            for c in range(3 * self.hd // cols):
                sl = slice(c * cols, (c + 1) * cols)
                out_ref[:, sl] = dot(x, self.wq_v[:, sl]).astype(BF16)

        row = lambda width: pl.BlockSpec((blk, width), lambda i: (i, 0))
        pltpu.emit_pipeline(body, grid=(self.s // blk,), in_specs=[row(self.w)], out_specs=[row(3 * self.hd)])(
            self.x_saved.at[l, m], self.qkv_hbm.at[pl.ds(m * self.s, self.s), :]
        )

    def head_loads(self, m, n):
        d = self.hd // self.heads
        slot = (m * self.heads + n) % 2
        base = 4 + 4 * self.heads + 3 * slot
        return [
            self.local(base + c, self.qkv_hbm.at[pl.ds(m * self.s, self.s), pl.ds((c * self.heads + n) * d, d)], self.head.at[slot, c])
            for c in range(3)
        ]

    def attn(self, l, m, n):
        s, d, blk = self.s, self.hd // self.heads, min(256, self.s)
        scale = d**-0.5
        slot = (m * self.heads + n) % 2
        for c in self.head_loads(m, n):
            c.wait()
        if n + 1 < self.heads:
            for c in self.head_loads(m, n + 1):
                c.start()
        mine = slice(m * s, (m + 1) * s)
        col = slice(n * d, (n + 1) * d)
        q_ref, k_ref, v_ref = (self.head.at[slot, c] for c in range(3))
        p_ref, ds_ref = self.dh_v.at[0:s, 0:s], self.dh_v.at[s : 2 * s, 0:s]
        do_ref = self.do_v
        do_ref[...] = dot(self.res[mine, :], self.wo_v[col, :], LANES).astype(BF16)
        keys, vals = k_ref[...], v_ref[...]
        keys_t, vals_t = keys.T, vals.T
        place = lambda c: slice((c * self.heads + n) * d, (c * self.heads + n + 1) * d)
        block = lambda i: slice(i * blk, (i + 1) * blk)
        scores = lambda i: (dot(keys, q_ref[block(i), :], LANES), dot(vals, do_ref[block(i), :], LANES))
        ahead = scores(0)
        for i in range(s // blk):
            sc, dp = ahead
            if i + 1 < s // blk:
                ahead = scores(i + 1)
            sl = block(i)
            out = slice(m * s + i * blk, m * s + (i + 1) * blk)
            top = jnp.max(sc, axis=0, keepdims=True)
            e = jnp.exp((sc - top) * scale)
            inv = 1.0 / jnp.sum(e, axis=0, keepdims=True)
            row_dot = jnp.sum(dp * e, axis=0, keepdims=True) * inv
            pb = (e * inv).astype(BF16)
            ds = (e * ((dp - row_dot) * (inv * scale))).astype(BF16)
            p_ref[:, sl] = pb
            ds_ref[:, sl] = ds
            self.o_v[out, col] = dot(vals_t, pb).T.astype(BF16)
            self.dqkv_v[out, place(0)] = dot(keys_t, ds).T.astype(BF16)
        self.dqkv_v[mine, place(1)] = dot(ds_ref[...], q_ref[...]).astype(BF16)
        self.dqkv_v[mine, place(2)] = dot(p_ref[...], do_ref[...]).astype(BF16)

    def attn_part(self, l, m, own):
        half, cols = self.half, min(512, self.w)
        start = (self.at.core if own else 1 - self.at.core) * half
        part = (self.own if own else self.part).at[m]

        @pl.loop(0, half // self.blk)
        def _(i):
            dqkv = self.dqkv_v[pl.ds(aligned(m * self.s + start + i * self.blk, self.blk), self.blk), :]
            for c in range(self.w // cols):
                sl = slice(c * cols, (c + 1) * cols)
                part[pl.ds(aligned(i * self.blk, self.blk), self.blk), sl] = dot(dqkv, self.wq_v[sl, :], LANES).astype(BF16)

    def tp_copy(self, k, m, src, dst, to):
        return pltpu.make_async_remote_copy(
            src_ref=src, dst_ref=dst, send_sem=self.tp_send.at[k, m], recv_sem=self.tp_recv.at[k, m], device_id={"tp": to}, device_id_type=MESH
        )

    def tp_line(self, k, m):
        at = self.at
        if k == 0:
            return self.tp_copy(0, m, self.part.at[m], self.from_core.at[m], at.other_core)
        if k == 1:
            return self.tp_copy(1, m, self.own.at[m], self.from_chip.at[m], at.other_chip)
        rows = self.res.at[pl.ds(aligned(m * self.s + at.core * self.half), self.half), :]
        return self.tp_copy(2, m, rows, rows, at.other_core)

    def tp_pair(self, m, first):
        line = self.tp_line(0, m)
        line.wait_recv()
        own, got = self.own.at[m], self.from_core.at[m]

        def add(i, n):
            r = pl.ds(i, n)
            own[r, :] = (own[r, :].astype(F32) + got[r, :].astype(F32)).astype(BF16)

        in_place(self.half, add)
        line.wait_send()
        if not first:
            pl.semaphore_wait(self.chip_free.at[m], 1)
        self.tp_line(1, m).start()

    def tp_total(self, m, last, credit):
        line = self.tp_line(1, m)
        line.wait_recv()
        own, got = self.own.at[m], self.from_chip.at[m]
        base = m * self.s + self.at.core * self.half

        def add(i, n):
            r, b = pl.ds(i, n), pl.ds(aligned(base + i, n), n)
            self.res[b, :] = (self.res[b, :].astype(F32) + (own[r, :].astype(F32) + got[r, :].astype(F32))).astype(BF16)

        in_place(self.half, add)
        line.wait_send()
        if not last:
            signal(self.chip_free.at[m], "tp", self.at.other_chip)
        if credit:
            pl.semaphore_wait(self.core_free, 1)
        self.tp_line(2, m).start()

    def tp_done(self, m):
        line = self.tp_line(2, m)
        line.wait_recv()
        line.wait_send()

    def release_rows(self):
        signal(self.core_free, "tp", self.at.other_core)

    def grad(self, kind, l, part):
        rhs = (self.res, self.dh_v, self.dqkv_v, self.res)[kind]
        g16, g32, rows = self.grads[kind, l]
        cols = g32.shape[1]
        lo, hi = part * rows, (part + 1) * rows
        tile = next(t for t in (256, 384, 128) if rows % t == 0)
        chunk = min(512 if cols % 512 == 0 else 384, cols)
        two = self.mbs * self.s

        def put(lhs, o16_ref, o32_ref):
            for c in range(cols // chunk):
                sl = slice(c * chunk, (c + 1) * chunk)
                v = dot(lhs, rhs[:, sl], ROWS)
                o32_ref[:, sl] = v
                o16_ref[:, sl] = v.astype(BF16)

        out = pl.BlockSpec((tile, cols), lambda j: (j, 0))
        dst = (g16.at[lo:hi, :], g32.at[lo:hi, :])
        grid = ((hi - lo) // tile,)
        if kind == OUT:

            def body(step, *outs):
                put(self.o_v[:, pl.ds(aligned(lo + step.index[0] * tile, tile), tile)], *outs)

            pltpu.emit_pipeline(body, grid=grid, in_specs=[], out_specs=[out, out], _explicit_indices=True)(*dst)
            return
        if kind == DOWN:
            src, spec = self.act.at[:, lo:hi], pl.BlockSpec((two, tile), lambda j: (0, j))
        else:
            src = (self.y_saved if kind == UP else self.x_saved).at[l, :, :, lo:hi]
            spec = pl.BlockSpec((self.mbs, self.s, tile), lambda j: (0, 0, j))

        def body(lhs_ref, *outs):
            put(lhs_ref[...].reshape(two, tile), *outs)

        pltpu.emit_pipeline(body, grid=grid, in_specs=[spec], out_specs=[out, out])(src, *dst)


def run(b, order):
    for what, *rest in order:
        if what == START:
            for c in b.mlp_weights(b.layers - 1):
                c.start()
            for m in range(b.mbs):
                b.top_grad(m).start()
            for c in b.attn_weights(b.layers - 1):
                c.start()
            entry_barrier(b.at)
            for m in range(b.mbs):
                b.top_grad(m).wait()
        elif what in (LOAD_MLP, LOAD_ATTN, LOAD_HEAD):
            for c in {LOAD_MLP: b.mlp_weights, LOAD_ATTN: b.attn_weights, LOAD_HEAD: b.head_loads}[what](*rest):
                c.start()
        elif what in (WAIT_MLP, WAIT_ATTN):
            for c in {WAIT_MLP: b.mlp_weights, WAIT_ATTN: b.attn_weights}[what](*rest):
                c.wait()
        elif what == SEND:
            b.tp_line(0, rest[0]).start()
        elif what == MEAN:
            *which, n = rest
            b.means[tuple(which)].step(n)
        elif what == FINISH:
            out = [b.local(2 + m, b.res.at[pl.ds(m * b.s, b.s), :], b.d_in.at[m]) for m in range(b.mbs)]
            for c in out:
                c.start()
            for c in out:
                c.wait()
        else:
            part = {
                MLP: b.mlp,
                PROJECT: b.qkv,
                HEAD: b.attn,
                PART: b.attn_part,
                PAIR: b.tp_pair,
                TOTAL: b.tp_total,
                DONE: b.tp_done,
                FREE: b.release_rows,
                GRAD: b.grad,
            }[what]
            part(*rest)


def mega_kernel(dims, order, *refs):
    run(Backward(dims, refs), order)


def backward(x_saved, y_saved, d_out, w_qkv, w_out, w_up, w_down, replicas):
    layers, mbs, s, w = x_saved.shape
    f, heads, d = w_up.shape[2], w_qkv.shape[2], w_qkv.shape[4]
    hd, rows = heads * d, mbs * s
    half = s // 2
    shapes = (f, w), (w, f), (w, 3 * hd), (hd, w)
    hbm = {"d_in": (mbs, s, w), "act": (rows, f), "qkv_hbm": (rows, 3 * hd)}
    fins = [(layers, *shape) for shape in shapes]
    cuts, tensors = {}, []
    for l in range(layers):
        for k in KINDS:
            r, c = shapes[k]
            parts, share = CUTS[l][k]
            n = r // parts
            first = round(n * share / 32) * 32
            cuts[k, l] = parts, first
            tensors += [((r, c), BF16), ((r, c), F32), ((parts, 4, first // 2, c), BF16)]
            if n > first:
                tensors += [((parts, n - first, c), BF16), ((parts, 4, (n - first) // 2, c), BF16)]
    vmem = {
        "wu_v": (w, f),
        "wd_v": (f, w),
        "wq_v": (w, 3 * hd),
        "wo_v": (hd, w),
        "res": (rows, w),
        "dh_v": (rows, f),
        "dqkv_v": (rows, 3 * hd),
        "o_v": (rows, hd),
        "part": (mbs, half, w),
        "own": (mbs, half, w),
        "from_core": (mbs, half, w),
        "from_chip": (mbs, half, w),
        "head": (2, 3, s, d),
        "do_v": (s, d),
        "narrow": (3, min(BLOCK, w // 2), w),
    }
    n = sum(parts for parts, _ in cuts.values())
    dma, regular = pltpu.SemaphoreType.DMA, pltpu.SemaphoreType.REGULAR
    sems = {
        "dp_send": dma((n, 12)),
        "dp_recv": dma((n, 12)),
        "tp_send": dma((3, mbs)),
        "tp_recv": dma((3, mbs)),
        "local_sem": dma((4 + 4 * heads + 6,)),
        "chip_free": regular((mbs,)),
        "core_free": regular,
        "combine_sem": dma((4,)),
        "wide": pltpu.VMEM((min(BLOCK, w // 2), w), F32),
    }
    ins = ("x_saved", "y_saved", "d_out", "w_qkv", "w_out", "w_up", "w_down")
    names = ((*ins, *hbm), (*vmem, *sems))
    dims = dict(names=names, count=len(tensors), layers=layers, mbs=mbs, s=s, w=w, f=f, heads=heads, hd=hd, replicas=replicas, cuts=cuts)
    outs = [(v, BF16) for v in (*hbm.values(), *fins)] + tensors
    outs = pl.pallas_call(
        functools.partial(mega_kernel, dims, ORDER),
        in_specs=[ANY] * len(ins),
        out_specs=[ANY] * len(outs),
        out_shape=[jax.ShapeDtypeStruct(*v) for v in outs],
        scratch_shapes=[pltpu.VMEM(v, BF16) for v in vmem.values()] + list(sems.values()),
        compiler_params=pltpu.CompilerParams(collective_id=0, has_side_effects=True, vmem_limit_bytes=67043328),
        name="backward",
    )(x_saved, y_saved, d_out, w_qkv, w_out, w_up, w_down)
    return outs[0], *outs[len(hbm) : len(hbm) + len(fins)]


def widen(a, pieces=0):
    layers, r, c = a.shape
    blk = min(512 if r % 512 == 0 else 384, r)
    src = pl.BlockSpec((None, blk, c), lambda l, i: (l, i, 0))
    if not pieces:
        dst, shape = src, (layers, r, c)
    else:
        dst, shape = pl.BlockSpec((None, pieces, blk, c // pieces), lambda l, i: (l, 0, i, 0)), (layers, pieces, r, c // pieces)

    def body(a_ref, o_ref):
        if not pieces:
            o_ref[...] = a_ref[...].astype(F32)
            return
        n = c // pieces
        for j in range(pieces):
            o_ref[j] = a_ref[:, j * n : (j + 1) * n].astype(F32)

    return pl.pallas_call(
        body, grid=(layers, r // blk), in_specs=[src], out_specs=dst, out_shape=jax.ShapeDtypeStruct(shape, F32), name="widen"
    )(a)


CUTS = (
    ((1, 0.5), (1, 0.5), (1, 0.5), (1, 1.0)),
    ((1, 0.5), (1, 0.5), (1, 0.5), (1, 1.0)),
)
ORDER = (
    (START,), (WAIT_MLP, 1), (MLP, 1, 0, False), (SEND, 0), (MLP, 1, 0, True), (PAIR, 0, True), (MLP, 1, 1, False), (SEND, 1),
    (MLP, 1, 1, True), (LOAD_MLP, 0), (PAIR, 1, True), (GRAD, DOWN, 1, 0), (FREE,), (MEAN, DOWN, 1, 0, 0), (GRAD, UP, 1, 0),
    (MEAN, UP, 1, 0, 0), (TOTAL, 0, False, True), (WAIT_ATTN, 1), (PROJECT, 1, 0), (PROJECT, 1, 1), (DONE, 0), (LOAD_HEAD, 0, 0),
    (HEAD, 1, 0, 0), (MEAN, DOWN, 1, 0, 1), (TOTAL, 1, False, False), (HEAD, 1, 0, 1), (DONE, 1), (HEAD, 1, 0, 2), (PART, 1, 0, False),
    (SEND, 0), (PART, 1, 0, True), (LOAD_HEAD, 1, 0), (HEAD, 1, 1, 0), (PAIR, 0, False), (HEAD, 1, 1, 1), (HEAD, 1, 1, 2), (MEAN, UP, 1, 0, 1),
    (PART, 1, 1, False), (SEND, 1), (PART, 1, 1, True), (LOAD_ATTN, 0), (GRAD, OUT, 1, 0), (FREE,), (MEAN, OUT, 1, 0, 0), (PAIR, 1, False),
    (GRAD, QKV, 1, 0), (MEAN, QKV, 1, 0, 0), (TOTAL, 0, False, True), (WAIT_ATTN, 0), (PROJECT, 0, 0), (MEAN, OUT, 1, 0, 1), (DONE, 0),
    (WAIT_MLP, 0), (MLP, 0, 0, False), (SEND, 0), (MLP, 0, 0, True), (PAIR, 0, False), (MEAN, DOWN, 1, 0, 2), (TOTAL, 1, False, False),
    (PROJECT, 0, 1), (DONE, 1), (MLP, 0, 1, False), (SEND, 1), (MEAN, UP, 1, 0, 2), (MLP, 0, 1, True), (PAIR, 1, False), (MEAN, DOWN, 1, 0, 3),
    (MEAN, QKV, 1, 0, 1), (GRAD, DOWN, 0, 0), (FREE,), (MEAN, DOWN, 0, 0, 0), (TOTAL, 0, False, True), (MEAN, UP, 1, 0, 3), (DONE, 0),
    (MEAN, OUT, 1, 0, 2), (GRAD, UP, 0, 0), (MEAN, UP, 0, 0, 0), (MEAN, DOWN, 1, 0, 4), (TOTAL, 1, False, False), (LOAD_HEAD, 0, 0),
    (HEAD, 0, 0, 0), (DONE, 1), (HEAD, 0, 0, 1), (MEAN, QKV, 1, 0, 2), (HEAD, 0, 0, 2), (MEAN, DOWN, 0, 0, 1), (PART, 0, 0, False), (SEND, 0),
    (PART, 0, 0, True), (LOAD_HEAD, 1, 0), (HEAD, 0, 1, 0), (MEAN, UP, 1, 0, 4), (PAIR, 0, False), (HEAD, 0, 1, 1), (MEAN, OUT, 1, 0, 3),
    (HEAD, 0, 1, 2), (PART, 0, 1, False), (SEND, 1), (PART, 0, 1, True), (GRAD, OUT, 0, 0), (FREE,), (MEAN, OUT, 0, 0, 0), (PAIR, 1, False),
    (GRAD, QKV, 0, 0), (MEAN, QKV, 0, 0, 0), (TOTAL, 0, True, True), (MEAN, UP, 0, 0, 1), (DONE, 0), (MEAN, QKV, 1, 0, 3),
    (TOTAL, 1, True, False), (MEAN, OUT, 0, 0, 1), (MEAN, OUT, 1, 0, 4), (DONE, 1), (FINISH,), (MEAN, DOWN, 0, 0, 2), (MEAN, QKV, 1, 0, 4),
    (MEAN, QKV, 0, 0, 1), (MEAN, DOWN, 0, 0, 3), (MEAN, UP, 0, 0, 2), (MEAN, OUT, 0, 0, 2), (MEAN, DOWN, 0, 0, 4), (MEAN, QKV, 0, 0, 2),
    (MEAN, UP, 0, 0, 3), (MEAN, OUT, 0, 0, 3), (MEAN, QKV, 0, 0, 3), (MEAN, UP, 0, 0, 4), (MEAN, OUT, 0, 0, 4), (MEAN, QKV, 0, 0, 4),
    (MEAN, DOWN, 1, 0, 5), (MEAN, UP, 1, 0, 5), (MEAN, OUT, 1, 0, 5), (MEAN, QKV, 1, 0, 5), (MEAN, DOWN, 0, 0, 5), (MEAN, OUT, 0, 0, 5),
    (MEAN, UP, 0, 0, 5), (MEAN, QKV, 0, 0, 5),
)


def solution(mesh):
    replicas = mesh.shape["dpy"] * mesh.shape["dpx"]
    data_axes = ("dpy", "dpx")
    act_spec = P(None, data_axes, None, None)
    tok_spec = P(data_axes, None, None)
    qkv_spec = P(None, None, None, "tp", None)
    wout_spec = P(None, "tp", None, None)
    up_spec = P(None, None, "tp")
    down_spec = P(None, "tp", None)

    def device_backward(x_saved, y_saved, d_out, w_qkv, w_out, w_up, w_down):
        layers, width, _, heads, d = w_qkv.shape
        by_head = jnp.transpose(w_qkv, (0, 2, 3, 1, 4))
        d_in, down, up, qkv, out = backward(x_saved, y_saved, d_out, by_head, w_out, w_up, w_down, replicas)
        g_qkv = jnp.transpose(widen(qkv, 3 * heads).reshape(layers, 3, heads, width, d), (0, 3, 1, 2, 4))
        g_out = widen(out).reshape(w_out.shape)
        return d_in, g_qkv, g_out, widen(up), widen(down)

    return jax.shard_map(
        device_backward,
        mesh=mesh,
        in_specs=(act_spec, act_spec, tok_spec, qkv_spec, wout_spec, up_spec, down_spec),
        out_specs=(tok_spec, qkv_spec, wout_spec, up_spec, down_spec),
        check_vma=False,
    )
```

```python
import functools

import jax
import jax.numpy as jnp
from jax import lax
from jax.experimental import pallas as pl
from jax.experimental.pallas import tpu as pltpu
from jax.sharding import PartitionSpec as P

F32, BF16 = jnp.float32, jnp.bfloat16
PLAIN = (((1,), (0,)), ((), ()))
BLOCK = 128
LANES = (((1,), (1,)), ((), ()))
ROWS = (((0,), (0,)), ((), ()))
ANY = pl.BlockSpec(memory_space=pl.ANY)
MESH = pl.DeviceIdType.MESH
TANH_1 = 0.7978845608028654
TANH_3 = 0.044715 * TANH_1
KINDS = DOWN, UP, QKV, OUT = range(4)
(
    START,
    LOAD_MLP,
    WAIT_MLP,
    LOAD_ATTN,
    WAIT_ATTN,
    LOAD_HEAD,
    ACT,
    MLP,
    PROJECT,
    HEAD,
    PART,
    SEND,
    PAIR,
    TOTAL,
    DONE,
    FREE,
    GRAD,
    MEAN,
    FINISH,
) = range(19)


def dot(a, b, dims=PLAIN):
    return lax.dot_general(a, b, dims, preferred_element_type=F32)


def aligned(i, n=16):
    return pl.multiple_of(i, n)


class Place:
    def __init__(self):
        self.iz, self.iy, self.tp = lax.axis_index("dpy"), lax.axis_index("dpx"), lax.axis_index("tp")
        self.core = self.tp % 2
        self.other_core = self.tp + 1 - 2 * self.core
        self.other_chip = self.tp + 2 - 4 * (self.tp // 2)
        self.inner = (self.iz == 1) | (self.iz == 2)
        self.outer = jnp.logical_not(self.inner)
        self.late = self.iz // 2
        self.fold = self.iz + 1 - 2 * (self.iz % 2)
        self.mid = 3 - self.iz


def signal(sem, axis, i):
    pl.semaphore_signal(sem, inc=1, device_id={axis: i}, device_id_type=MESH)


def entry_barrier(at):
    sem = pltpu.get_barrier_semaphore()
    signal(sem, "dpx", 1 - at.iy)
    signal(sem, "dpy", at.fold)
    signal(sem, "tp", at.other_core)
    signal(sem, "tp", at.other_chip)

    @pl.when(at.inner)
    def _():
        signal(sem, "dpy", at.mid)

    pl.semaphore_wait(sem, 4 + (at.iz + 1) // 2 - 2 * (at.iz // 3))


def in_place(rows, fn):
    n = next(b for b in (64, 48, 32, 16) if rows % b == 0)

    @pl.loop(0, rows // n)
    def _(i):
        fn(aligned(i * n, n), n)


class Combine:
    def __init__(self, wide, narrow, sem):
        self.wide, self.narrow, self.sem = wide, narrow, sem
        self.rows = wide.shape[1]

    def __call__(self, fn, ins, out):
        rows, cols = out.shape
        pieces = [(lo, min(self.rows, rows - lo)) for lo in range(0, rows, self.rows)]
        loads, bufs, stores = [], [], []
        for k, (lo, n) in enumerate(pieces):
            slot = k % 2
            narrow = [self.narrow.at[slot, b, 0:n, 0:cols] for b in range(3)]
            mine = narrow.pop()
            here = [self.wide.at[slot, 0:n, 0:cols] if r.dtype == F32 else narrow.pop() for r in ins]
            part = lambda ref: ref.at[pl.ds(lo, n), :]
            loads.append([pltpu.make_async_copy(part(r), b, self.sem.at[slot, q]) for q, (r, b) in enumerate(zip(ins, here))])
            bufs.append((here, mine))
            stores.append(pltpu.make_async_copy(mine, part(out), self.sem.at[slot, 3]))
        for c in loads[0]:
            c.start()
        for k, (lo, n) in enumerate(pieces):
            if k + 1 < len(pieces):
                for c in loads[k + 1]:
                    c.start()
            for c in loads[k]:
                c.wait()
            if k >= 2:
                stores[k - 2].wait()
            here, mine = bufs[k]

            def block(i, size, here=here, mine=mine):
                at = pl.ds(i, size)
                mine[at, :] = fn(*(b[at, :].astype(F32) for b in here)).astype(BF16)

            in_place(n, block)
            stores[k].start()
        for c in stores[-2:]:
            c.wait()


class Mean:
    steps = 6

    def __init__(self, at, combine, replicas, base, rows, first, g16, g32, fin, a_bufs, b_bufs, send, recv):
        self.at, self.combine, self.scale = at, combine, 1.0 / replicas
        self.g16, self.g32, self.fin = g16, g32, fin
        self.h, self.h2 = first // 2, (rows - first) // 2
        self.base, self.first = base, base + first
        self.r0, self.r1, self.r2, self.s1 = a_bufs
        if self.h2:
            self.b0, self.b1, self.b2, self.t1, self.t2 = b_bufs
        self.send, self.recv = send, recv

    def a(self, ref, own):
        start = self.base + (self.at.iy if own else 1 - self.at.iy) * self.h
        return ref.at[pl.ds(aligned(start), self.h), :]

    def b(self, ref, own, base):
        start = base + (self.at.late if own else 1 - self.at.late) * self.h2
        return ref.at[pl.ds(aligned(start), self.h2), :]

    def copy(self, k, src, dst, axis, to):
        return pltpu.make_async_remote_copy(
            src_ref=src, dst_ref=dst, send_sem=self.send.at[k], recv_sem=self.recv.at[k], device_id={axis: to}, device_id_type=MESH
        )

    def line(self, k):
        at, fin = self.at, self.fin
        if k == 0:
            return self.copy(k, self.a(self.g16, False), self.r0, "dpx", 1 - at.iy)
        if k == 1:
            return self.copy(k, self.s1, self.r1, "dpy", at.fold)
        if k == 2:
            return self.copy(k, self.s1, self.r2, "dpy", at.mid)
        if k == 3:
            return self.copy(k, self.a(fin, True), self.a(fin, True), "dpy", at.fold)
        if k == 4:
            return self.copy(k, self.a(fin, True), self.a(fin, True), "dpx", 1 - at.iy)
        if k in (5, 6):
            return self.copy(k, self.b(self.g16, k == 6, self.first), self.b(self.b0, k == 6, 0), "dpy", at.fold)
        if k == 7:
            return self.copy(k, self.t1, self.b1, "dpy", at.mid)
        if k == 8:
            return self.copy(k, self.t2, self.b2, "dpx", 1 - at.iy)
        if k == 9:
            return self.copy(k, self.b(fin, True, self.first), self.b(fin, True, self.first), "dpy", at.mid)
        own = k == 10
        return self.copy(k, self.b(fin, own, self.first), self.b(fin, own, self.first), "dpy", at.fold)

    def landed(self, k):
        self.line(k).wait_recv()

    def step(self, n):
        at, two = self.at, bool(self.h2)
        if n == 0:
            self.line(0).start()
            if two:

                @pl.when(at.outer)
                def _():
                    self.line(5).start()
                    self.line(6).start()

        elif n == 1:
            self.landed(0)

            @pl.when(at.outer)
            def _():
                self.combine(lambda g, r: g + r, [self.a(self.g32, True), self.r0], self.s1)
                self.line(1).start()

            if two:

                @pl.when(at.inner)
                def _():
                    self.landed(5)
                    self.combine(lambda g, r: g + r, [self.b(self.g32, False, self.first), self.b(self.b0, False, 0)], self.t1)
                    self.line(7).start()

        elif n == 2:

            @pl.when(at.inner)
            def _():
                self.landed(1)
                self.combine(lambda g, r, q: g + r + q, [self.a(self.g32, True), self.r0, self.r1], self.s1)
                self.line(2).start()
                if two:
                    self.landed(6)
                    self.landed(7)
                    own = [self.b(self.g32, True, self.first), self.b(self.b0, True, 0), self.b1]
                    self.combine(lambda g, r, q: g + r + q, own, self.t2)
                    self.line(8).start()

        elif n == 3:

            @pl.when(at.inner)
            def _():
                self.landed(2)
                self.combine(lambda s, r: (s + r) * self.scale, [self.s1, self.r2], self.a(self.fin, True))
                self.line(3).start()
                self.line(4).start()
                if two:
                    self.landed(8)
                    self.combine(lambda s, r: (s + r) * self.scale, [self.t2, self.b2], self.b(self.fin, True, self.first))
                    self.line(9).start()
                    self.line(10).start()

        elif n == 4:

            @pl.when(at.outer)
            def _():
                self.landed(3)
                self.line(4).start()

            if two:

                @pl.when(at.inner)
                def _():
                    self.landed(9)
                    self.line(11).start()

        else:
            self.landed(4)
            self.line(0).wait_send()
            self.line(4).wait_send()

            @pl.when(at.outer)
            def _():
                self.line(1).wait_send()
                if two:
                    self.landed(10)
                    self.landed(11)
                    self.line(5).wait_send()
                    self.line(6).wait_send()

            @pl.when(at.inner)
            def _():
                self.line(2).wait_send()
                self.line(3).wait_send()
                if two:
                    for k in (7, 8, 9, 10, 11):
                        self.line(k).wait_send()


class Backward:
    def __init__(self, dims, refs):
        self.__dict__.update(dims)
        self.at = Place()
        self.early = {entry[1] for entry in ORDER if entry[0] == ACT}
        refs = list(refs)
        for name in self.names[0]:
            setattr(self, name, refs.pop(0))
        self.fins = [refs.pop(0) for _ in KINDS]
        self.tensors = [refs.pop(0) for _ in range(self.count)]
        for name, ref in zip(self.names[1], refs, strict=True):
            setattr(self, name, ref)
        self.half = self.s // 2
        self.blk = min(256, self.half)
        self.means, self.grads = {}, {}
        tensors, i = list(self.tensors), 0
        combine = Combine(self.wide, self.narrow, self.combine_sem)
        for l in range(self.layers):
            for kind in KINDS:
                parts, first = self.cuts[kind, l]
                g16, g32, a = tensors.pop(0), tensors.pop(0), tensors.pop(0)
                rows = g16.shape[0] // parts
                b0, b = (tensors.pop(0), tensors.pop(0)) if rows > first else (None, None)
                self.grads[kind, l] = g16, g32, rows
                for p in range(parts):
                    a_bufs = [a.at[p, j] for j in range(4)]
                    b_bufs = [b0.at[p]] + [b.at[p, j] for j in range(4)] if rows > first else None
                    sems = self.dp_send.at[i], self.dp_recv.at[i]
                    self.means[kind, l, p] = Mean(self.at, combine, self.replicas, p * rows, rows, first, g16, g32, self.fins[kind].at[l], a_bufs, b_bufs, *sems)
                    i += 1

    def local(self, k, src, dst):
        return pltpu.make_async_copy(src, dst, self.local_sem.at[k])

    def mlp_weights(self, l):
        return [self.local(0, self.w_up.at[l], self.wu_v), self.local(1, self.w_down.at[l], self.wd_v)]

    def attn_weights(self, l):
        d, heads = self.hd // self.heads, self.heads
        cols = [self.local(4 + c * heads + n, self.w_qkv.at[l, c, n], self.wq_v.at[:, pl.ds((c * heads + n) * d, d)]) for c in range(3) for n in range(heads)]
        rows = [self.local(4 + 3 * heads + n, self.w_out.at[l, n], self.wo_v.at[pl.ds(n * d, d), :]) for n in range(heads)]
        return cols + rows

    def top_grad(self, m):
        return self.local(2 + m, self.d_out.at[m], self.res.at[pl.ds(m * self.s, self.s), :])

    def act_only(self, l, m):
        blk, cols = self.blk, min(512, self.f)

        def body(y_ref, a_ref):
            y = y_ref[...]
            for c in range(self.f // cols):
                sl = slice(c * cols, (c + 1) * cols)
                h = dot(y, self.wu_v[:, sl])
                t = jnp.tanh(h * (TANH_1 + TANH_3 * (h * h)))
                a_ref[:, sl] = (h * (0.5 * t + 0.5)).astype(BF16)

        row = lambda width: pl.BlockSpec((blk, width), lambda i: (i, 0))
        pltpu.emit_pipeline(body, grid=(self.s // blk,), in_specs=[row(self.w)], out_specs=[row(self.f)])(
            self.y_saved.at[l, m], self.act.at[pl.ds(m * self.s, self.s), :]
        )

    def mlp(self, l, m, own):
        half, blk, cols = self.half, self.blk, min(512, self.f)
        start = (self.at.core if own else 1 - self.at.core) * half
        part = (self.own if own else self.part).at[m]

        def body(step, y_ref, *a_ref):
            i = step.index[0]
            rows = pl.ds(aligned(m * self.s + start + i * blk, blk), blk)
            y, g = y_ref[...], self.res[rows, :]
            for c in range(self.f // cols):
                sl = slice(c * cols, (c + 1) * cols)
                h = dot(y, self.wu_v[:, sl])
                da = dot(g, self.wd_v[sl, :], LANES)
                h2 = h * h
                t = jnp.tanh(h * (TANH_1 + TANH_3 * h2))
                cdf = 0.5 * t + 0.5
                slope = cdf + (0.5 * h) * (1.0 - t * t) * (TANH_1 + (3.0 * TANH_3) * h2)
                for a in a_ref:
                    a[:, sl] = (h * cdf).astype(BF16)
                self.dh_v[rows, sl] = (da * slope).astype(BF16)
            dh = self.dh_v[rows, :]
            wcols = min(512, self.w)
            for c in range(self.w // wcols):
                sl = slice(c * wcols, (c + 1) * wcols)
                part[pl.ds(aligned(i * blk, blk), blk), sl] = dot(dh, self.wu_v[sl, :], LANES).astype(BF16)

        row = lambda width: pl.BlockSpec((blk, width), lambda i: (i, 0))
        outs = [] if l in self.early else [self.act.at[pl.ds(aligned(m * self.s + start, blk), half), :]]
        pltpu.emit_pipeline(body, grid=(half // blk,), in_specs=[row(self.w)], out_specs=[row(self.f)] * len(outs), _explicit_indices=True)(
            self.y_saved.at[l, m, pl.ds(aligned(start, blk), half), :], *outs
        )

    def qkv(self, l, m):
        blk, cols = self.blk, min(384, 3 * self.hd)

        def body(x_ref, out_ref):
            x = x_ref[...]
            for c in range(3 * self.hd // cols):
                sl = slice(c * cols, (c + 1) * cols)
                out_ref[:, sl] = dot(x, self.wq_v[:, sl]).astype(BF16)

        row = lambda width: pl.BlockSpec((blk, width), lambda i: (i, 0))
        pltpu.emit_pipeline(body, grid=(self.s // blk,), in_specs=[row(self.w)], out_specs=[row(3 * self.hd)])(
            self.x_saved.at[l, m], self.qkv_hbm.at[pl.ds(m * self.s, self.s), :]
        )

    def head_loads(self, m, n):
        d = self.hd // self.heads
        slot = (m * self.heads + n) % 2
        base = 4 + 4 * self.heads + 3 * slot
        return [
            self.local(base + c, self.qkv_hbm.at[pl.ds(m * self.s, self.s), pl.ds((c * self.heads + n) * d, d)], self.head.at[slot, c])
            for c in range(3)
        ]

    def attn(self, l, m, n):
        s, d, blk = self.s, self.hd // self.heads, min(256, self.s)
        scale = d**-0.5
        slot = (m * self.heads + n) % 2
        for c in self.head_loads(m, n):
            c.wait()
        if n + 1 < self.heads:
            for c in self.head_loads(m, n + 1):
                c.start()
        mine = slice(m * s, (m + 1) * s)
        col = slice(n * d, (n + 1) * d)
        q_ref, k_ref, v_ref = (self.head.at[slot, c] for c in range(3))
        p_ref, ds_ref = self.dh_v.at[0:s, 0:s], self.dh_v.at[s : 2 * s, 0:s]
        do_ref = self.do_v
        do_ref[...] = dot(self.res[mine, :], self.wo_v[col, :], LANES).astype(BF16)
        keys, vals = k_ref[...], v_ref[...]
        keys_t, vals_t = keys.T, vals.T
        place = lambda c: slice((c * self.heads + n) * d, (c * self.heads + n + 1) * d)
        block = lambda i: slice(i * blk, (i + 1) * blk)
        scores = lambda i: (dot(keys, q_ref[block(i), :], LANES), dot(vals, do_ref[block(i), :], LANES))
        ahead = scores(0)
        for i in range(s // blk):
            sc, dp = ahead
            if i + 1 < s // blk:
                ahead = scores(i + 1)
            sl = block(i)
            out = slice(m * s + i * blk, m * s + (i + 1) * blk)
            top = jnp.max(sc, axis=0, keepdims=True)
            e = jnp.exp((sc - top) * scale)
            inv = 1.0 / jnp.sum(e, axis=0, keepdims=True)
            row_dot = jnp.sum(dp * e, axis=0, keepdims=True) * inv
            pb = (e * inv).astype(BF16)
            ds = (e * ((dp - row_dot) * (inv * scale))).astype(BF16)
            p_ref[:, sl] = pb
            ds_ref[:, sl] = ds
            self.o_v[out, col] = dot(vals_t, pb).T.astype(BF16)
            self.dqkv_v[out, place(0)] = dot(keys_t, ds).T.astype(BF16)
        self.dqkv_v[mine, place(1)] = dot(ds_ref[...], q_ref[...]).astype(BF16)
        self.dqkv_v[mine, place(2)] = dot(p_ref[...], do_ref[...]).astype(BF16)

    def attn_part(self, l, m, own):
        half, cols = self.half, min(512, self.w)
        start = (self.at.core if own else 1 - self.at.core) * half
        part = (self.own if own else self.part).at[m]

        @pl.loop(0, half // self.blk)
        def _(i):
            dqkv = self.dqkv_v[pl.ds(aligned(m * self.s + start + i * self.blk, self.blk), self.blk), :]
            for c in range(self.w // cols):
                sl = slice(c * cols, (c + 1) * cols)
                part[pl.ds(aligned(i * self.blk, self.blk), self.blk), sl] = dot(dqkv, self.wq_v[sl, :], LANES).astype(BF16)

    def tp_copy(self, k, m, src, dst, to):
        return pltpu.make_async_remote_copy(
            src_ref=src, dst_ref=dst, send_sem=self.tp_send.at[k, m], recv_sem=self.tp_recv.at[k, m], device_id={"tp": to}, device_id_type=MESH
        )

    def tp_line(self, k, m):
        at = self.at
        if k == 0:
            return self.tp_copy(0, m, self.part.at[m], self.from_core.at[m], at.other_core)
        if k == 1:
            return self.tp_copy(1, m, self.own.at[m], self.from_chip.at[m], at.other_chip)
        rows = self.res.at[pl.ds(aligned(m * self.s + at.core * self.half), self.half), :]
        return self.tp_copy(2, m, rows, rows, at.other_core)

    def tp_pair(self, m, first):
        line = self.tp_line(0, m)
        line.wait_recv()
        own, got = self.own.at[m], self.from_core.at[m]

        def add(i, n):
            r = pl.ds(i, n)
            own[r, :] = (own[r, :].astype(F32) + got[r, :].astype(F32)).astype(BF16)

        in_place(self.half, add)
        line.wait_send()
        if not first:
            pl.semaphore_wait(self.chip_free.at[m], 1)
        self.tp_line(1, m).start()

    def tp_total(self, m, last, credit):
        line = self.tp_line(1, m)
        line.wait_recv()
        own, got = self.own.at[m], self.from_chip.at[m]
        base = m * self.s + self.at.core * self.half

        def add(i, n):
            r, b = pl.ds(i, n), pl.ds(aligned(base + i, n), n)
            self.res[b, :] = (self.res[b, :].astype(F32) + (own[r, :].astype(F32) + got[r, :].astype(F32))).astype(BF16)

        in_place(self.half, add)
        line.wait_send()
        if not last:
            signal(self.chip_free.at[m], "tp", self.at.other_chip)
        if credit:
            pl.semaphore_wait(self.core_free, 1)
        self.tp_line(2, m).start()

    def tp_done(self, m):
        line = self.tp_line(2, m)
        line.wait_recv()
        line.wait_send()

    def release_rows(self):
        signal(self.core_free, "tp", self.at.other_core)

    def grad(self, kind, l, part):
        rhs = (self.res, self.dh_v, self.dqkv_v, self.res)[kind]
        g16, g32, rows = self.grads[kind, l]
        cols = g32.shape[1]
        lo, hi = part * rows, (part + 1) * rows
        tile = next(t for t in (256, 384, 128) if rows % t == 0)
        chunk = min(512 if cols % 512 == 0 else 384, cols)
        two = self.mbs * self.s

        def put(lhs, o16_ref, o32_ref):
            for c in range(cols // chunk):
                sl = slice(c * chunk, (c + 1) * chunk)
                v = dot(lhs, rhs[:, sl], ROWS)
                o32_ref[:, sl] = v
                o16_ref[:, sl] = v.astype(BF16)

        out = pl.BlockSpec((tile, cols), lambda j: (j, 0))
        dst = (g16.at[lo:hi, :], g32.at[lo:hi, :])
        grid = ((hi - lo) // tile,)
        if kind == OUT:

            def body(step, *outs):
                put(self.o_v[:, pl.ds(aligned(lo + step.index[0] * tile, tile), tile)], *outs)

            pltpu.emit_pipeline(body, grid=grid, in_specs=[], out_specs=[out, out], _explicit_indices=True)(*dst)
            return
        if kind == DOWN:
            src, spec = self.act.at[:, lo:hi], pl.BlockSpec((two, tile), lambda j: (0, j))
        else:
            src = (self.y_saved if kind == UP else self.x_saved).at[l, :, :, lo:hi]
            spec = pl.BlockSpec((self.mbs, self.s, tile), lambda j: (0, 0, j))

        def body(lhs_ref, *outs):
            put(lhs_ref[...].reshape(two, tile), *outs)

        pltpu.emit_pipeline(body, grid=grid, in_specs=[spec], out_specs=[out, out])(src, *dst)


def run(b, order):
    for what, *rest in order:
        if what == START:
            up, down = b.mlp_weights(b.layers - 1)
            up.start()
            entry_barrier(b.at)
            up.wait()
            for c in [b.top_grad(m) for m in range(b.mbs)] + [down] + b.attn_weights(b.layers - 1):
                c.start()
            waiting = [b.top_grad(m) for m in range(b.mbs)]
        elif what in (LOAD_MLP, LOAD_ATTN, LOAD_HEAD):
            for c in {LOAD_MLP: b.mlp_weights, LOAD_ATTN: b.attn_weights, LOAD_HEAD: b.head_loads}[what](*rest):
                c.start()
        elif what == WAIT_MLP:
            up, down = b.mlp_weights(*rest)
            if rest[0] < b.layers - 1:
                up.wait()
            down.wait()
        elif what == WAIT_ATTN:
            for c in b.attn_weights(*rest):
                c.wait()
        elif what == SEND:
            b.tp_line(0, rest[0]).start()
        elif what == MEAN:
            *which, n = rest
            b.means[tuple(which)].step(n)
        elif what == FINISH:
            out = [b.local(2 + m, b.res.at[pl.ds(m * b.s, b.s), :], b.d_in.at[m]) for m in range(b.mbs)]
            for c in out:
                c.start()
            for c in out:
                c.wait()
        else:
            if what in (MLP, GRAD):
                while waiting:
                    waiting.pop().wait()
            part = {
                ACT: b.act_only,
                MLP: b.mlp,
                PROJECT: b.qkv,
                HEAD: b.attn,
                PART: b.attn_part,
                PAIR: b.tp_pair,
                TOTAL: b.tp_total,
                DONE: b.tp_done,
                FREE: b.release_rows,
                GRAD: b.grad,
            }[what]
            part(*rest)


def mega_kernel(dims, order, *refs):
    run(Backward(dims, refs), order)


def backward(x_saved, y_saved, d_out, w_qkv, w_out, w_up, w_down, replicas):
    layers, mbs, s, w = x_saved.shape
    f, heads, d = w_up.shape[2], w_qkv.shape[2], w_qkv.shape[4]
    hd, rows = heads * d, mbs * s
    half = s // 2
    shapes = (f, w), (w, f), (w, 3 * hd), (hd, w)
    hbm = {"d_in": (mbs, s, w), "act": (rows, f), "qkv_hbm": (rows, 3 * hd)}
    fins = [(layers, *shape) for shape in shapes]
    cuts, tensors = {}, []
    for l in range(layers):
        for k in KINDS:
            r, c = shapes[k]
            parts, share = CUTS[l][k]
            n = r // parts
            first = round(n * share / 32) * 32
            cuts[k, l] = parts, first
            tensors += [((r, c), BF16), ((r, c), F32), ((parts, 4, first // 2, c), BF16)]
            if n > first:
                tensors += [((parts, n - first, c), BF16), ((parts, 4, (n - first) // 2, c), BF16)]
    vmem = {
        "wu_v": (w, f),
        "wd_v": (f, w),
        "wq_v": (w, 3 * hd),
        "wo_v": (hd, w),
        "res": (rows, w),
        "dh_v": (rows, f),
        "dqkv_v": (rows, 3 * hd),
        "o_v": (rows, hd),
        "part": (mbs, half, w),
        "own": (mbs, half, w),
        "from_core": (mbs, half, w),
        "from_chip": (mbs, half, w),
        "head": (2, 3, s, d),
        "do_v": (s, d),
        "narrow": (2, 3, min(BLOCK, w // 2), w),
    }
    n = sum(parts for parts, _ in cuts.values())
    dma, regular = pltpu.SemaphoreType.DMA, pltpu.SemaphoreType.REGULAR
    sems = {
        "dp_send": dma((n, 12)),
        "dp_recv": dma((n, 12)),
        "tp_send": dma((3, mbs)),
        "tp_recv": dma((3, mbs)),
        "local_sem": dma((4 + 4 * heads + 6,)),
        "chip_free": regular((mbs,)),
        "core_free": regular,
        "combine_sem": dma((2, 4)),
        "wide": pltpu.VMEM((2, min(BLOCK, w // 2), w), F32),
    }
    ins = ("x_saved", "y_saved", "d_out", "w_qkv", "w_out", "w_up", "w_down")
    names = ((*ins, *hbm), (*vmem, *sems))
    dims = dict(names=names, count=len(tensors), layers=layers, mbs=mbs, s=s, w=w, f=f, heads=heads, hd=hd, replicas=replicas, cuts=cuts)
    outs = [(v, BF16) for v in (*hbm.values(), *fins)] + tensors
    outs = pl.pallas_call(
        functools.partial(mega_kernel, dims, ORDER),
        in_specs=[ANY] * len(ins),
        out_specs=[ANY] * len(outs),
        out_shape=[jax.ShapeDtypeStruct(*v) for v in outs],
        scratch_shapes=[pltpu.VMEM(v, BF16) for v in vmem.values()] + list(sems.values()),
        compiler_params=pltpu.CompilerParams(collective_id=0, has_side_effects=True, vmem_limit_bytes=67043328),
        name="backward",
    )(x_saved, y_saved, d_out, w_qkv, w_out, w_up, w_down)
    return outs[0], *outs[len(hbm) : len(hbm) + len(fins)]


def finish_kernel(jobs, *refs):
    n = len({job[0] for job in jobs})
    ins, outs = refs[:n], refs[n : 2 * n]
    narrow, wide, in_sem, out_sem = refs[2 * n :]
    depth = narrow.shape[0]

    def load(k):
        which, l, lo, rows, _ = jobs[k]
        src = ins[which].at[l, pl.ds(lo, rows), :]
        return pltpu.make_async_copy(src, narrow.at[k % depth, 0:rows, 0 : src.shape[1]], in_sem.at[k % depth])

    def store(k):
        which, l, lo, rows, pieces = jobs[k]
        cols = ins[which].shape[2]
        if pieces:
            src, dst = wide.at[k % depth, 0:rows, 0:cols], outs[which]
            width = cols // pieces
            return [
                pltpu.make_async_copy(src.at[:, pl.ds(p * width, width)], dst.at[l, p, pl.ds(lo, rows), :], out_sem.at[k % depth, p])
                for p in range(pieces)
            ]
        return [pltpu.make_async_copy(narrow.at[k % depth, 0:rows, 0:cols], outs[which].at[l, pl.ds(lo, rows), :], out_sem.at[k % depth, 0])]

    ahead = depth // 2
    for k in range(ahead):
        load(k).start()
    for k, (which, l, lo, rows, pieces) in enumerate(jobs):
        if k + ahead < len(jobs):
            if k + ahead >= depth:
                for c in store(k + ahead - depth):
                    c.wait()
            load(k + ahead).start()
        load(k).wait()
        if pieces:
            src, dst = narrow.at[k % depth], wide.at[k % depth]
            cols = ins[which].shape[2]

            def block(i, size):
                dst[pl.ds(i, size), 0:cols] = src[pl.ds(i, size), 0:cols].astype(F32)

            in_place(rows, block)
        for c in store(k):
            c.start()
    for k in range(len(jobs) - depth, len(jobs)):
        for c in store(k):
            c.wait()


def finish(d_in, fins, heads):
    ins = (d_in, *fins)
    pieces = (0, 1, 1, 3 * heads, 1)
    jobs = []
    for which, a in enumerate(ins):
        layers, r, c = a.shape
        blk = next(b for b in (256, 192, 128) if r % b == 0)
        jobs += [(which, l, lo, blk, pieces[which]) for l in range(layers) for lo in range(0, r, blk)]
    out = lambda a, p: jax.ShapeDtypeStruct(a.shape if not p else (a.shape[0], p, a.shape[1], a.shape[2] // p), F32 if p else BF16)
    depth, width = 4, max(a.shape[2] for a in ins)
    return pl.pallas_call(
        functools.partial(finish_kernel, jobs),
        in_specs=[ANY] * len(ins),
        out_specs=[ANY] * len(ins),
        out_shape=[out(a, p) for a, p in zip(ins, pieces)],
        scratch_shapes=[
            pltpu.VMEM((depth, 256, width), BF16),
            pltpu.VMEM((depth, 256, width), F32),
            pltpu.SemaphoreType.DMA((depth,)),
            pltpu.SemaphoreType.DMA((depth, 3 * heads)),
        ],
        name="finish",
    )(*ins)


CUTS = (
    ((3, 0.5833), (2, 1.0), (2, 0.6667), (1, 1.0)),
    ((1, 0.5), (1, 0.5), (1, 0.5), (1, 1.0)),
)
ORDER = (
    (START,), (ACT, 1, 0), (ACT, 1, 1), (GRAD, DOWN, 1, 0), (FREE,), (MEAN, DOWN, 1, 0, 0), (WAIT_MLP, 1), (MLP, 1, 0, False), (SEND, 0),
    (MLP, 1, 0, True), (PAIR, 0, True), (MLP, 1, 1, False), (SEND, 1), (MLP, 1, 1, True), (LOAD_MLP, 0), (PAIR, 1, True),
    (MEAN, DOWN, 1, 0, 1), (GRAD, UP, 1, 0), (MEAN, UP, 1, 0, 0), (TOTAL, 0, False, True), (WAIT_ATTN, 1), (PROJECT, 1, 0), (PROJECT, 1, 1),
    (DONE, 0), (LOAD_HEAD, 0, 0), (HEAD, 1, 0, 0), (MEAN, DOWN, 1, 0, 2), (HEAD, 1, 0, 1), (TOTAL, 1, False, False), (HEAD, 1, 0, 2),
    (DONE, 1), (PART, 1, 0, False), (SEND, 0), (PART, 1, 0, True), (MEAN, UP, 1, 0, 1), (PAIR, 0, False), (LOAD_HEAD, 1, 0), (HEAD, 1, 1, 0),
    (MEAN, DOWN, 1, 0, 3), (HEAD, 1, 1, 1), (HEAD, 1, 1, 2), (PART, 1, 1, False), (SEND, 1), (PART, 1, 1, True), (LOAD_ATTN, 0),
    (GRAD, QKV, 1, 0), (MEAN, QKV, 1, 0, 0), (PAIR, 1, False), (MEAN, UP, 1, 0, 2), (MEAN, DOWN, 1, 0, 4), (GRAD, OUT, 1, 0), (FREE,),
    (MEAN, OUT, 1, 0, 0), (TOTAL, 0, False, True), (WAIT_ATTN, 0), (PROJECT, 0, 0), (PROJECT, 0, 1), (DONE, 0), (WAIT_MLP, 0),
    (MLP, 0, 0, False), (SEND, 0), (MLP, 0, 0, True), (TOTAL, 1, False, False), (PAIR, 0, False), (MEAN, QKV, 1, 0, 1), (MEAN, UP, 1, 0, 3),
    (DONE, 1), (MLP, 0, 1, False), (SEND, 1), (MLP, 0, 1, True), (GRAD, DOWN, 0, 0), (MEAN, DOWN, 0, 0, 0), (GRAD, DOWN, 0, 1),
    (MEAN, DOWN, 0, 1, 0), (GRAD, DOWN, 0, 2), (FREE,), (MEAN, DOWN, 0, 2, 0), (PAIR, 1, False), (TOTAL, 0, False, True), (MEAN, OUT, 1, 0, 1),
    (MEAN, QKV, 1, 0, 2), (MEAN, UP, 1, 0, 4), (DONE, 0), (MEAN, DOWN, 0, 0, 1), (GRAD, UP, 0, 0), (MEAN, UP, 0, 0, 0), (MEAN, DOWN, 0, 1, 1),
    (GRAD, UP, 0, 1), (MEAN, UP, 0, 1, 0), (MEAN, DOWN, 0, 2, 1), (LOAD_HEAD, 0, 0), (HEAD, 0, 0, 0), (TOTAL, 1, False, False),
    (HEAD, 0, 0, 1), (DONE, 1), (MEAN, QKV, 1, 0, 3), (MEAN, OUT, 1, 0, 2), (HEAD, 0, 0, 2), (PART, 0, 0, False), (SEND, 0),
    (PART, 0, 0, True), (MEAN, DOWN, 0, 0, 2), (PAIR, 0, False), (MEAN, DOWN, 0, 1, 2), (MEAN, QKV, 1, 0, 4), (MEAN, UP, 0, 0, 1),
    (MEAN, DOWN, 0, 2, 2), (LOAD_HEAD, 1, 0), (HEAD, 0, 1, 0), (MEAN, OUT, 1, 0, 3), (HEAD, 0, 1, 1), (MEAN, UP, 0, 1, 1), (HEAD, 0, 1, 2),
    (PART, 0, 1, False), (SEND, 1), (PART, 0, 1, True), (GRAD, QKV, 0, 0), (MEAN, QKV, 0, 0, 0), (PAIR, 1, False), (GRAD, QKV, 0, 1),
    (MEAN, QKV, 0, 1, 0), (MEAN, OUT, 1, 0, 4), (MEAN, UP, 0, 0, 2), (MEAN, DOWN, 0, 0, 3), (MEAN, UP, 0, 1, 2), (MEAN, DOWN, 0, 1, 3),
    (GRAD, OUT, 0, 0), (FREE,), (MEAN, OUT, 0, 0, 0), (TOTAL, 0, True, True), (MEAN, DOWN, 0, 2, 3), (DONE, 0), (MEAN, UP, 0, 0, 3),
    (TOTAL, 1, True, False), (MEAN, DOWN, 0, 0, 4), (MEAN, QKV, 0, 0, 1), (DONE, 1), (FINISH,), (MEAN, QKV, 0, 1, 1), (MEAN, UP, 0, 1, 3),
    (MEAN, DOWN, 0, 1, 4), (MEAN, DOWN, 0, 2, 4), (MEAN, UP, 0, 0, 4), (MEAN, QKV, 0, 0, 2), (MEAN, OUT, 0, 0, 1), (MEAN, QKV, 0, 1, 2),
    (MEAN, OUT, 0, 0, 2), (MEAN, UP, 0, 1, 4), (MEAN, OUT, 0, 0, 3), (MEAN, OUT, 0, 0, 4), (MEAN, QKV, 0, 0, 3), (MEAN, QKV, 0, 1, 3),
    (MEAN, QKV, 0, 0, 4), (MEAN, QKV, 0, 1, 4), (MEAN, DOWN, 1, 0, 5), (MEAN, UP, 1, 0, 5), (MEAN, QKV, 1, 0, 5), (MEAN, OUT, 1, 0, 5),
    (MEAN, DOWN, 0, 0, 5), (MEAN, UP, 0, 0, 5), (MEAN, DOWN, 0, 1, 5), (MEAN, DOWN, 0, 2, 5), (MEAN, UP, 0, 1, 5), (MEAN, OUT, 0, 0, 5),
    (MEAN, QKV, 0, 0, 5), (MEAN, QKV, 0, 1, 5),
)


def solution(mesh):
    replicas = mesh.shape["dpy"] * mesh.shape["dpx"]
    data_axes = ("dpy", "dpx")
    act_spec = P(None, data_axes, None, None)
    tok_spec = P(data_axes, None, None)
    qkv_spec = P(None, None, None, "tp", None)
    wout_spec = P(None, "tp", None, None)
    up_spec = P(None, None, "tp")
    down_spec = P(None, "tp", None)

    def device_backward(x_saved, y_saved, d_out, w_qkv, w_out, w_up, w_down):
        layers, width, _, heads, d = w_qkv.shape
        by_head = jnp.transpose(w_qkv, (0, 2, 3, 1, 4))
        d_in, *fins = backward(x_saved, y_saved, d_out, by_head, w_out, w_up, w_down, replicas)
        d_in, down, up, qkv, out = finish(d_in, fins, heads)
        g_qkv = jnp.transpose(qkv.reshape(layers, 3, heads, width, d), (0, 3, 1, 2, 4))
        return d_in, g_qkv, out.reshape(w_out.shape), up.reshape(w_up.shape), down.reshape(w_down.shape)

    return jax.shard_map(
        device_backward,
        mesh=mesh,
        in_specs=(act_spec, act_spec, tok_spec, qkv_spec, wout_spec, up_spec, down_spec),
        out_specs=(tok_spec, qkv_spec, wout_spec, up_spec, down_spec),
        check_vma=False,
    )
```

```python
import functools

import jax
import jax.numpy as jnp
from jax import lax
from jax.experimental import pallas as pl
from jax.experimental.pallas import tpu as pltpu
from jax.sharding import PartitionSpec as P

F32, BF16 = jnp.float32, jnp.bfloat16
PLAIN = (((1,), (0,)), ((), ()))
BLOCK = 128
LANES = (((1,), (1,)), ((), ()))
ROWS = (((0,), (0,)), ((), ()))
ANY = pl.BlockSpec(memory_space=pl.ANY)
MESH = pl.DeviceIdType.MESH
TANH_1 = 0.7978845608028654
TANH_3 = 0.044715 * TANH_1
KINDS = DOWN, UP, QKV, OUT = range(4)
(
    START,
    LOAD_MLP,
    WAIT_MLP,
    LOAD_ATTN,
    WAIT_ATTN,
    LOAD_HEAD,
    ACT,
    MLP,
    PROJECT,
    HEAD,
    PART,
    SEND,
    PAIR,
    TOTAL,
    DONE,
    FREE,
    GRAD,
    MEAN,
    FINISH,
) = range(19)


def dot(a, b, dims=PLAIN):
    return lax.dot_general(a, b, dims, preferred_element_type=F32)


def aligned(i, n=16):
    return pl.multiple_of(i, n)


class Place:
    def __init__(self):
        self.iz, self.iy, self.tp = lax.axis_index("dpy"), lax.axis_index("dpx"), lax.axis_index("tp")
        self.core = self.tp % 2
        self.other_core = self.tp + 1 - 2 * self.core
        self.other_chip = self.tp + 2 - 4 * (self.tp // 2)
        self.inner = (self.iz == 1) | (self.iz == 2)
        self.outer = jnp.logical_not(self.inner)
        self.late = self.iz // 2
        self.fold = self.iz + 1 - 2 * (self.iz % 2)
        self.mid = 3 - self.iz


def signal(sem, axis, i):
    pl.semaphore_signal(sem, inc=1, device_id={axis: i}, device_id_type=MESH)


def entry_barrier(at):
    sem = pltpu.get_barrier_semaphore()
    signal(sem, "dpx", 1 - at.iy)
    signal(sem, "dpy", at.fold)
    signal(sem, "tp", at.other_core)
    signal(sem, "tp", at.other_chip)

    @pl.when(at.inner)
    def _():
        signal(sem, "dpy", at.mid)

    pl.semaphore_wait(sem, 4 + (at.iz + 1) // 2 - 2 * (at.iz // 3))


def in_place(rows, fn):
    n = next(b for b in (64, 48, 32, 16) if rows % b == 0)

    @pl.loop(0, rows // n)
    def _(i):
        fn(aligned(i * n, n), n)


class Combine:
    def __init__(self, wide, narrow, sem):
        self.wide, self.narrow, self.sem = wide, narrow, sem
        self.rows = wide.shape[1]

    def __call__(self, fn, ins, out):
        rows, cols = out.shape
        pieces = [(lo, min(self.rows, rows - lo)) for lo in range(0, rows, self.rows)]
        loads, bufs, stores = [], [], []
        for k, (lo, n) in enumerate(pieces):
            slot = k % 2
            narrow = [self.narrow.at[slot, b, 0:n, 0:cols] for b in range(3)]
            mine = narrow.pop()
            here = [self.wide.at[slot, 0:n, 0:cols] if r.dtype == F32 else narrow.pop() for r in ins]
            part = lambda ref: ref.at[pl.ds(lo, n), :]
            loads.append([pltpu.make_async_copy(part(r), b, self.sem.at[slot, q]) for q, (r, b) in enumerate(zip(ins, here))])
            bufs.append((here, mine))
            stores.append(pltpu.make_async_copy(mine, part(out), self.sem.at[slot, 3]))
        for c in loads[0]:
            c.start()
        for k, (lo, n) in enumerate(pieces):
            if k + 1 < len(pieces):
                for c in loads[k + 1]:
                    c.start()
            for c in loads[k]:
                c.wait()
            if k >= 2:
                stores[k - 2].wait()
            here, mine = bufs[k]

            def block(i, size, here=here, mine=mine):
                at = pl.ds(i, size)
                mine[at, :] = fn(*(b[at, :].astype(F32) for b in here)).astype(BF16)

            in_place(n, block)
            stores[k].start()
        for c in stores[-2:]:
            c.wait()


class Mean:
    steps = 6

    def __init__(self, at, combine, replicas, base, rows, first, g16, g32, fin, a_bufs, b_bufs, send, recv):
        self.at, self.combine, self.scale = at, combine, 1.0 / replicas
        self.g16, self.g32, self.fin = g16, g32, fin
        self.h, self.h2 = first // 2, (rows - first) // 2
        self.base, self.first = base, base + first
        self.r0, self.r1, self.r2, self.s1 = a_bufs
        if self.h2:
            self.b0, self.b1, self.b2, self.t1, self.t2 = b_bufs
        self.send, self.recv = send, recv

    def a(self, ref, own):
        start = self.base + (self.at.iy if own else 1 - self.at.iy) * self.h
        return ref.at[pl.ds(aligned(start), self.h), :]

    def b(self, ref, own, base):
        start = base + (self.at.late if own else 1 - self.at.late) * self.h2
        return ref.at[pl.ds(aligned(start), self.h2), :]

    def copy(self, k, src, dst, axis, to):
        return pltpu.make_async_remote_copy(
            src_ref=src, dst_ref=dst, send_sem=self.send.at[k], recv_sem=self.recv.at[k], device_id={axis: to}, device_id_type=MESH
        )

    def line(self, k):
        at, fin = self.at, self.fin
        if k == 0:
            return self.copy(k, self.a(self.g16, False), self.r0, "dpx", 1 - at.iy)
        if k == 1:
            return self.copy(k, self.s1, self.r1, "dpy", at.fold)
        if k == 2:
            return self.copy(k, self.s1, self.r2, "dpy", at.mid)
        if k == 3:
            return self.copy(k, self.a(fin, True), self.a(fin, True), "dpy", at.fold)
        if k == 4:
            return self.copy(k, self.a(fin, True), self.a(fin, True), "dpx", 1 - at.iy)
        if k in (5, 6):
            return self.copy(k, self.b(self.g16, k == 6, self.first), self.b(self.b0, k == 6, 0), "dpy", at.fold)
        if k == 7:
            return self.copy(k, self.t1, self.b1, "dpy", at.mid)
        if k == 8:
            return self.copy(k, self.t2, self.b2, "dpx", 1 - at.iy)
        if k == 9:
            return self.copy(k, self.b(fin, True, self.first), self.b(fin, True, self.first), "dpy", at.mid)
        own = k == 10
        return self.copy(k, self.b(fin, own, self.first), self.b(fin, own, self.first), "dpy", at.fold)

    def landed(self, k):
        self.line(k).wait_recv()

    def step(self, n):
        at, two = self.at, bool(self.h2)
        if n == 0:
            self.line(0).start()
            if two:

                @pl.when(at.outer)
                def _():
                    self.line(5).start()
                    self.line(6).start()

        elif n == 1:
            self.landed(0)

            @pl.when(at.outer)
            def _():
                self.combine(lambda g, r: g + r, [self.a(self.g32, True), self.r0], self.s1)
                self.line(1).start()

            if two:

                @pl.when(at.inner)
                def _():
                    self.landed(5)
                    self.combine(lambda g, r: g + r, [self.b(self.g32, False, self.first), self.b(self.b0, False, 0)], self.t1)
                    self.line(7).start()

        elif n == 2:

            @pl.when(at.inner)
            def _():
                self.landed(1)
                self.combine(lambda g, r, q: g + r + q, [self.a(self.g32, True), self.r0, self.r1], self.s1)
                self.line(2).start()
                if two:
                    self.landed(6)
                    self.landed(7)
                    own = [self.b(self.g32, True, self.first), self.b(self.b0, True, 0), self.b1]
                    self.combine(lambda g, r, q: g + r + q, own, self.t2)
                    self.line(8).start()

        elif n == 3:

            @pl.when(at.inner)
            def _():
                self.landed(2)
                self.combine(lambda s, r: (s + r) * self.scale, [self.s1, self.r2], self.a(self.fin, True))
                self.line(3).start()
                self.line(4).start()
                if two:
                    self.landed(8)
                    self.combine(lambda s, r: (s + r) * self.scale, [self.t2, self.b2], self.b(self.fin, True, self.first))
                    self.line(9).start()
                    self.line(10).start()

        elif n == 4:

            @pl.when(at.outer)
            def _():
                self.landed(3)
                self.line(4).start()

            if two:

                @pl.when(at.inner)
                def _():
                    self.landed(9)
                    self.line(11).start()

        else:
            self.landed(4)
            self.line(0).wait_send()
            self.line(4).wait_send()

            @pl.when(at.outer)
            def _():
                self.line(1).wait_send()
                if two:
                    self.landed(10)
                    self.landed(11)
                    self.line(5).wait_send()
                    self.line(6).wait_send()

            @pl.when(at.inner)
            def _():
                self.line(2).wait_send()
                self.line(3).wait_send()
                if two:
                    for k in (7, 8, 9, 10, 11):
                        self.line(k).wait_send()


class Backward:
    def __init__(self, dims, refs):
        self.__dict__.update(dims)
        self.at = Place()
        self.early = {entry[1] for entry in ORDER if entry[0] == ACT}
        refs = list(refs)
        for name in self.names[0]:
            setattr(self, name, refs.pop(0))
        self.fins = [refs.pop(0) for _ in KINDS]
        self.tensors = [refs.pop(0) for _ in range(self.count)]
        for name, ref in zip(self.names[1], refs, strict=True):
            setattr(self, name, ref)
        self.half = self.s // 2
        self.blk = min(256, self.half)
        self.means, self.grads = {}, {}
        tensors, i = list(self.tensors), 0
        combine = Combine(self.wide, self.narrow, self.combine_sem)
        for l in range(self.layers):
            for kind in KINDS:
                g16, g32 = tensors.pop(0), tensors.pop(0)
                self.grads[kind, l], base = (g16, g32), 0
                for p, (rows, first) in enumerate(CUTS[l][kind]):
                    a = tensors.pop(0)
                    a_bufs, b_bufs = [a.at[j] for j in range(4)], None
                    if rows > first:
                        b0, b = tensors.pop(0), tensors.pop(0)
                        b_bufs = [b0] + [b.at[j] for j in range(4)]
                    sems = self.dp_send.at[i], self.dp_recv.at[i]
                    self.means[kind, l, p] = Mean(self.at, combine, self.replicas, base, rows, first, g16, g32, self.fins[kind].at[l], a_bufs, b_bufs, *sems)
                    base += rows
                    i += 1

    def local(self, k, src, dst):
        return pltpu.make_async_copy(src, dst, self.local_sem.at[k])

    def mlp_weights(self, l):
        return [self.local(0, self.w_up.at[l], self.wu_v), self.local(1, self.w_down.at[l], self.wd_v)]

    def attn_weights(self, l):
        d, heads = self.hd // self.heads, self.heads
        cols = [self.local(4 + c * heads + n, self.w_qkv.at[l, c, n], self.wq_v.at[:, pl.ds((c * heads + n) * d, d)]) for c in range(3) for n in range(heads)]
        rows = [self.local(4 + 3 * heads + n, self.w_out.at[l, n], self.wo_v.at[pl.ds(n * d, d), :]) for n in range(heads)]
        return cols + rows

    def top_grad(self, m):
        return self.local(2 + m, self.d_out.at[m], self.res.at[pl.ds(m * self.s, self.s), :])

    def act_only(self, l, m):
        blk, cols = self.blk, min(512, self.f)

        def body(y_ref, a_ref):
            y = y_ref[...]
            for c in range(self.f // cols):
                sl = slice(c * cols, (c + 1) * cols)
                h = dot(y, self.wu_v[:, sl])
                t = jnp.tanh(h * (TANH_1 + TANH_3 * (h * h)))
                a_ref[:, sl] = (h * (0.5 * t + 0.5)).astype(BF16)

        row = lambda width: pl.BlockSpec((blk, width), lambda i: (i, 0))
        pltpu.emit_pipeline(body, grid=(self.s // blk,), in_specs=[row(self.w)], out_specs=[row(self.f)])(
            self.y_saved.at[l, m], self.act.at[pl.ds(m * self.s, self.s), :]
        )

    def mlp(self, l, m, own):
        half, blk, cols = self.half, self.blk, min(512, self.f)
        start = (self.at.core if own else 1 - self.at.core) * half
        part = (self.own if own else self.part).at[m]

        def body(step, y_ref, *a_ref):
            i = step.index[0]
            rows = pl.ds(aligned(m * self.s + start + i * blk, blk), blk)
            y, g = y_ref[...], self.res[rows, :]
            for c in range(self.f // cols):
                sl = slice(c * cols, (c + 1) * cols)
                h = dot(y, self.wu_v[:, sl])
                da = dot(g, self.wd_v[sl, :], LANES)
                h2 = h * h
                t = jnp.tanh(h * (TANH_1 + TANH_3 * h2))
                cdf = 0.5 * t + 0.5
                slope = cdf + (0.5 * h) * (1.0 - t * t) * (TANH_1 + (3.0 * TANH_3) * h2)
                for a in a_ref:
                    a[:, sl] = (h * cdf).astype(BF16)
                self.dh_v[rows, sl] = (da * slope).astype(BF16)
            dh = self.dh_v[rows, :]
            wcols = min(512, self.w)
            for c in range(self.w // wcols):
                sl = slice(c * wcols, (c + 1) * wcols)
                part[pl.ds(aligned(i * blk, blk), blk), sl] = dot(dh, self.wu_v[sl, :], LANES).astype(BF16)

        row = lambda width: pl.BlockSpec((blk, width), lambda i: (i, 0))
        outs = [] if l in self.early else [self.act.at[pl.ds(aligned(m * self.s + start, blk), half), :]]
        pltpu.emit_pipeline(body, grid=(half // blk,), in_specs=[row(self.w)], out_specs=[row(self.f)] * len(outs), _explicit_indices=True)(
            self.y_saved.at[l, m, pl.ds(aligned(start, blk), half), :], *outs
        )

    def qkv(self, l, m):
        blk, cols = self.blk, min(384, 3 * self.hd)

        def body(x_ref, out_ref):
            x = x_ref[...]
            for c in range(3 * self.hd // cols):
                sl = slice(c * cols, (c + 1) * cols)
                out_ref[:, sl] = dot(x, self.wq_v[:, sl]).astype(BF16)

        row = lambda width: pl.BlockSpec((blk, width), lambda i: (i, 0))
        pltpu.emit_pipeline(body, grid=(self.s // blk,), in_specs=[row(self.w)], out_specs=[row(3 * self.hd)])(
            self.x_saved.at[l, m], self.qkv_hbm.at[pl.ds(m * self.s, self.s), :]
        )

    def head_loads(self, m, n):
        d = self.hd // self.heads
        slot = (m * self.heads + n) % 2
        base = 4 + 4 * self.heads + 3 * slot
        return [
            self.local(base + c, self.qkv_hbm.at[pl.ds(m * self.s, self.s), pl.ds((c * self.heads + n) * d, d)], self.head.at[slot, c])
            for c in range(3)
        ]

    def attn(self, l, m, n):
        s, d, blk = self.s, self.hd // self.heads, min(256, self.s)
        scale = d**-0.5
        slot = (m * self.heads + n) % 2
        for c in self.head_loads(m, n):
            c.wait()
        if n + 1 < self.heads:
            for c in self.head_loads(m, n + 1):
                c.start()
        mine = slice(m * s, (m + 1) * s)
        col = slice(n * d, (n + 1) * d)
        q_ref, k_ref, v_ref = (self.head.at[slot, c] for c in range(3))
        p_ref, ds_ref = self.dh_v.at[0:s, 0:s], self.dh_v.at[s : 2 * s, 0:s]
        do_ref = self.do_v
        do_ref[...] = dot(self.res[mine, :], self.wo_v[col, :], LANES).astype(BF16)
        keys, vals = k_ref[...], v_ref[...]
        keys_t, vals_t = keys.T, vals.T
        place = lambda c: slice((c * self.heads + n) * d, (c * self.heads + n + 1) * d)
        block = lambda i: slice(i * blk, (i + 1) * blk)
        scores = lambda i: (dot(keys, q_ref[block(i), :], LANES), dot(vals, do_ref[block(i), :], LANES))
        ahead = scores(0)
        for i in range(s // blk):
            sc, dp = ahead
            if i + 1 < s // blk:
                ahead = scores(i + 1)
            sl = block(i)
            out = slice(m * s + i * blk, m * s + (i + 1) * blk)
            top = jnp.max(sc, axis=0, keepdims=True)
            e = jnp.exp((sc - top) * scale)
            inv = 1.0 / jnp.sum(e, axis=0, keepdims=True)
            row_dot = jnp.sum(dp * e, axis=0, keepdims=True) * inv
            pb = (e * inv).astype(BF16)
            ds = (e * ((dp - row_dot) * (inv * scale))).astype(BF16)
            p_ref[:, sl] = pb
            ds_ref[:, sl] = ds
            self.o_v[out, col] = dot(vals_t, pb).T.astype(BF16)
            self.dqkv_v[out, place(0)] = dot(keys_t, ds).T.astype(BF16)
        self.dqkv_v[mine, place(1)] = dot(ds_ref[...], q_ref[...]).astype(BF16)
        self.dqkv_v[mine, place(2)] = dot(p_ref[...], do_ref[...]).astype(BF16)

    def attn_part(self, l, m, own):
        half, cols = self.half, min(512, self.w)
        start = (self.at.core if own else 1 - self.at.core) * half
        part = (self.own if own else self.part).at[m]

        @pl.loop(0, half // self.blk)
        def _(i):
            dqkv = self.dqkv_v[pl.ds(aligned(m * self.s + start + i * self.blk, self.blk), self.blk), :]
            for c in range(self.w // cols):
                sl = slice(c * cols, (c + 1) * cols)
                part[pl.ds(aligned(i * self.blk, self.blk), self.blk), sl] = dot(dqkv, self.wq_v[sl, :], LANES).astype(BF16)

    def tp_copy(self, k, m, src, dst, to):
        return pltpu.make_async_remote_copy(
            src_ref=src, dst_ref=dst, send_sem=self.tp_send.at[k, m], recv_sem=self.tp_recv.at[k, m], device_id={"tp": to}, device_id_type=MESH
        )

    def tp_line(self, k, m):
        at = self.at
        if k == 0:
            return self.tp_copy(0, m, self.part.at[m], self.from_core.at[m], at.other_core)
        if k == 1:
            return self.tp_copy(1, m, self.own.at[m], self.from_chip.at[m], at.other_chip)
        rows = self.res.at[pl.ds(aligned(m * self.s + at.core * self.half), self.half), :]
        return self.tp_copy(2, m, rows, rows, at.other_core)

    def tp_pair(self, m, first):
        line = self.tp_line(0, m)
        line.wait_recv()
        own, got = self.own.at[m], self.from_core.at[m]

        def add(i, n):
            r = pl.ds(i, n)
            own[r, :] = (own[r, :].astype(F32) + got[r, :].astype(F32)).astype(BF16)

        in_place(self.half, add)
        line.wait_send()
        if not first:
            pl.semaphore_wait(self.chip_free.at[m], 1)
        self.tp_line(1, m).start()

    def tp_total(self, m, last, credit):
        line = self.tp_line(1, m)
        line.wait_recv()
        own, got = self.own.at[m], self.from_chip.at[m]
        base = m * self.s + self.at.core * self.half

        def add(i, n):
            r, b = pl.ds(i, n), pl.ds(aligned(base + i, n), n)
            self.res[b, :] = (self.res[b, :].astype(F32) + (own[r, :].astype(F32) + got[r, :].astype(F32))).astype(BF16)

        in_place(self.half, add)
        line.wait_send()
        if not last:
            signal(self.chip_free.at[m], "tp", self.at.other_chip)
        if credit:
            pl.semaphore_wait(self.core_free, 1)
        self.tp_line(2, m).start()

    def tp_done(self, m):
        line = self.tp_line(2, m)
        line.wait_recv()
        line.wait_send()

    def release_rows(self):
        signal(self.core_free, "tp", self.at.other_core)

    def grad(self, kind, l, part):
        rhs = (self.res, self.dh_v, self.dqkv_v, self.res)[kind]
        g16, g32 = self.grads[kind, l]
        cols = g32.shape[1]
        sizes = [rows for rows, _ in CUTS[l][kind]]
        lo, rows = sum(sizes[:part]), sizes[part]
        hi = lo + rows
        tile = next(t for t in (256, 384, 128) if rows % t == 0)
        chunk = min(512 if cols % 512 == 0 else 384, cols)
        two = self.mbs * self.s

        def put(lhs, o16_ref, o32_ref):
            for c in range(cols // chunk):
                sl = slice(c * chunk, (c + 1) * chunk)
                v = dot(lhs, rhs[:, sl], ROWS)
                o32_ref[:, sl] = v
                o16_ref[:, sl] = v.astype(BF16)

        out = pl.BlockSpec((tile, cols), lambda j: (j, 0))
        dst = (g16.at[lo:hi, :], g32.at[lo:hi, :])
        grid = ((hi - lo) // tile,)
        if kind == OUT:

            def body(step, *outs):
                put(self.o_v[:, pl.ds(aligned(lo + step.index[0] * tile, tile), tile)], *outs)

            pltpu.emit_pipeline(body, grid=grid, in_specs=[], out_specs=[out, out], _explicit_indices=True)(*dst)
            return
        if kind == DOWN:
            src, spec = self.act.at[:, lo:hi], pl.BlockSpec((two, tile), lambda j: (0, j))
        else:
            src = (self.y_saved if kind == UP else self.x_saved).at[l, :, :, lo:hi]
            spec = pl.BlockSpec((self.mbs, self.s, tile), lambda j: (0, 0, j))

        def body(lhs_ref, *outs):
            put(lhs_ref[...].reshape(two, tile), *outs)

        pltpu.emit_pipeline(body, grid=grid, in_specs=[spec], out_specs=[out, out])(src, *dst)


def run(b, order):
    for what, *rest in order:
        if what == START:
            up, down = b.mlp_weights(b.layers - 1)
            up.start()
            entry_barrier(b.at)
            up.wait()
            for c in [b.top_grad(m) for m in range(b.mbs)] + [down] + b.attn_weights(b.layers - 1):
                c.start()
            waiting = [b.top_grad(m) for m in range(b.mbs)]
        elif what in (LOAD_MLP, LOAD_ATTN, LOAD_HEAD):
            for c in {LOAD_MLP: b.mlp_weights, LOAD_ATTN: b.attn_weights, LOAD_HEAD: b.head_loads}[what](*rest):
                c.start()
        elif what == WAIT_MLP:
            up, down = b.mlp_weights(*rest)
            if rest[0] < b.layers - 1:
                up.wait()
            down.wait()
        elif what == WAIT_ATTN:
            for c in b.attn_weights(*rest):
                c.wait()
        elif what == SEND:
            b.tp_line(0, rest[0]).start()
        elif what == MEAN:
            *which, n = rest
            b.means[tuple(which)].step(n)
        elif what == FINISH:
            out = [b.local(2 + m, b.res.at[pl.ds(m * b.s, b.s), :], b.d_in.at[m]) for m in range(b.mbs)]
            for c in out:
                c.start()
            for c in out:
                c.wait()
        else:
            if what in (MLP, GRAD):
                while waiting:
                    waiting.pop().wait()
            part = {
                ACT: b.act_only,
                MLP: b.mlp,
                PROJECT: b.qkv,
                HEAD: b.attn,
                PART: b.attn_part,
                PAIR: b.tp_pair,
                TOTAL: b.tp_total,
                DONE: b.tp_done,
                FREE: b.release_rows,
                GRAD: b.grad,
            }[what]
            part(*rest)


def mega_kernel(dims, order, *refs):
    run(Backward(dims, refs), order)


def backward(x_saved, y_saved, d_out, w_qkv, w_out, w_up, w_down, replicas):
    layers, mbs, s, w = x_saved.shape
    f, heads, d = w_up.shape[2], w_qkv.shape[2], w_qkv.shape[4]
    hd, rows = heads * d, mbs * s
    half = s // 2
    shapes = (f, w), (w, f), (w, 3 * hd), (hd, w)
    hbm = {"d_in": (mbs, s, w), "act": (rows, f), "qkv_hbm": (rows, 3 * hd)}
    fins = [(layers, *shape) for shape in shapes]
    tensors = []
    for l in range(layers):
        for (r, c), cuts in zip(shapes, CUTS[l], strict=True):
            tensors += [((r, c), BF16), ((r, c), F32)]
            for n, first in cuts:
                tensors += [((4, first // 2, c), BF16)]
                if n > first:
                    tensors += [((n - first, c), BF16), ((4, (n - first) // 2, c), BF16)]
    vmem = {
        "wu_v": (w, f),
        "wd_v": (f, w),
        "wq_v": (w, 3 * hd),
        "wo_v": (hd, w),
        "res": (rows, w),
        "dh_v": (rows, f),
        "dqkv_v": (rows, 3 * hd),
        "o_v": (rows, hd),
        "part": (mbs, half, w),
        "own": (mbs, half, w),
        "from_core": (mbs, half, w),
        "from_chip": (mbs, half, w),
        "head": (2, 3, s, d),
        "do_v": (s, d),
        "narrow": (2, 3, min(BLOCK, w // 2), w),
    }
    n = sum(len(cuts) for layer in CUTS for cuts in layer)
    dma, regular = pltpu.SemaphoreType.DMA, pltpu.SemaphoreType.REGULAR
    sems = {
        "dp_send": dma((n, 12)),
        "dp_recv": dma((n, 12)),
        "tp_send": dma((3, mbs)),
        "tp_recv": dma((3, mbs)),
        "local_sem": dma((4 + 4 * heads + 6,)),
        "chip_free": regular((mbs,)),
        "core_free": regular,
        "combine_sem": dma((2, 4)),
        "wide": pltpu.VMEM((2, min(BLOCK, w // 2), w), F32),
    }
    ins = ("x_saved", "y_saved", "d_out", "w_qkv", "w_out", "w_up", "w_down")
    names = ((*ins, *hbm), (*vmem, *sems))
    dims = dict(names=names, count=len(tensors), layers=layers, mbs=mbs, s=s, w=w, f=f, heads=heads, hd=hd, replicas=replicas)
    outs = [(v, BF16) for v in (*hbm.values(), *fins)] + tensors
    outs = pl.pallas_call(
        functools.partial(mega_kernel, dims, ORDER),
        in_specs=[ANY] * len(ins),
        out_specs=[ANY] * len(outs),
        out_shape=[jax.ShapeDtypeStruct(*v) for v in outs],
        scratch_shapes=[pltpu.VMEM(v, BF16) for v in vmem.values()] + list(sems.values()),
        compiler_params=pltpu.CompilerParams(collective_id=0, has_side_effects=True, vmem_limit_bytes=67043328),
        name="backward",
    )(x_saved, y_saved, d_out, w_qkv, w_out, w_up, w_down)
    return outs[0], *outs[len(hbm) : len(hbm) + len(fins)]


def finish_kernel(jobs, *refs):
    n = len({job[0] for job in jobs})
    ins, outs = refs[:n], refs[n : 2 * n]
    narrow, wide, in_sem, out_sem = refs[2 * n :]
    depth = narrow.shape[0]

    def load(k):
        which, l, lo, rows, _ = jobs[k]
        src = ins[which].at[l, pl.ds(lo, rows), :]
        return pltpu.make_async_copy(src, narrow.at[k % depth, 0:rows, 0 : src.shape[1]], in_sem.at[k % depth])

    def store(k):
        which, l, lo, rows, pieces = jobs[k]
        cols = ins[which].shape[2]
        if pieces:
            src, dst = wide.at[k % depth, 0:rows, 0:cols], outs[which]
            width = cols // pieces
            return [
                pltpu.make_async_copy(src.at[:, pl.ds(p * width, width)], dst.at[l, p, pl.ds(lo, rows), :], out_sem.at[k % depth, p])
                for p in range(pieces)
            ]
        return [pltpu.make_async_copy(narrow.at[k % depth, 0:rows, 0:cols], outs[which].at[l, pl.ds(lo, rows), :], out_sem.at[k % depth, 0])]

    ahead = depth // 2
    for k in range(ahead):
        load(k).start()
    for k, (which, l, lo, rows, pieces) in enumerate(jobs):
        if k + ahead < len(jobs):
            if k + ahead >= depth:
                for c in store(k + ahead - depth):
                    c.wait()
            load(k + ahead).start()
        load(k).wait()
        if pieces:
            src, dst = narrow.at[k % depth], wide.at[k % depth]
            cols = ins[which].shape[2]

            def block(i, size):
                dst[pl.ds(i, size), 0:cols] = src[pl.ds(i, size), 0:cols].astype(F32)

            in_place(rows, block)
        for c in store(k):
            c.start()
    for k in range(len(jobs) - depth, len(jobs)):
        for c in store(k):
            c.wait()


def finish(d_in, fins, heads):
    ins = (d_in, *fins)
    pieces = (0, 1, 1, 3 * heads, 1)
    jobs = []
    for which, a in enumerate(ins):
        layers, r, c = a.shape
        blk = next(b for b in (256, 192, 128) if r % b == 0)
        jobs += [(which, l, lo, blk, pieces[which]) for l in range(layers) for lo in range(0, r, blk)]
    out = lambda a, p: jax.ShapeDtypeStruct(a.shape if not p else (a.shape[0], p, a.shape[1], a.shape[2] // p), F32 if p else BF16)
    depth, width = 6, max(a.shape[2] for a in ins)
    return pl.pallas_call(
        functools.partial(finish_kernel, jobs),
        in_specs=[ANY] * len(ins),
        out_specs=[ANY] * len(ins),
        out_shape=[out(a, p) for a, p in zip(ins, pieces)],
        scratch_shapes=[
            pltpu.VMEM((depth, 256, width), BF16),
            pltpu.VMEM((depth, 256, width), F32),
            pltpu.SemaphoreType.DMA((depth,)),
            pltpu.SemaphoreType.DMA((depth, 3 * heads)),
        ],
        name="finish",
    )(*ins)


CUTS = (
    (((896, 288), (384, 384), (128, 96), (128, 128)), ((896, 896), (512, 512), (128, 64)), ((512, 512), (1024, 640)), ((384, 384),)),
    (((1536, 864),), ((1536, 704),), ((1536, 288),), ((384, 384),)),
)
ORDER = (
    (START,), (ACT, 1, 0), (ACT, 1, 1), (GRAD, DOWN, 1, 0), (FREE,), (MEAN, DOWN, 1, 0, 0), (WAIT_MLP, 1), (MLP, 1, 0, False), (SEND, 0),
    (MLP, 1, 0, True), (PAIR, 0, True), (MLP, 1, 1, False), (SEND, 1), (MEAN, DOWN, 1, 0, 1), (MLP, 1, 1, True), (LOAD_MLP, 0),
    (PAIR, 1, True), (GRAD, UP, 1, 0), (MEAN, UP, 1, 0, 0), (TOTAL, 0, False, True), (WAIT_ATTN, 1), (PROJECT, 1, 0), (DONE, 0),
    (PROJECT, 1, 1), (LOAD_HEAD, 0, 0), (HEAD, 1, 0, 0), (MEAN, DOWN, 1, 0, 2), (HEAD, 1, 0, 1), (TOTAL, 1, False, False), (HEAD, 1, 0, 2),
    (MEAN, UP, 1, 0, 1), (DONE, 1), (PART, 1, 0, False), (SEND, 0), (PART, 1, 0, True), (LOAD_HEAD, 1, 0), (HEAD, 1, 1, 0),
    (MEAN, DOWN, 1, 0, 3), (PAIR, 0, False), (HEAD, 1, 1, 1), (HEAD, 1, 1, 2), (GRAD, QKV, 1, 0), (MEAN, QKV, 1, 0, 0), (MEAN, UP, 1, 0, 2),
    (PART, 1, 1, False), (SEND, 1), (MEAN, DOWN, 1, 0, 4), (PART, 1, 1, True), (LOAD_ATTN, 0), (GRAD, OUT, 1, 0), (FREE,),
    (MEAN, OUT, 1, 0, 0), (TOTAL, 0, False, True), (PAIR, 1, False), (WAIT_ATTN, 0), (PROJECT, 0, 0), (DONE, 0), (PROJECT, 0, 1),
    (MEAN, QKV, 1, 0, 1), (WAIT_MLP, 0), (MLP, 0, 0, False), (SEND, 0), (MEAN, UP, 1, 0, 3), (MLP, 0, 0, True), (MEAN, OUT, 1, 0, 1),
    (PAIR, 0, False), (TOTAL, 1, False, False), (MEAN, QKV, 1, 0, 2), (DONE, 1), (MLP, 0, 1, False), (SEND, 1), (MEAN, OUT, 1, 0, 2),
    (MLP, 0, 1, True), (PAIR, 1, False), (MEAN, UP, 1, 0, 4), (GRAD, DOWN, 0, 0), (MEAN, DOWN, 0, 0, 0), (GRAD, DOWN, 0, 1),
    (MEAN, DOWN, 0, 1, 0), (MEAN, QKV, 1, 0, 3), (GRAD, DOWN, 0, 2), (MEAN, DOWN, 0, 2, 0), (GRAD, DOWN, 0, 3), (FREE,), (MEAN, DOWN, 0, 3, 0),
    (TOTAL, 0, False, True), (MEAN, OUT, 1, 0, 3), (GRAD, UP, 0, 0), (MEAN, UP, 0, 0, 0), (DONE, 0), (GRAD, UP, 0, 1), (MEAN, UP, 0, 1, 0),
    (MEAN, DOWN, 0, 0, 1), (TOTAL, 1, False, False), (GRAD, UP, 0, 2), (MEAN, UP, 0, 2, 0), (LOAD_HEAD, 0, 0), (HEAD, 0, 0, 0),
    (MEAN, QKV, 1, 0, 4), (MEAN, DOWN, 0, 1, 1), (MEAN, DOWN, 0, 2, 1), (MEAN, DOWN, 0, 3, 1), (DONE, 1), (HEAD, 0, 0, 1), (HEAD, 0, 0, 2),
    (MEAN, DOWN, 0, 0, 2), (PART, 0, 0, False), (SEND, 0), (MEAN, DOWN, 0, 1, 2), (MEAN, DOWN, 0, 2, 2), (MEAN, OUT, 1, 0, 4),
    (MEAN, DOWN, 0, 3, 2), (PART, 0, 0, True), (PAIR, 0, False), (MEAN, UP, 0, 0, 1), (LOAD_HEAD, 1, 0), (HEAD, 0, 1, 0),
    (MEAN, DOWN, 0, 1, 3), (HEAD, 0, 1, 1), (MEAN, UP, 0, 1, 1), (MEAN, UP, 0, 2, 1), (MEAN, DOWN, 0, 3, 3), (HEAD, 0, 1, 2),
    (GRAD, QKV, 0, 0), (MEAN, QKV, 0, 0, 0), (MEAN, UP, 0, 0, 2), (MEAN, DOWN, 0, 1, 4), (MEAN, DOWN, 0, 0, 3), (MEAN, DOWN, 0, 3, 4),
    (MEAN, DOWN, 0, 2, 3), (GRAD, QKV, 0, 1), (MEAN, QKV, 0, 1, 0), (MEAN, UP, 0, 1, 2), (MEAN, UP, 0, 2, 2), (PART, 0, 1, False), (SEND, 1),
    (PART, 0, 1, True), (GRAD, OUT, 0, 0), (FREE,), (MEAN, OUT, 0, 0, 0), (MEAN, QKV, 0, 0, 1), (MEAN, UP, 0, 0, 3), (TOTAL, 0, True, True),
    (PAIR, 1, False), (DONE, 0), (MEAN, QKV, 0, 0, 2), (MEAN, DOWN, 0, 0, 4), (MEAN, DOWN, 0, 2, 4), (MEAN, QKV, 0, 1, 1), (MEAN, UP, 0, 0, 4),
    (MEAN, UP, 0, 1, 3), (MEAN, OUT, 0, 0, 1), (MEAN, UP, 0, 2, 3), (TOTAL, 1, True, False), (MEAN, QKV, 0, 0, 3), (MEAN, OUT, 0, 0, 2),
    (DONE, 1), (FINISH,), (MEAN, QKV, 0, 1, 2), (MEAN, UP, 0, 1, 4), (MEAN, UP, 0, 2, 4), (MEAN, OUT, 0, 0, 3), (MEAN, QKV, 0, 0, 4),
    (MEAN, OUT, 0, 0, 4), (MEAN, QKV, 0, 1, 3), (MEAN, QKV, 0, 1, 4), (MEAN, DOWN, 1, 0, 5), (MEAN, UP, 1, 0, 5), (MEAN, QKV, 1, 0, 5),
    (MEAN, OUT, 1, 0, 5), (MEAN, DOWN, 0, 1, 5), (MEAN, DOWN, 0, 3, 5), (MEAN, DOWN, 0, 0, 5), (MEAN, DOWN, 0, 2, 5), (MEAN, UP, 0, 0, 5),
    (MEAN, UP, 0, 1, 5), (MEAN, UP, 0, 2, 5), (MEAN, QKV, 0, 0, 5), (MEAN, OUT, 0, 0, 5), (MEAN, QKV, 0, 1, 5),
)


def solution(mesh):
    replicas = mesh.shape["dpy"] * mesh.shape["dpx"]
    data_axes = ("dpy", "dpx")
    act_spec = P(None, data_axes, None, None)
    tok_spec = P(data_axes, None, None)
    qkv_spec = P(None, None, None, "tp", None)
    wout_spec = P(None, "tp", None, None)
    up_spec = P(None, None, "tp")
    down_spec = P(None, "tp", None)

    def device_backward(x_saved, y_saved, d_out, w_qkv, w_out, w_up, w_down):
        layers, width, _, heads, d = w_qkv.shape
        by_head = jnp.transpose(w_qkv, (0, 2, 3, 1, 4))
        d_in, *fins = backward(x_saved, y_saved, d_out, by_head, w_out, w_up, w_down, replicas)
        d_in, down, up, qkv, out = finish(d_in, fins, heads)
        g_qkv = jnp.transpose(qkv.reshape(layers, 3, heads, width, d), (0, 3, 1, 2, 4))
        return d_in, g_qkv, out.reshape(w_out.shape), up.reshape(w_up.shape), down.reshape(w_down.shape)

    return jax.shard_map(
        device_backward,
        mesh=mesh,
        in_specs=(act_spec, act_spec, tok_spec, qkv_spec, wout_spec, up_spec, down_spec),
        out_specs=(tok_spec, qkv_spec, wout_spec, up_spec, down_spec),
        check_vma=False,
    )
```

```python
import functools

import jax
import jax.numpy as jnp
from jax import lax
from jax.experimental import pallas as pl
from jax.experimental.pallas import tpu as pltpu
from jax.sharding import PartitionSpec as P

F32, BF16 = jnp.float32, jnp.bfloat16
PLAIN = (((1,), (0,)), ((), ()))
BLOCK = 128
LANES = (((1,), (1,)), ((), ()))
ROWS = (((0,), (0,)), ((), ()))
ANY = pl.BlockSpec(memory_space=pl.ANY)
MESH = pl.DeviceIdType.MESH
TANH_1 = 0.7978845608028654
TANH_3 = 0.044715 * TANH_1
KINDS = DOWN, UP, QKV, OUT = range(4)
(
    START,
    LOAD_MLP,
    WAIT_MLP,
    LOAD_ATTN,
    WAIT_ATTN,
    LOAD_HEAD,
    ACT,
    MLP,
    PROJECT,
    HEAD,
    PART,
    SEND,
    PAIR,
    TOTAL,
    DONE,
    FREE,
    GRAD,
    MEAN,
    FINISH,
) = range(19)


def dot(a, b, dims=PLAIN):
    return lax.dot_general(a, b, dims, preferred_element_type=F32)


def aligned(i, n=16):
    return pl.multiple_of(i, n)


class Place:
    def __init__(self):
        self.iz, self.iy, self.tp = lax.axis_index("dpy"), lax.axis_index("dpx"), lax.axis_index("tp")
        self.core = self.tp % 2
        self.other_core = self.tp + 1 - 2 * self.core
        self.other_chip = self.tp + 2 - 4 * (self.tp // 2)
        self.inner = (self.iz == 1) | (self.iz == 2)
        self.outer = jnp.logical_not(self.inner)
        self.late = self.iz // 2
        self.fold = self.iz + 1 - 2 * (self.iz % 2)
        self.mid = 3 - self.iz


def signal(sem, axis, i):
    pl.semaphore_signal(sem, inc=1, device_id={axis: i}, device_id_type=MESH)


def entry_barrier(at):
    sem = pltpu.get_barrier_semaphore()
    signal(sem, "dpx", 1 - at.iy)
    signal(sem, "dpy", at.fold)
    signal(sem, "tp", at.other_core)
    signal(sem, "tp", at.other_chip)

    @pl.when(at.inner)
    def _():
        signal(sem, "dpy", at.mid)

    pl.semaphore_wait(sem, 4 + (at.iz + 1) // 2 - 2 * (at.iz // 3))


def in_place(rows, fn):
    n = next(b for b in (64, 48, 32, 16) if rows % b == 0)

    @pl.loop(0, rows // n)
    def _(i):
        fn(aligned(i * n, n), n)


class Combine:
    def __init__(self, wide, narrow, sem):
        self.wide, self.narrow, self.sem = wide, narrow, sem
        self.rows = wide.shape[1]

    def __call__(self, fn, ins, out):
        rows, cols = out.shape
        size = -(-rows // (-(-rows // self.rows) * 32)) * 32
        pieces = [(lo, min(size, rows - lo)) for lo in range(0, rows, size)]
        loads, bufs, stores = [], [], []
        for k, (lo, n) in enumerate(pieces):
            slot = k % 2
            narrow = [self.narrow.at[slot, b, 0:n, 0:cols] for b in range(3)]
            mine = narrow.pop()
            here = [self.wide.at[slot, 0:n, 0:cols] if r.dtype == F32 else narrow.pop() for r in ins]
            part = lambda ref: ref.at[pl.ds(lo, n), :]
            loads.append([pltpu.make_async_copy(part(r), b, self.sem.at[slot, q]) for q, (r, b) in enumerate(zip(ins, here))])
            bufs.append((here, mine))
            stores.append(pltpu.make_async_copy(mine, part(out), self.sem.at[slot, 3]))
        for c in loads[0]:
            c.start()
        for k, (lo, n) in enumerate(pieces):
            if k + 1 < len(pieces):
                for c in loads[k + 1]:
                    c.start()
            for c in loads[k]:
                c.wait()
            if k >= 2:
                stores[k - 2].wait()
            here, mine = bufs[k]

            def block(i, size, here=here, mine=mine):
                at = pl.ds(i, size)
                mine[at, :] = fn(*(b[at, :].astype(F32) for b in here)).astype(BF16)

            in_place(n, block)
            stores[k].start()
        for c in stores[-2:]:
            c.wait()


class Mean:
    steps = 6

    def __init__(self, at, combine, replicas, base, rows, first, g16, g32, fin, a_bufs, b_bufs, send, recv):
        self.at, self.combine, self.scale = at, combine, 1.0 / replicas
        self.g16, self.g32, self.fin = g16, g32, fin
        self.h, self.h2 = first // 2, (rows - first) // 2
        self.base, self.first = base, base + first
        self.r0, self.r1, self.r2, self.s1 = a_bufs
        if self.h2:
            self.b0, self.b1, self.b2, self.t1, self.t2 = b_bufs
        self.send, self.recv = send, recv

    def a(self, ref, own):
        start = self.base + (self.at.iy if own else 1 - self.at.iy) * self.h
        return ref.at[pl.ds(aligned(start), self.h), :]

    def b(self, ref, own, base):
        start = base + (self.at.late if own else 1 - self.at.late) * self.h2
        return ref.at[pl.ds(aligned(start), self.h2), :]

    def copy(self, k, src, dst, axis, to):
        return pltpu.make_async_remote_copy(
            src_ref=src, dst_ref=dst, send_sem=self.send.at[k], recv_sem=self.recv.at[k], device_id={axis: to}, device_id_type=MESH
        )

    def line(self, k):
        at, fin = self.at, self.fin
        if k == 0:
            return self.copy(k, self.a(self.g16, False), self.r0, "dpx", 1 - at.iy)
        if k == 1:
            return self.copy(k, self.s1, self.r1, "dpy", at.fold)
        if k == 2:
            return self.copy(k, self.s1, self.r2, "dpy", at.mid)
        if k == 3:
            return self.copy(k, self.a(fin, True), self.a(fin, True), "dpy", at.fold)
        if k == 4:
            return self.copy(k, self.a(fin, True), self.a(fin, True), "dpx", 1 - at.iy)
        if k in (5, 6):
            return self.copy(k, self.b(self.g16, k == 6, self.first), self.b(self.b0, k == 6, 0), "dpy", at.fold)
        if k == 7:
            return self.copy(k, self.t1, self.b1, "dpy", at.mid)
        if k == 8:
            return self.copy(k, self.t2, self.b2, "dpx", 1 - at.iy)
        if k == 9:
            return self.copy(k, self.b(fin, True, self.first), self.b(fin, True, self.first), "dpy", at.mid)
        own = k == 10
        return self.copy(k, self.b(fin, own, self.first), self.b(fin, own, self.first), "dpy", at.fold)

    def landed(self, k):
        self.line(k).wait_recv()

    def step(self, n):
        at, two = self.at, bool(self.h2)
        if n == 0:
            self.line(0).start()
            if two:

                @pl.when(at.outer)
                def _():
                    self.line(5).start()
                    self.line(6).start()

        elif n == 1:
            self.landed(0)

            @pl.when(at.outer)
            def _():
                self.combine(lambda g, r: g + r, [self.a(self.g32, True), self.r0], self.s1)
                self.line(1).start()

            if two:

                @pl.when(at.inner)
                def _():
                    self.landed(5)
                    self.combine(lambda g, r: g + r, [self.b(self.g32, False, self.first), self.b(self.b0, False, 0)], self.t1)
                    self.line(7).start()

        elif n == 2:

            @pl.when(at.inner)
            def _():
                self.landed(1)
                self.combine(lambda g, r, q: g + r + q, [self.a(self.g32, True), self.r0, self.r1], self.s1)
                self.line(2).start()
                if two:
                    self.landed(6)
                    self.landed(7)
                    own = [self.b(self.g32, True, self.first), self.b(self.b0, True, 0), self.b1]
                    self.combine(lambda g, r, q: g + r + q, own, self.t2)
                    self.line(8).start()

        elif n == 3:

            @pl.when(at.inner)
            def _():
                self.landed(2)
                self.combine(lambda s, r: (s + r) * self.scale, [self.s1, self.r2], self.a(self.fin, True))
                self.line(3).start()
                self.line(4).start()
                if two:
                    self.landed(8)
                    self.combine(lambda s, r: (s + r) * self.scale, [self.t2, self.b2], self.b(self.fin, True, self.first))
                    self.line(9).start()
                    self.line(10).start()

        elif n == 4:

            @pl.when(at.outer)
            def _():
                self.landed(3)
                self.line(4).start()

            if two:

                @pl.when(at.inner)
                def _():
                    self.landed(9)
                    self.line(11).start()

        else:
            self.landed(4)
            self.line(0).wait_send()
            self.line(4).wait_send()

            @pl.when(at.outer)
            def _():
                self.line(1).wait_send()
                if two:
                    self.landed(10)
                    self.landed(11)
                    self.line(5).wait_send()
                    self.line(6).wait_send()

            @pl.when(at.inner)
            def _():
                self.line(2).wait_send()
                self.line(3).wait_send()
                if two:
                    for k in (7, 8, 9, 10, 11):
                        self.line(k).wait_send()


class Backward:
    def __init__(self, dims, refs):
        self.__dict__.update(dims)
        self.at = Place()
        self.early = {entry[1] for entry in ORDER if entry[0] == ACT}
        refs = list(refs)
        for name in self.names[0]:
            setattr(self, name, refs.pop(0))
        self.fins = [refs.pop(0) for _ in KINDS]
        self.tensors = [refs.pop(0) for _ in range(self.count)]
        for name, ref in zip(self.names[1], refs, strict=True):
            setattr(self, name, ref)
        self.half = self.s // 2
        self.blk = min(256, self.half)
        self.means, self.grads = {}, {}
        tensors, i = list(self.tensors), 0
        combine = Combine(self.wide, self.narrow, self.combine_sem)
        for l in range(self.layers):
            for kind in KINDS:
                g16, g32 = tensors.pop(0), tensors.pop(0)
                self.grads[kind, l], base = (g16, g32), 0
                for p, (rows, first) in enumerate(CUTS[l][kind]):
                    a = tensors.pop(0)
                    a_bufs, b_bufs = [a.at[j] for j in range(4)], None
                    if rows > first:
                        b0, b = tensors.pop(0), tensors.pop(0)
                        b_bufs = [b0] + [b.at[j] for j in range(4)]
                    sems = self.dp_send.at[i], self.dp_recv.at[i]
                    self.means[kind, l, p] = Mean(self.at, combine, self.replicas, base, rows, first, g16, g32, self.fins[kind].at[l], a_bufs, b_bufs, *sems)
                    base += rows
                    i += 1

    def local(self, k, src, dst):
        return pltpu.make_async_copy(src, dst, self.local_sem.at[k])

    def mlp_weights(self, l):
        return [self.local(0, self.w_up.at[l], self.wu_v), self.local(1, self.w_down.at[l], self.wd_v)]

    def attn_weights(self, l):
        d, heads = self.hd // self.heads, self.heads
        cols = [self.local(4 + c * heads + n, self.w_qkv.at[l, c, n], self.wq_v.at[:, pl.ds((c * heads + n) * d, d)]) for c in range(3) for n in range(heads)]
        rows = [self.local(4 + 3 * heads + n, self.w_out.at[l, n], self.wo_v.at[pl.ds(n * d, d), :]) for n in range(heads)]
        return cols + rows

    def top_grad(self, m):
        return self.local(2 + m, self.d_out.at[m], self.res.at[pl.ds(m * self.s, self.s), :])

    def act_only(self, l, m):
        blk, cols = self.blk, min(512, self.f)

        def body(y_ref, a_ref):
            y = y_ref[...]
            for c in range(self.f // cols):
                sl = slice(c * cols, (c + 1) * cols)
                h = dot(y, self.wu_v[:, sl])
                t = jnp.tanh(h * (TANH_1 + TANH_3 * (h * h)))
                a_ref[:, sl] = (h * (0.5 * t + 0.5)).astype(BF16)

        row = lambda width: pl.BlockSpec((blk, width), lambda i: (i, 0))
        pltpu.emit_pipeline(body, grid=(self.s // blk,), in_specs=[row(self.w)], out_specs=[row(self.f)])(
            self.y_saved.at[l, m], self.act.at[pl.ds(m * self.s, self.s), :]
        )

    def mlp(self, l, m, own):
        half, blk, cols = self.half, self.blk, min(512, self.f)
        start = (self.at.core if own else 1 - self.at.core) * half
        part = (self.own if own else self.part).at[m]

        def body(step, y_ref, *a_ref):
            i = step.index[0]
            rows = pl.ds(aligned(m * self.s + start + i * blk, blk), blk)
            y, g = y_ref[...], self.res[rows, :]
            for c in range(self.f // cols):
                sl = slice(c * cols, (c + 1) * cols)
                h = dot(y, self.wu_v[:, sl])
                da = dot(g, self.wd_v[sl, :], LANES)
                h2 = h * h
                t = jnp.tanh(h * (TANH_1 + TANH_3 * h2))
                cdf = 0.5 * t + 0.5
                slope = cdf + (0.5 * h) * (1.0 - t * t) * (TANH_1 + (3.0 * TANH_3) * h2)
                for a in a_ref:
                    a[:, sl] = (h * cdf).astype(BF16)
                self.dh_v[rows, sl] = (da * slope).astype(BF16)
            dh = self.dh_v[rows, :]
            wcols = min(512, self.w)
            for c in range(self.w // wcols):
                sl = slice(c * wcols, (c + 1) * wcols)
                part[pl.ds(aligned(i * blk, blk), blk), sl] = dot(dh, self.wu_v[sl, :], LANES).astype(BF16)

        row = lambda width: pl.BlockSpec((blk, width), lambda i: (i, 0))
        outs = [] if l in self.early else [self.act.at[pl.ds(aligned(m * self.s + start, blk), half), :]]
        pltpu.emit_pipeline(body, grid=(half // blk,), in_specs=[row(self.w)], out_specs=[row(self.f)] * len(outs), _explicit_indices=True)(
            self.y_saved.at[l, m, pl.ds(aligned(start, blk), half), :], *outs
        )

    def qkv(self, l, m):
        blk, cols = self.blk, min(384, 3 * self.hd)

        def body(x_ref, out_ref):
            x = x_ref[...]
            for c in range(3 * self.hd // cols):
                sl = slice(c * cols, (c + 1) * cols)
                out_ref[:, sl] = dot(x, self.wq_v[:, sl]).astype(BF16)

        row = lambda width: pl.BlockSpec((blk, width), lambda i: (i, 0))
        pltpu.emit_pipeline(body, grid=(self.s // blk,), in_specs=[row(self.w)], out_specs=[row(3 * self.hd)])(
            self.x_saved.at[l, m], self.qkv_hbm.at[pl.ds(m * self.s, self.s), :]
        )

    def head_loads(self, m, n):
        d = self.hd // self.heads
        slot = (m * self.heads + n) % 2
        base = 4 + 4 * self.heads + 3 * slot
        return [
            self.local(base + c, self.qkv_hbm.at[pl.ds(m * self.s, self.s), pl.ds((c * self.heads + n) * d, d)], self.head.at[slot, c])
            for c in range(3)
        ]

    def attn(self, l, m, n):
        s, d, blk = self.s, self.hd // self.heads, min(256, self.s)
        scale = d**-0.5
        slot = (m * self.heads + n) % 2
        for c in self.head_loads(m, n):
            c.wait()
        if n + 1 < self.heads:
            for c in self.head_loads(m, n + 1):
                c.start()
        mine = slice(m * s, (m + 1) * s)
        col = slice(n * d, (n + 1) * d)
        q_ref, k_ref, v_ref = (self.head.at[slot, c] for c in range(3))
        p_ref, ds_ref = self.dh_v.at[0:s, 0:s], self.dh_v.at[s : 2 * s, 0:s]
        do_ref = self.do_v
        do_ref[...] = dot(self.res[mine, :], self.wo_v[col, :], LANES).astype(BF16)
        keys, vals = k_ref[...], v_ref[...]
        keys_t, vals_t = keys.T, vals.T
        place = lambda c: slice((c * self.heads + n) * d, (c * self.heads + n + 1) * d)
        block = lambda i: slice(i * blk, (i + 1) * blk)
        scores = lambda i: (dot(keys, q_ref[block(i), :], LANES), dot(vals, do_ref[block(i), :], LANES))
        ahead = scores(0)
        for i in range(s // blk):
            sc, dp = ahead
            if i + 1 < s // blk:
                ahead = scores(i + 1)
            sl = block(i)
            out = slice(m * s + i * blk, m * s + (i + 1) * blk)
            top = jnp.max(sc, axis=0, keepdims=True)
            e = jnp.exp((sc - top) * scale)
            inv = 1.0 / jnp.sum(e, axis=0, keepdims=True)
            row_dot = jnp.sum(dp * e, axis=0, keepdims=True) * inv
            pb = (e * inv).astype(BF16)
            ds = (e * ((dp - row_dot) * (inv * scale))).astype(BF16)
            p_ref[:, sl] = pb
            ds_ref[:, sl] = ds
            self.o_v[out, col] = dot(vals_t, pb).T.astype(BF16)
            self.dqkv_v[out, place(0)] = dot(keys_t, ds).T.astype(BF16)
        self.dqkv_v[mine, place(1)] = dot(ds_ref[...], q_ref[...]).astype(BF16)
        self.dqkv_v[mine, place(2)] = dot(p_ref[...], do_ref[...]).astype(BF16)

    def attn_part(self, l, m, own):
        half, cols = self.half, min(512, self.w)
        start = (self.at.core if own else 1 - self.at.core) * half
        part = (self.own if own else self.part).at[m]

        @pl.loop(0, half // self.blk)
        def _(i):
            dqkv = self.dqkv_v[pl.ds(aligned(m * self.s + start + i * self.blk, self.blk), self.blk), :]
            for c in range(self.w // cols):
                sl = slice(c * cols, (c + 1) * cols)
                part[pl.ds(aligned(i * self.blk, self.blk), self.blk), sl] = dot(dqkv, self.wq_v[sl, :], LANES).astype(BF16)

    def tp_copy(self, k, m, src, dst, to):
        return pltpu.make_async_remote_copy(
            src_ref=src, dst_ref=dst, send_sem=self.tp_send.at[k, m], recv_sem=self.tp_recv.at[k, m], device_id={"tp": to}, device_id_type=MESH
        )

    def tp_line(self, k, m):
        at = self.at
        if k == 0:
            return self.tp_copy(0, m, self.part.at[m], self.from_core.at[m], at.other_core)
        if k == 1:
            return self.tp_copy(1, m, self.own.at[m], self.from_chip.at[m], at.other_chip)
        rows = self.res.at[pl.ds(aligned(m * self.s + at.core * self.half), self.half), :]
        return self.tp_copy(2, m, rows, rows, at.other_core)

    def tp_pair(self, m, first):
        line = self.tp_line(0, m)
        line.wait_recv()
        own, got = self.own.at[m], self.from_core.at[m]

        def add(i, n):
            r = pl.ds(i, n)
            own[r, :] = (own[r, :].astype(F32) + got[r, :].astype(F32)).astype(BF16)

        in_place(self.half, add)
        line.wait_send()
        if not first:
            pl.semaphore_wait(self.chip_free.at[m], 1)
        self.tp_line(1, m).start()

    def tp_total(self, m, last, credit):
        line = self.tp_line(1, m)
        line.wait_recv()
        own, got = self.own.at[m], self.from_chip.at[m]
        base = m * self.s + self.at.core * self.half

        def add(i, n):
            r, b = pl.ds(i, n), pl.ds(aligned(base + i, n), n)
            self.res[b, :] = (self.res[b, :].astype(F32) + (own[r, :].astype(F32) + got[r, :].astype(F32))).astype(BF16)

        in_place(self.half, add)
        line.wait_send()
        if not last:
            signal(self.chip_free.at[m], "tp", self.at.other_chip)
        if credit:
            pl.semaphore_wait(self.core_free, 1)
        self.tp_line(2, m).start()

    def tp_done(self, m):
        line = self.tp_line(2, m)
        line.wait_recv()
        line.wait_send()

    def release_rows(self):
        signal(self.core_free, "tp", self.at.other_core)

    def grad(self, kind, l, part):
        rhs = (self.res, self.dh_v, self.dqkv_v, self.res)[kind]
        g16, g32 = self.grads[kind, l]
        cols = g32.shape[1]
        sizes = [rows for rows, _ in CUTS[l][kind]]
        lo, rows = sum(sizes[:part]), sizes[part]
        hi = lo + rows
        tile = next(t for t in (256, 384, 128) if rows % t == 0)
        chunk = min(512 if cols % 512 == 0 else 384, cols)
        two = self.mbs * self.s

        def put(lhs, o16_ref, o32_ref):
            for c in range(cols // chunk):
                sl = slice(c * chunk, (c + 1) * chunk)
                v = dot(lhs, rhs[:, sl], ROWS)
                o32_ref[:, sl] = v
                o16_ref[:, sl] = v.astype(BF16)

        out = pl.BlockSpec((tile, cols), lambda j: (j, 0))
        dst = (g16.at[lo:hi, :], g32.at[lo:hi, :])
        grid = ((hi - lo) // tile,)
        if kind == OUT:

            def body(step, *outs):
                put(self.o_v[:, pl.ds(aligned(lo + step.index[0] * tile, tile), tile)], *outs)

            pltpu.emit_pipeline(body, grid=grid, in_specs=[], out_specs=[out, out], _explicit_indices=True)(*dst)
            return
        if kind == DOWN:
            src, spec = self.act.at[:, lo:hi], pl.BlockSpec((two, tile), lambda j: (0, j))
        else:
            src = (self.y_saved if kind == UP else self.x_saved).at[l, :, :, lo:hi]
            spec = pl.BlockSpec((self.mbs, self.s, tile), lambda j: (0, 0, j))

        def body(lhs_ref, *outs):
            put(lhs_ref[...].reshape(two, tile), *outs)

        pltpu.emit_pipeline(body, grid=grid, in_specs=[spec], out_specs=[out, out])(src, *dst)


def run(b, order):
    for what, *rest in order:
        if what == START:
            up, down = b.mlp_weights(b.layers - 1)
            up.start()
            entry_barrier(b.at)
            up.wait()
            for c in [b.top_grad(m) for m in range(b.mbs)] + [down] + b.attn_weights(b.layers - 1):
                c.start()
            waiting = [b.top_grad(m) for m in range(b.mbs)]
        elif what in (LOAD_MLP, LOAD_ATTN, LOAD_HEAD):
            for c in {LOAD_MLP: b.mlp_weights, LOAD_ATTN: b.attn_weights, LOAD_HEAD: b.head_loads}[what](*rest):
                c.start()
        elif what == WAIT_MLP:
            up, down = b.mlp_weights(*rest)
            if rest[0] < b.layers - 1:
                up.wait()
            down.wait()
        elif what == WAIT_ATTN:
            for c in b.attn_weights(*rest):
                c.wait()
        elif what == SEND:
            b.tp_line(0, rest[0]).start()
        elif what == MEAN:
            *which, n = rest
            b.means[tuple(which)].step(n)
        elif what == FINISH:
            out = [b.local(2 + m, b.res.at[pl.ds(m * b.s, b.s), :], b.d_in.at[m]) for m in range(b.mbs)]
            for c in out:
                c.start()
            for c in out:
                c.wait()
        else:
            if what in (MLP, GRAD):
                while waiting:
                    waiting.pop().wait()
            part = {
                ACT: b.act_only,
                MLP: b.mlp,
                PROJECT: b.qkv,
                HEAD: b.attn,
                PART: b.attn_part,
                PAIR: b.tp_pair,
                TOTAL: b.tp_total,
                DONE: b.tp_done,
                FREE: b.release_rows,
                GRAD: b.grad,
            }[what]
            part(*rest)


def mega_kernel(dims, order, *refs):
    run(Backward(dims, refs), order)


def backward(x_saved, y_saved, d_out, w_qkv, w_out, w_up, w_down, replicas):
    layers, mbs, s, w = x_saved.shape
    f, heads, d = w_up.shape[2], w_qkv.shape[2], w_qkv.shape[4]
    hd, rows = heads * d, mbs * s
    half = s // 2
    shapes = (f, w), (w, f), (w, 3 * hd), (hd, w)
    hbm = {"d_in": (mbs, s, w), "act": (rows, f), "qkv_hbm": (rows, 3 * hd)}
    fins = [(layers, *shape) for shape in shapes]
    tensors = []
    for l in range(layers):
        for (r, c), cuts in zip(shapes, CUTS[l], strict=True):
            tensors += [((r, c), BF16), ((r, c), F32)]
            for n, first in cuts:
                tensors += [((4, first // 2, c), BF16)]
                if n > first:
                    tensors += [((n - first, c), BF16), ((4, (n - first) // 2, c), BF16)]
    vmem = {
        "wu_v": (w, f),
        "wd_v": (f, w),
        "wq_v": (w, 3 * hd),
        "wo_v": (hd, w),
        "res": (rows, w),
        "dh_v": (rows, f),
        "dqkv_v": (rows, 3 * hd),
        "o_v": (rows, hd),
        "part": (mbs, half, w),
        "own": (mbs, half, w),
        "from_core": (mbs, half, w),
        "from_chip": (mbs, half, w),
        "head": (2, 3, s, d),
        "do_v": (s, d),
        "narrow": (2, 3, min(BLOCK, w // 2), w),
    }
    n = sum(len(cuts) for layer in CUTS for cuts in layer)
    dma, regular = pltpu.SemaphoreType.DMA, pltpu.SemaphoreType.REGULAR
    sems = {
        "dp_send": dma((n, 12)),
        "dp_recv": dma((n, 12)),
        "tp_send": dma((3, mbs)),
        "tp_recv": dma((3, mbs)),
        "local_sem": dma((4 + 4 * heads + 6,)),
        "chip_free": regular((mbs,)),
        "core_free": regular,
        "combine_sem": dma((2, 4)),
        "wide": pltpu.VMEM((2, min(BLOCK, w // 2), w), F32),
    }
    ins = ("x_saved", "y_saved", "d_out", "w_qkv", "w_out", "w_up", "w_down")
    names = ((*ins, *hbm), (*vmem, *sems))
    dims = dict(names=names, count=len(tensors), layers=layers, mbs=mbs, s=s, w=w, f=f, heads=heads, hd=hd, replicas=replicas)
    outs = [(v, BF16) for v in (*hbm.values(), *fins)] + tensors
    outs = pl.pallas_call(
        functools.partial(mega_kernel, dims, ORDER),
        in_specs=[ANY] * len(ins),
        out_specs=[ANY] * len(outs),
        out_shape=[jax.ShapeDtypeStruct(*v) for v in outs],
        scratch_shapes=[pltpu.VMEM(v, BF16) for v in vmem.values()] + list(sems.values()),
        compiler_params=pltpu.CompilerParams(collective_id=0, has_side_effects=True, vmem_limit_bytes=67043328),
        name="backward",
    )(x_saved, y_saved, d_out, w_qkv, w_out, w_up, w_down)
    return outs[0], *outs[len(hbm) : len(hbm) + len(fins)]


def finish_kernel(jobs, *refs):
    n = len({job[0] for job in jobs})
    ins, outs = refs[:n], refs[n : 2 * n]
    narrow, wide, in_sem, out_sem = refs[2 * n :]
    depth = narrow.shape[0]

    def load(k):
        which, l, lo, rows, _ = jobs[k]
        src = ins[which].at[l, pl.ds(lo, rows), :]
        return pltpu.make_async_copy(src, narrow.at[k % depth, 0:rows, 0 : src.shape[1]], in_sem.at[k % depth])

    def store(k):
        which, l, lo, rows, pieces = jobs[k]
        cols = ins[which].shape[2]
        if pieces:
            src, dst = wide.at[k % depth, 0:rows, 0:cols], outs[which]
            width = cols // pieces
            return [
                pltpu.make_async_copy(src.at[:, pl.ds(p * width, width)], dst.at[l, p, pl.ds(lo, rows), :], out_sem.at[k % depth, p])
                for p in range(pieces)
            ]
        return [pltpu.make_async_copy(narrow.at[k % depth, 0:rows, 0:cols], outs[which].at[l, pl.ds(lo, rows), :], out_sem.at[k % depth, 0])]

    ahead = depth // 2
    for k in range(ahead):
        load(k).start()
    for k, (which, l, lo, rows, pieces) in enumerate(jobs):
        if k + ahead < len(jobs):
            if k + ahead >= depth:
                for c in store(k + ahead - depth):
                    c.wait()
            load(k + ahead).start()
        load(k).wait()
        if pieces:
            src, dst = narrow.at[k % depth], wide.at[k % depth]
            cols = ins[which].shape[2]

            def block(i, size):
                dst[pl.ds(i, size), 0:cols] = src[pl.ds(i, size), 0:cols].astype(F32)

            in_place(rows, block)
        for c in store(k):
            c.start()
    for k in range(len(jobs) - depth, len(jobs)):
        for c in store(k):
            c.wait()


def finish(d_in, fins, heads):
    ins = (d_in, *fins)
    pieces = (0, 1, 1, 3 * heads, 1)
    jobs = []
    for which, a in enumerate(ins):
        layers, r, c = a.shape
        blk = next(b for b in (256, 192, 128) if r % b == 0)
        jobs += [(which, l, lo, blk, pieces[which]) for l in range(layers) for lo in range(0, r, blk)]
    out = lambda a, p: jax.ShapeDtypeStruct(a.shape if not p else (a.shape[0], p, a.shape[1], a.shape[2] // p), F32 if p else BF16)
    depth, width = 6, max(a.shape[2] for a in ins)
    return pl.pallas_call(
        functools.partial(finish_kernel, jobs),
        in_specs=[ANY] * len(ins),
        out_specs=[ANY] * len(ins),
        out_shape=[out(a, p) for a, p in zip(ins, pieces)],
        scratch_shapes=[
            pltpu.VMEM((depth, 256, width), BF16),
            pltpu.VMEM((depth, 256, width), F32),
            pltpu.SemaphoreType.DMA((depth,)),
            pltpu.SemaphoreType.DMA((depth, 3 * heads)),
        ],
        name="finish",
    )(*ins)


CUTS = (
    (((1024, 384), (512, 224)), ((896, 896), (640, 640)), ((1024, 640), (512, 384)), ((384, 384),)),
    (((1536, 800),), ((1536, 992),), ((1536, 416),), ((384, 384),)),
)
ORDER = (
    (START,), (ACT, 1, 1), (ACT, 1, 0), (GRAD, DOWN, 1, 0), (FREE,), (MEAN, DOWN, 1, 0, 0), (WAIT_MLP, 1), (MLP, 1, 0, False), (SEND, 0),
    (MLP, 1, 0, True), (PAIR, 0, True), (MLP, 1, 1, False), (SEND, 1), (MLP, 1, 1, True), (MEAN, DOWN, 1, 0, 1), (GRAD, UP, 1, 0),
    (MEAN, UP, 1, 0, 0), (WAIT_ATTN, 1), (PROJECT, 1, 0), (TOTAL, 0, False, True), (PAIR, 1, True), (PROJECT, 1, 1), (DONE, 0),
    (LOAD_HEAD, 0, 0), (HEAD, 1, 0, 0), (MEAN, DOWN, 1, 0, 2), (HEAD, 1, 0, 1), (HEAD, 1, 0, 2), (PART, 1, 0, False), (SEND, 0),
    (TOTAL, 1, False, False), (MEAN, UP, 1, 0, 1), (PART, 1, 0, True), (PAIR, 0, False), (MEAN, DOWN, 1, 0, 3), (DONE, 1), (LOAD_HEAD, 1, 0),
    (HEAD, 1, 1, 0), (HEAD, 1, 1, 1), (HEAD, 1, 1, 2), (MEAN, UP, 1, 0, 2), (GRAD, OUT, 1, 0), (FREE,), (GRAD, QKV, 1, 0),
    (MEAN, QKV, 1, 0, 0), (PART, 1, 1, False), (SEND, 1), (TOTAL, 0, False, True), (MEAN, DOWN, 1, 0, 4), (PART, 1, 1, True), (LOAD_ATTN, 0),
    (PAIR, 1, False), (MEAN, OUT, 1, 0, 0), (LOAD_MLP, 0), (DONE, 0), (WAIT_MLP, 0), (MLP, 0, 0, False), (SEND, 0), (MEAN, QKV, 1, 0, 1),
    (MEAN, UP, 1, 0, 3), (MLP, 0, 0, True), (WAIT_ATTN, 0), (PROJECT, 0, 0), (TOTAL, 1, False, False), (PAIR, 0, False), (MEAN, QKV, 1, 0, 2),
    (MEAN, OUT, 1, 0, 1), (DONE, 1), (MLP, 0, 1, False), (SEND, 1), (MLP, 0, 1, True), (MEAN, UP, 1, 0, 4), (GRAD, DOWN, 0, 0),
    (MEAN, DOWN, 0, 0, 0), (MEAN, QKV, 1, 0, 3), (GRAD, DOWN, 0, 1), (FREE,), (TOTAL, 0, False, True), (PAIR, 1, False), (GRAD, UP, 0, 0),
    (MEAN, UP, 0, 0, 0), (MEAN, DOWN, 0, 0, 1), (MEAN, OUT, 1, 0, 2), (MEAN, DOWN, 0, 1, 0), (DONE, 0), (PROJECT, 0, 1), (GRAD, UP, 0, 1),
    (MEAN, QKV, 1, 0, 4), (LOAD_HEAD, 0, 0), (HEAD, 0, 0, 0), (TOTAL, 1, False, False), (MEAN, DOWN, 0, 0, 2), (HEAD, 0, 0, 1),
    (MEAN, UP, 0, 1, 0), (MEAN, DOWN, 0, 1, 1), (MEAN, OUT, 1, 0, 3), (MEAN, UP, 0, 0, 1), (HEAD, 0, 0, 2), (MEAN, DOWN, 0, 0, 3), (DONE, 1),
    (LOAD_HEAD, 1, 0), (HEAD, 0, 1, 0), (MEAN, DOWN, 0, 1, 2), (HEAD, 0, 1, 1), (MEAN, UP, 0, 1, 1), (MEAN, UP, 0, 0, 2),
    (MEAN, DOWN, 0, 0, 4), (PART, 0, 0, False), (SEND, 0), (HEAD, 0, 1, 2), (GRAD, OUT, 0, 0), (FREE,), (MEAN, OUT, 0, 0, 0),
    (MEAN, DOWN, 0, 1, 3), (GRAD, QKV, 0, 0), (MEAN, UP, 0, 1, 2), (MEAN, OUT, 0, 0, 1), (MEAN, DOWN, 1, 0, 5), (MEAN, QKV, 0, 0, 0),
    (MEAN, UP, 0, 0, 3), (MEAN, DOWN, 0, 1, 4), (MEAN, OUT, 1, 0, 4), (GRAD, QKV, 0, 1), (PART, 0, 0, True), (PAIR, 0, False),
    (MEAN, DOWN, 0, 0, 5), (MEAN, QKV, 0, 1, 0), (PART, 0, 1, False), (SEND, 1), (MEAN, QKV, 0, 0, 1), (PART, 0, 1, True), (PAIR, 1, False),
    (MEAN, OUT, 1, 0, 5), (MEAN, OUT, 0, 0, 2), (MEAN, UP, 0, 1, 3), (MEAN, UP, 0, 0, 4), (MEAN, QKV, 0, 0, 2), (MEAN, OUT, 0, 0, 3),
    (MEAN, QKV, 0, 1, 1), (MEAN, UP, 0, 1, 4), (MEAN, QKV, 0, 1, 2), (MEAN, OUT, 0, 0, 4), (MEAN, QKV, 0, 0, 3), (MEAN, QKV, 0, 1, 3),
    (TOTAL, 0, True, True), (MEAN, UP, 0, 1, 5), (MEAN, QKV, 0, 0, 4), (TOTAL, 1, True, False), (MEAN, QKV, 0, 1, 4), (DONE, 1),
    (MEAN, OUT, 0, 0, 5), (DONE, 0), (MEAN, UP, 0, 0, 5), (MEAN, UP, 1, 0, 5), (FINISH,), (MEAN, QKV, 0, 0, 5), (MEAN, QKV, 1, 0, 5),
    (MEAN, DOWN, 0, 1, 5), (MEAN, QKV, 0, 1, 5),
)


def solution(mesh):
    replicas = mesh.shape["dpy"] * mesh.shape["dpx"]
    data_axes = ("dpy", "dpx")
    act_spec = P(None, data_axes, None, None)
    tok_spec = P(data_axes, None, None)
    qkv_spec = P(None, None, None, "tp", None)
    wout_spec = P(None, "tp", None, None)
    up_spec = P(None, None, "tp")
    down_spec = P(None, "tp", None)

    def device_backward(x_saved, y_saved, d_out, w_qkv, w_out, w_up, w_down):
        layers, width, _, heads, d = w_qkv.shape
        by_head = jnp.transpose(w_qkv, (0, 2, 3, 1, 4))
        d_in, *fins = backward(x_saved, y_saved, d_out, by_head, w_out, w_up, w_down, replicas)
        d_in, down, up, qkv, out = finish(d_in, fins, heads)
        g_qkv = jnp.transpose(qkv.reshape(layers, 3, heads, width, d), (0, 3, 1, 2, 4))
        return d_in, g_qkv, out.reshape(w_out.shape), up.reshape(w_up.shape), down.reshape(w_down.shape)

    return jax.shard_map(
        device_backward,
        mesh=mesh,
        in_specs=(act_spec, act_spec, tok_spec, qkv_spec, wout_spec, up_spec, down_spec),
        out_specs=(tok_spec, qkv_spec, wout_spec, up_spec, down_spec),
        check_vma=False,
    )
```

```python
import functools

import jax
import jax.numpy as jnp
from jax import lax
from jax.experimental import pallas as pl
from jax.experimental.pallas import tpu as pltpu
from jax.sharding import PartitionSpec as P

F32, BF16 = jnp.float32, jnp.bfloat16
PLAIN = (((1,), (0,)), ((), ()))
BLOCK = 128
LANES = (((1,), (1,)), ((), ()))
ROWS = (((0,), (0,)), ((), ()))
ANY = pl.BlockSpec(memory_space=pl.ANY)
MESH = pl.DeviceIdType.MESH
TANH_1 = 0.7978845608028654
TANH_3 = 0.044715 * TANH_1
KINDS = DOWN, UP, QKV, OUT = range(4)
(
    START,
    LOAD_MLP,
    WAIT_MLP,
    LOAD_ATTN,
    WAIT_ATTN,
    LOAD_HEAD,
    ACT,
    MLP,
    PROJECT,
    HEAD,
    PART,
    SEND,
    PAIR,
    TOTAL,
    DONE,
    FREE,
    GRAD,
    MEAN,
    FINISH,
) = range(19)


def dot(a, b, dims=PLAIN):
    return lax.dot_general(a, b, dims, preferred_element_type=F32)


def aligned(i, n=16):
    return pl.multiple_of(i, n)


class Place:
    def __init__(self):
        self.iz, self.iy, self.tp = lax.axis_index("dpy"), lax.axis_index("dpx"), lax.axis_index("tp")
        self.core = self.tp % 2
        self.other_core = self.tp + 1 - 2 * self.core
        self.other_chip = self.tp + 2 - 4 * (self.tp // 2)
        self.inner = (self.iz == 1) | (self.iz == 2)
        self.outer = jnp.logical_not(self.inner)
        self.late = self.iz // 2
        self.fold = self.iz + 1 - 2 * (self.iz % 2)
        self.mid = 3 - self.iz


def signal(sem, axis, i):
    pl.semaphore_signal(sem, inc=1, device_id={axis: i}, device_id_type=MESH)


def entry_barrier(at):
    sem = pltpu.get_barrier_semaphore()
    signal(sem, "dpx", 1 - at.iy)
    signal(sem, "dpy", at.fold)
    signal(sem, "tp", at.other_core)
    signal(sem, "tp", at.other_chip)

    @pl.when(at.inner)
    def _():
        signal(sem, "dpy", at.mid)

    pl.semaphore_wait(sem, 4 + (at.iz + 1) // 2 - 2 * (at.iz // 3))


def in_place(rows, fn):
    n = next(b for b in (64, 48, 32, 16) if rows % b == 0)

    @pl.loop(0, rows // n)
    def _(i):
        fn(aligned(i * n, n), n)


class Combine:
    def __init__(self, wide, narrow, sem):
        self.wide, self.narrow, self.sem = wide, narrow, sem
        self.rows = wide.shape[1]

    def __call__(self, fn, ins, out, ready, early=1):
        rows, cols = out.shape
        size = -(-rows // (-(-rows // self.rows) * 32)) * 32
        pieces = [(lo, min(size, rows - lo)) for lo in range(0, rows, size)]
        loads, bufs, stores = [], [], []
        for k, (lo, n) in enumerate(pieces):
            slot = k % 2
            narrow = [self.narrow.at[slot, b, 0:n, 0:cols] for b in range(3)]
            mine = narrow.pop()
            here = [self.wide.at[slot, 0:n, 0:cols] if r.dtype == F32 else narrow.pop() for r in ins]
            part = lambda ref: ref.at[pl.ds(lo, n), :]
            loads.append([pltpu.make_async_copy(part(r), b, self.sem.at[slot, q]) for q, (r, b) in enumerate(zip(ins, here))])
            bufs.append((here, mine))
            stores.append(pltpu.make_async_copy(mine, part(out), self.sem.at[slot, 3]))
        for c in loads[0][:early]:
            c.start()
        ready()
        for c in loads[0][early:]:
            c.start()
        for k, (lo, n) in enumerate(pieces):
            if k + 1 < len(pieces):
                for c in loads[k + 1]:
                    c.start()
            for c in loads[k]:
                c.wait()
            if k >= 2:
                stores[k - 2].wait()
            here, mine = bufs[k]

            def block(i, size, here=here, mine=mine):
                at = pl.ds(i, size)
                mine[at, :] = fn(*(b[at, :].astype(F32) for b in here)).astype(BF16)

            in_place(n, block)
            stores[k].start()
        for c in stores[-2:]:
            c.wait()


class Mean:
    steps = 6

    def __init__(self, at, combine, replicas, base, rows, first, g16, g32, fin, a_bufs, b_bufs, send, recv):
        self.at, self.combine, self.scale = at, combine, 1.0 / replicas
        self.g16, self.g32, self.fin = g16, g32, fin
        self.h, self.h2 = first // 2, (rows - first) // 2
        self.base, self.first = base, base + first
        self.r0, self.r1, self.r2, self.s1 = a_bufs
        if self.h2:
            self.b0, self.b1, self.b2, self.t1, self.t2 = b_bufs
        self.send, self.recv = send, recv

    def a(self, ref, own):
        start = self.base + (self.at.iy if own else 1 - self.at.iy) * self.h
        return ref.at[pl.ds(aligned(start), self.h), :]

    def b(self, ref, own, base):
        start = base + (self.at.late if own else 1 - self.at.late) * self.h2
        return ref.at[pl.ds(aligned(start), self.h2), :]

    def copy(self, k, src, dst, axis, to):
        return pltpu.make_async_remote_copy(
            src_ref=src, dst_ref=dst, send_sem=self.send.at[k], recv_sem=self.recv.at[k], device_id={axis: to}, device_id_type=MESH
        )

    def line(self, k):
        at, fin = self.at, self.fin
        if k == 0:
            return self.copy(k, self.a(self.g16, False), self.r0, "dpx", 1 - at.iy)
        if k == 1:
            return self.copy(k, self.s1, self.r1, "dpy", at.fold)
        if k == 2:
            return self.copy(k, self.s1, self.r2, "dpy", at.mid)
        if k == 3:
            return self.copy(k, self.a(fin, True), self.a(fin, True), "dpy", at.fold)
        if k == 4:
            return self.copy(k, self.a(fin, True), self.a(fin, True), "dpx", 1 - at.iy)
        if k in (5, 6):
            return self.copy(k, self.b(self.g16, k == 6, self.first), self.b(self.b0, k == 6, 0), "dpy", at.fold)
        if k == 7:
            return self.copy(k, self.t1, self.b1, "dpy", at.mid)
        if k == 8:
            return self.copy(k, self.t2, self.b2, "dpx", 1 - at.iy)
        if k == 9:
            return self.copy(k, self.b(fin, True, self.first), self.b(fin, True, self.first), "dpy", at.mid)
        own = k == 10
        return self.copy(k, self.b(fin, own, self.first), self.b(fin, own, self.first), "dpy", at.fold)

    def landed(self, k):
        self.line(k).wait_recv()

    def step(self, n):
        at, two = self.at, bool(self.h2)
        if n == 0:
            self.line(0).start()
            if two:

                @pl.when(at.outer)
                def _():
                    self.line(5).start()
                    self.line(6).start()

        elif n == 1:

            @pl.when(at.outer)
            def _():
                self.combine(lambda g, r: g + r, [self.a(self.g32, True), self.r0], self.s1, lambda: self.landed(0))
                self.line(1).start()

            @pl.when(at.inner)
            def _():
                self.landed(0)
                if two:
                    other = [self.b(self.g32, False, self.first), self.b(self.b0, False, 0)]
                    self.combine(lambda g, r: g + r, other, self.t1, lambda: self.landed(5))
                    self.line(7).start()

        elif n == 2:

            @pl.when(at.inner)
            def _():
                self.combine(lambda g, r, q: g + r + q, [self.a(self.g32, True), self.r0, self.r1], self.s1, lambda: self.landed(1), 2)
                self.line(2).start()
                if two:

                    def folded():
                        self.landed(6)
                        self.landed(7)

                    own = [self.b(self.g32, True, self.first), self.b(self.b0, True, 0), self.b1]
                    self.combine(lambda g, r, q: g + r + q, own, self.t2, folded)
                    self.line(8).start()

        elif n == 3:

            @pl.when(at.inner)
            def _():
                self.combine(lambda s, r: (s + r) * self.scale, [self.s1, self.r2], self.a(self.fin, True), lambda: self.landed(2))
                self.line(3).start()
                self.line(4).start()
                if two:
                    total = self.b(self.fin, True, self.first)
                    self.combine(lambda s, r: (s + r) * self.scale, [self.t2, self.b2], total, lambda: self.landed(8))
                    self.line(9).start()
                    self.line(10).start()

        elif n == 4:

            @pl.when(at.outer)
            def _():
                self.landed(3)
                self.line(4).start()

            if two:

                @pl.when(at.inner)
                def _():
                    self.landed(9)
                    self.line(11).start()

        else:
            self.landed(4)
            self.line(0).wait_send()
            self.line(4).wait_send()

            @pl.when(at.outer)
            def _():
                self.line(1).wait_send()
                if two:
                    self.landed(10)
                    self.landed(11)
                    self.line(5).wait_send()
                    self.line(6).wait_send()

            @pl.when(at.inner)
            def _():
                self.line(2).wait_send()
                self.line(3).wait_send()
                if two:
                    for k in (7, 8, 9, 10, 11):
                        self.line(k).wait_send()


class Backward:
    def __init__(self, dims, refs):
        self.__dict__.update(dims)
        self.at = Place()
        self.early = {entry[1] for entry in ORDER if entry[0] == ACT}
        refs = list(refs)
        for name in self.names[0]:
            setattr(self, name, refs.pop(0))
        self.fins = [refs.pop(0) for _ in KINDS]
        self.tensors = [refs.pop(0) for _ in range(self.count)]
        for name, ref in zip(self.names[1], refs, strict=True):
            setattr(self, name, ref)
        self.half = self.s // 2
        self.blk = min(256, self.half)
        self.means, self.grads = {}, {}
        tensors, i = list(self.tensors), 0
        combine = Combine(self.wide, self.narrow, self.combine_sem)
        for l in range(self.layers):
            for kind in KINDS:
                g16, g32 = tensors.pop(0), tensors.pop(0)
                self.grads[kind, l], base = (g16, g32), 0
                for p, (rows, first) in enumerate(CUTS[l][kind]):
                    a = tensors.pop(0)
                    a_bufs, b_bufs = [a.at[j] for j in range(4)], None
                    if rows > first:
                        b0, b = tensors.pop(0), tensors.pop(0)
                        b_bufs = [b0] + [b.at[j] for j in range(4)]
                    sems = self.dp_send.at[i], self.dp_recv.at[i]
                    self.means[kind, l, p] = Mean(self.at, combine, self.replicas, base, rows, first, g16, g32, self.fins[kind].at[l], a_bufs, b_bufs, *sems)
                    base += rows
                    i += 1

    def local(self, k, src, dst):
        return pltpu.make_async_copy(src, dst, self.local_sem.at[k])

    def mlp_weights(self, l):
        return [self.local(0, self.w_up.at[l], self.wu_v), self.local(1, self.w_down.at[l], self.wd_v)]

    def attn_weights(self, l):
        d, heads = self.hd // self.heads, self.heads
        cols = [self.local(4 + c * heads + n, self.w_qkv.at[l, c, n], self.wq_v.at[:, pl.ds((c * heads + n) * d, d)]) for c in range(3) for n in range(heads)]
        rows = [self.local(4 + 3 * heads + n, self.w_out.at[l, n], self.wo_v.at[pl.ds(n * d, d), :]) for n in range(heads)]
        return cols + rows

    def top_grad(self, m):
        return self.local(2 + m, self.d_out.at[m], self.res.at[pl.ds(m * self.s, self.s), :])

    def act_only(self, l, m):
        blk, cols = self.blk, min(512, self.f)

        def body(y_ref, a_ref):
            y = y_ref[...]
            for c in range(self.f // cols):
                sl = slice(c * cols, (c + 1) * cols)
                h = dot(y, self.wu_v[:, sl])
                t = jnp.tanh(h * (TANH_1 + TANH_3 * (h * h)))
                a_ref[:, sl] = (h * (0.5 * t + 0.5)).astype(BF16)

        row = lambda width: pl.BlockSpec((blk, width), lambda i: (i, 0))
        pltpu.emit_pipeline(body, grid=(self.s // blk,), in_specs=[row(self.w)], out_specs=[row(self.f)])(
            self.y_saved.at[l, m], self.act.at[pl.ds(m * self.s, self.s), :]
        )

    def mlp(self, l, m, own):
        half, blk, cols = self.half, self.blk, min(512, self.f)
        start = (self.at.core if own else 1 - self.at.core) * half
        part = (self.own if own else self.part).at[m]

        def body(step, y_ref, *a_ref):
            i = step.index[0]
            rows = pl.ds(aligned(m * self.s + start + i * blk, blk), blk)
            y, g = y_ref[...], self.res[rows, :]
            for c in range(self.f // cols):
                sl = slice(c * cols, (c + 1) * cols)
                h = dot(y, self.wu_v[:, sl])
                da = dot(g, self.wd_v[sl, :], LANES)
                h2 = h * h
                t = jnp.tanh(h * (TANH_1 + TANH_3 * h2))
                cdf = 0.5 * t + 0.5
                slope = cdf + (0.5 * h) * (1.0 - t * t) * (TANH_1 + (3.0 * TANH_3) * h2)
                for a in a_ref:
                    a[:, sl] = (h * cdf).astype(BF16)
                self.dh_v[rows, sl] = (da * slope).astype(BF16)
            dh = self.dh_v[rows, :]
            wcols = min(512, self.w)
            for c in range(self.w // wcols):
                sl = slice(c * wcols, (c + 1) * wcols)
                part[pl.ds(aligned(i * blk, blk), blk), sl] = dot(dh, self.wu_v[sl, :], LANES).astype(BF16)

        row = lambda width: pl.BlockSpec((blk, width), lambda i: (i, 0))
        outs = [] if l in self.early else [self.act.at[pl.ds(aligned(m * self.s + start, blk), half), :]]
        pltpu.emit_pipeline(body, grid=(half // blk,), in_specs=[row(self.w)], out_specs=[row(self.f)] * len(outs), _explicit_indices=True)(
            self.y_saved.at[l, m, pl.ds(aligned(start, blk), half), :], *outs
        )

    def qkv(self, l, m):
        blk, cols = self.blk, min(384, 3 * self.hd)

        def body(x_ref, out_ref):
            x = x_ref[...]
            for c in range(3 * self.hd // cols):
                sl = slice(c * cols, (c + 1) * cols)
                out_ref[:, sl] = dot(x, self.wq_v[:, sl]).astype(BF16)

        row = lambda width: pl.BlockSpec((blk, width), lambda i: (i, 0))
        pltpu.emit_pipeline(body, grid=(self.s // blk,), in_specs=[row(self.w)], out_specs=[row(3 * self.hd)])(
            self.x_saved.at[l, m], self.qkv_hbm.at[pl.ds(m * self.s, self.s), :]
        )

    def head_loads(self, m, n):
        d = self.hd // self.heads
        slot = (m * self.heads + n) % 2
        base = 4 + 4 * self.heads + 3 * slot
        return [
            self.local(base + c, self.qkv_hbm.at[pl.ds(m * self.s, self.s), pl.ds((c * self.heads + n) * d, d)], self.head.at[slot, c])
            for c in range(3)
        ]

    def attn(self, l, m, n):
        s, d, blk = self.s, self.hd // self.heads, min(256, self.s)
        scale = d**-0.5
        slot = (m * self.heads + n) % 2
        for c in self.head_loads(m, n):
            c.wait()
        if n + 1 < self.heads:
            for c in self.head_loads(m, n + 1):
                c.start()
        mine = slice(m * s, (m + 1) * s)
        col = slice(n * d, (n + 1) * d)
        q_ref, k_ref, v_ref = (self.head.at[slot, c] for c in range(3))
        p_ref, ds_ref = self.dh_v.at[0:s, 0:s], self.dh_v.at[s : 2 * s, 0:s]
        do_ref = self.do_v
        do_ref[...] = dot(self.res[mine, :], self.wo_v[col, :], LANES).astype(BF16)
        keys, vals = k_ref[...], v_ref[...]
        keys_t, vals_t = keys.T, vals.T
        place = lambda c: slice((c * self.heads + n) * d, (c * self.heads + n + 1) * d)
        block = lambda i: slice(i * blk, (i + 1) * blk)
        scores = lambda i: (dot(keys, q_ref[block(i), :], LANES), dot(vals, do_ref[block(i), :], LANES))
        ahead = scores(0)
        for i in range(s // blk):
            sc, dp = ahead
            if i + 1 < s // blk:
                ahead = scores(i + 1)
            sl = block(i)
            out = slice(m * s + i * blk, m * s + (i + 1) * blk)
            top = jnp.max(sc, axis=0, keepdims=True)
            e = jnp.exp((sc - top) * scale)
            inv = 1.0 / jnp.sum(e, axis=0, keepdims=True)
            row_dot = jnp.sum(dp * e, axis=0, keepdims=True) * inv
            pb = (e * inv).astype(BF16)
            ds = (e * ((dp - row_dot) * (inv * scale))).astype(BF16)
            p_ref[:, sl] = pb
            ds_ref[:, sl] = ds
            self.o_v[out, col] = dot(vals_t, pb).T.astype(BF16)
            self.dqkv_v[out, place(0)] = dot(keys_t, ds).T.astype(BF16)
        self.dqkv_v[mine, place(1)] = dot(ds_ref[...], q_ref[...]).astype(BF16)
        self.dqkv_v[mine, place(2)] = dot(p_ref[...], do_ref[...]).astype(BF16)

    def attn_part(self, l, m, own):
        half, cols = self.half, min(512, self.w)
        start = (self.at.core if own else 1 - self.at.core) * half
        part = (self.own if own else self.part).at[m]

        @pl.loop(0, half // self.blk)
        def _(i):
            dqkv = self.dqkv_v[pl.ds(aligned(m * self.s + start + i * self.blk, self.blk), self.blk), :]
            for c in range(self.w // cols):
                sl = slice(c * cols, (c + 1) * cols)
                part[pl.ds(aligned(i * self.blk, self.blk), self.blk), sl] = dot(dqkv, self.wq_v[sl, :], LANES).astype(BF16)

    def tp_copy(self, k, m, src, dst, to):
        return pltpu.make_async_remote_copy(
            src_ref=src, dst_ref=dst, send_sem=self.tp_send.at[k, m], recv_sem=self.tp_recv.at[k, m], device_id={"tp": to}, device_id_type=MESH
        )

    def tp_line(self, k, m):
        at = self.at
        if k == 0:
            return self.tp_copy(0, m, self.part.at[m], self.from_core.at[m], at.other_core)
        if k == 1:
            return self.tp_copy(1, m, self.own.at[m], self.from_chip.at[m], at.other_chip)
        rows = self.res.at[pl.ds(aligned(m * self.s + at.core * self.half), self.half), :]
        return self.tp_copy(2, m, rows, rows, at.other_core)

    def tp_pair(self, m, first):
        line = self.tp_line(0, m)
        line.wait_recv()
        own, got = self.own.at[m], self.from_core.at[m]

        def add(i, n):
            r = pl.ds(i, n)
            own[r, :] = (own[r, :].astype(F32) + got[r, :].astype(F32)).astype(BF16)

        in_place(self.half, add)
        line.wait_send()
        if not first:
            pl.semaphore_wait(self.chip_free.at[m], 1)
        self.tp_line(1, m).start()

    def tp_total(self, m, last, credit):
        line = self.tp_line(1, m)
        line.wait_recv()
        own, got = self.own.at[m], self.from_chip.at[m]
        base = m * self.s + self.at.core * self.half

        def add(i, n):
            r, b = pl.ds(i, n), pl.ds(aligned(base + i, n), n)
            self.res[b, :] = (self.res[b, :].astype(F32) + (own[r, :].astype(F32) + got[r, :].astype(F32))).astype(BF16)

        in_place(self.half, add)
        line.wait_send()
        if not last:
            signal(self.chip_free.at[m], "tp", self.at.other_chip)
        if credit:
            pl.semaphore_wait(self.core_free, 1)
        self.tp_line(2, m).start()

    def tp_done(self, m):
        line = self.tp_line(2, m)
        line.wait_recv()
        line.wait_send()

    def release_rows(self):
        signal(self.core_free, "tp", self.at.other_core)

    def grad(self, kind, l, part):
        rhs = (self.res, self.dh_v, self.dqkv_v, self.res)[kind]
        g16, g32 = self.grads[kind, l]
        cols = g32.shape[1]
        sizes = [rows for rows, _ in CUTS[l][kind]]
        lo, rows = sum(sizes[:part]), sizes[part]
        hi = lo + rows
        tile = next(t for t in (256, 384, 128) if rows % t == 0)
        chunk = min(512 if cols % 512 == 0 else 384, cols)
        two = self.mbs * self.s

        def put(lhs, o16_ref, o32_ref):
            for c in range(cols // chunk):
                sl = slice(c * chunk, (c + 1) * chunk)
                v = dot(lhs, rhs[:, sl], ROWS)
                o32_ref[:, sl] = v
                o16_ref[:, sl] = v.astype(BF16)

        out = pl.BlockSpec((tile, cols), lambda j: (j, 0))
        dst = (g16.at[lo:hi, :], g32.at[lo:hi, :])
        grid = ((hi - lo) // tile,)
        if kind == OUT:

            def body(step, *outs):
                put(self.o_v[:, pl.ds(aligned(lo + step.index[0] * tile, tile), tile)], *outs)

            pltpu.emit_pipeline(body, grid=grid, in_specs=[], out_specs=[out, out], _explicit_indices=True)(*dst)
            return
        if kind == DOWN:
            src, spec = self.act.at[:, lo:hi], pl.BlockSpec((two, tile), lambda j: (0, j))
        else:
            src = (self.y_saved if kind == UP else self.x_saved).at[l, :, :, lo:hi]
            spec = pl.BlockSpec((self.mbs, self.s, tile), lambda j: (0, 0, j))

        def body(lhs_ref, *outs):
            put(lhs_ref[...].reshape(two, tile), *outs)

        pltpu.emit_pipeline(body, grid=grid, in_specs=[spec], out_specs=[out, out])(src, *dst)


def run(b, order):
    for what, *rest in order:
        if what == START:
            up, down = b.mlp_weights(b.layers - 1)
            up.start()
            entry_barrier(b.at)
            up.wait()
            for c in [b.top_grad(m) for m in range(b.mbs)] + [down] + b.attn_weights(b.layers - 1):
                c.start()
            waiting = [b.top_grad(m) for m in range(b.mbs)]
        elif what in (LOAD_MLP, LOAD_ATTN, LOAD_HEAD):
            for c in {LOAD_MLP: b.mlp_weights, LOAD_ATTN: b.attn_weights, LOAD_HEAD: b.head_loads}[what](*rest):
                c.start()
        elif what == WAIT_MLP:
            up, down = b.mlp_weights(*rest)
            if rest[0] < b.layers - 1:
                up.wait()
            down.wait()
        elif what == WAIT_ATTN:
            for c in b.attn_weights(*rest):
                c.wait()
        elif what == SEND:
            b.tp_line(0, rest[0]).start()
        elif what == MEAN:
            *which, n = rest
            b.means[tuple(which)].step(n)
        elif what == FINISH:
            out = [b.local(2 + m, b.res.at[pl.ds(m * b.s, b.s), :], b.d_in.at[m]) for m in range(b.mbs)]
            for c in out:
                c.start()
            for c in out:
                c.wait()
        else:
            if what in (MLP, GRAD):
                while waiting:
                    waiting.pop().wait()
            part = {
                ACT: b.act_only,
                MLP: b.mlp,
                PROJECT: b.qkv,
                HEAD: b.attn,
                PART: b.attn_part,
                PAIR: b.tp_pair,
                TOTAL: b.tp_total,
                DONE: b.tp_done,
                FREE: b.release_rows,
                GRAD: b.grad,
            }[what]
            part(*rest)


def mega_kernel(dims, order, *refs):
    run(Backward(dims, refs), order)


def backward(x_saved, y_saved, d_out, w_qkv, w_out, w_up, w_down, replicas):
    layers, mbs, s, w = x_saved.shape
    f, heads, d = w_up.shape[2], w_qkv.shape[2], w_qkv.shape[4]
    hd, rows = heads * d, mbs * s
    half = s // 2
    shapes = (f, w), (w, f), (w, 3 * hd), (hd, w)
    hbm = {"d_in": (mbs, s, w), "act": (rows, f), "qkv_hbm": (rows, 3 * hd)}
    fins = [(layers, *shape) for shape in shapes]
    tensors = []
    for l in range(layers):
        for (r, c), cuts in zip(shapes, CUTS[l], strict=True):
            tensors += [((r, c), BF16), ((r, c), F32)]
            for n, first in cuts:
                tensors += [((4, first // 2, c), BF16)]
                if n > first:
                    tensors += [((n - first, c), BF16), ((4, (n - first) // 2, c), BF16)]
    vmem = {
        "wu_v": (w, f),
        "wd_v": (f, w),
        "wq_v": (w, 3 * hd),
        "wo_v": (hd, w),
        "res": (rows, w),
        "dh_v": (rows, f),
        "dqkv_v": (rows, 3 * hd),
        "o_v": (rows, hd),
        "part": (mbs, half, w),
        "own": (mbs, half, w),
        "from_core": (mbs, half, w),
        "from_chip": (mbs, half, w),
        "head": (2, 3, s, d),
        "do_v": (s, d),
        "narrow": (2, 3, min(BLOCK, w // 2), w),
    }
    n = sum(len(cuts) for layer in CUTS for cuts in layer)
    dma, regular = pltpu.SemaphoreType.DMA, pltpu.SemaphoreType.REGULAR
    sems = {
        "dp_send": dma((n, 12)),
        "dp_recv": dma((n, 12)),
        "tp_send": dma((3, mbs)),
        "tp_recv": dma((3, mbs)),
        "local_sem": dma((4 + 4 * heads + 6,)),
        "chip_free": regular((mbs,)),
        "core_free": regular,
        "combine_sem": dma((2, 4)),
        "wide": pltpu.VMEM((2, min(BLOCK, w // 2), w), F32),
    }
    ins = ("x_saved", "y_saved", "d_out", "w_qkv", "w_out", "w_up", "w_down")
    names = ((*ins, *hbm), (*vmem, *sems))
    dims = dict(names=names, count=len(tensors), layers=layers, mbs=mbs, s=s, w=w, f=f, heads=heads, hd=hd, replicas=replicas)
    outs = [(v, BF16) for v in (*hbm.values(), *fins)] + tensors
    outs = pl.pallas_call(
        functools.partial(mega_kernel, dims, ORDER),
        in_specs=[ANY] * len(ins),
        out_specs=[ANY] * len(outs),
        out_shape=[jax.ShapeDtypeStruct(*v) for v in outs],
        scratch_shapes=[pltpu.VMEM(v, BF16) for v in vmem.values()] + list(sems.values()),
        compiler_params=pltpu.CompilerParams(collective_id=0, has_side_effects=True, vmem_limit_bytes=67043328),
        name="backward",
    )(x_saved, y_saved, d_out, w_qkv, w_out, w_up, w_down)
    return outs[0], *outs[len(hbm) : len(hbm) + len(fins)]


def finish_kernel(jobs, *refs):
    n = len({job[0] for job in jobs})
    ins, outs = refs[:n], refs[n : 2 * n]
    narrow, wide, in_sem, out_sem = refs[2 * n :]
    depth = narrow.shape[0]

    def load(k):
        which, l, lo, rows, _ = jobs[k]
        src = ins[which].at[l, pl.ds(lo, rows), :]
        return pltpu.make_async_copy(src, narrow.at[k % depth, 0:rows, 0 : src.shape[1]], in_sem.at[k % depth])

    def store(k):
        which, l, lo, rows, pieces = jobs[k]
        cols = ins[which].shape[2]
        if pieces:
            src, dst = wide.at[k % depth, 0:rows, 0:cols], outs[which]
            width = cols // pieces
            return [
                pltpu.make_async_copy(src.at[:, pl.ds(p * width, width)], dst.at[l, p, pl.ds(lo, rows), :], out_sem.at[k % depth, p])
                for p in range(pieces)
            ]
        return [pltpu.make_async_copy(narrow.at[k % depth, 0:rows, 0:cols], outs[which].at[l, pl.ds(lo, rows), :], out_sem.at[k % depth, 0])]

    ahead = depth // 2
    for k in range(ahead):
        load(k).start()
    for k, (which, l, lo, rows, pieces) in enumerate(jobs):
        if k + ahead < len(jobs):
            if k + ahead >= depth:
                for c in store(k + ahead - depth):
                    c.wait()
            load(k + ahead).start()
        load(k).wait()
        if pieces:
            src, dst = narrow.at[k % depth], wide.at[k % depth]
            cols = ins[which].shape[2]

            def block(i, size):
                dst[pl.ds(i, size), 0:cols] = src[pl.ds(i, size), 0:cols].astype(F32)

            in_place(rows, block)
        for c in store(k):
            c.start()
    for k in range(len(jobs) - depth, len(jobs)):
        for c in store(k):
            c.wait()


def finish(d_in, fins, heads):
    ins = (d_in, *fins)
    pieces = (0, 1, 1, 3 * heads, 1)
    jobs = []
    for which, a in enumerate(ins):
        layers, r, c = a.shape
        blk = next(b for b in (256, 192, 128) if r % b == 0)
        jobs += [(which, l, lo, blk, pieces[which]) for l in range(layers) for lo in range(0, r, blk)]
    out = lambda a, p: jax.ShapeDtypeStruct(a.shape if not p else (a.shape[0], p, a.shape[1], a.shape[2] // p), F32 if p else BF16)
    depth, width = 8, max(a.shape[2] for a in ins)
    return pl.pallas_call(
        functools.partial(finish_kernel, jobs),
        in_specs=[ANY] * len(ins),
        out_specs=[ANY] * len(ins),
        out_shape=[out(a, p) for a, p in zip(ins, pieces)],
        scratch_shapes=[
            pltpu.VMEM((depth, 256, width), BF16),
            pltpu.VMEM((depth, 256, width), F32),
            pltpu.SemaphoreType.DMA((depth,)),
            pltpu.SemaphoreType.DMA((depth, 3 * heads)),
        ],
        name="finish",
    )(*ins)


CUTS = (
    (((1024, 384), (512, 224)), ((896, 896), (640, 640)), ((1024, 640), (512, 384)), ((384, 384),)),
    (((1536, 800),), ((1536, 992),), ((1536, 416),), ((384, 384),)),
)
ORDER = (
    (START,), (ACT, 1, 1), (ACT, 1, 0), (GRAD, DOWN, 1, 0), (FREE,), (MEAN, DOWN, 1, 0, 0), (WAIT_MLP, 1), (MLP, 1, 0, False), (SEND, 0),
    (MLP, 1, 0, True), (PAIR, 0, True), (MLP, 1, 1, False), (SEND, 1), (MLP, 1, 1, True), (MEAN, DOWN, 1, 0, 1), (GRAD, UP, 1, 0),
    (MEAN, UP, 1, 0, 0), (WAIT_ATTN, 1), (PROJECT, 1, 0), (TOTAL, 0, False, True), (PAIR, 1, True), (PROJECT, 1, 1), (DONE, 0),
    (LOAD_HEAD, 0, 0), (HEAD, 1, 0, 0), (MEAN, DOWN, 1, 0, 2), (HEAD, 1, 0, 1), (HEAD, 1, 0, 2), (PART, 1, 0, False), (SEND, 0),
    (TOTAL, 1, False, False), (MEAN, UP, 1, 0, 1), (PART, 1, 0, True), (PAIR, 0, False), (MEAN, DOWN, 1, 0, 3), (DONE, 1), (LOAD_HEAD, 1, 0),
    (HEAD, 1, 1, 0), (HEAD, 1, 1, 1), (HEAD, 1, 1, 2), (MEAN, UP, 1, 0, 2), (GRAD, OUT, 1, 0), (FREE,), (GRAD, QKV, 1, 0),
    (MEAN, QKV, 1, 0, 0), (PART, 1, 1, False), (SEND, 1), (TOTAL, 0, False, True), (MEAN, DOWN, 1, 0, 4), (PART, 1, 1, True), (LOAD_ATTN, 0),
    (PAIR, 1, False), (MEAN, OUT, 1, 0, 0), (LOAD_MLP, 0), (DONE, 0), (WAIT_MLP, 0), (MLP, 0, 0, False), (SEND, 0), (MEAN, QKV, 1, 0, 1),
    (MEAN, UP, 1, 0, 3), (MLP, 0, 0, True), (WAIT_ATTN, 0), (PROJECT, 0, 0), (TOTAL, 1, False, False), (PAIR, 0, False), (MEAN, QKV, 1, 0, 2),
    (MEAN, OUT, 1, 0, 1), (DONE, 1), (MLP, 0, 1, False), (SEND, 1), (MLP, 0, 1, True), (MEAN, UP, 1, 0, 4), (GRAD, DOWN, 0, 0),
    (MEAN, DOWN, 0, 0, 0), (MEAN, QKV, 1, 0, 3), (GRAD, DOWN, 0, 1), (FREE,), (TOTAL, 0, False, True), (PAIR, 1, False), (GRAD, UP, 0, 0),
    (MEAN, UP, 0, 0, 0), (MEAN, DOWN, 0, 0, 1), (MEAN, OUT, 1, 0, 2), (MEAN, DOWN, 0, 1, 0), (DONE, 0), (PROJECT, 0, 1), (GRAD, UP, 0, 1),
    (MEAN, QKV, 1, 0, 4), (LOAD_HEAD, 0, 0), (HEAD, 0, 0, 0), (TOTAL, 1, False, False), (MEAN, DOWN, 0, 0, 2), (HEAD, 0, 0, 1),
    (MEAN, UP, 0, 1, 0), (MEAN, DOWN, 0, 1, 1), (MEAN, OUT, 1, 0, 3), (MEAN, UP, 0, 0, 1), (HEAD, 0, 0, 2), (MEAN, DOWN, 0, 0, 3), (DONE, 1),
    (LOAD_HEAD, 1, 0), (HEAD, 0, 1, 0), (MEAN, DOWN, 0, 1, 2), (HEAD, 0, 1, 1), (MEAN, UP, 0, 1, 1), (MEAN, UP, 0, 0, 2),
    (MEAN, DOWN, 0, 0, 4), (PART, 0, 0, False), (SEND, 0), (HEAD, 0, 1, 2), (GRAD, OUT, 0, 0), (FREE,), (MEAN, OUT, 0, 0, 0),
    (MEAN, DOWN, 0, 1, 3), (GRAD, QKV, 0, 0), (MEAN, UP, 0, 1, 2), (MEAN, OUT, 0, 0, 1), (MEAN, DOWN, 1, 0, 5), (MEAN, QKV, 0, 0, 0),
    (MEAN, UP, 0, 0, 3), (MEAN, DOWN, 0, 1, 4), (MEAN, OUT, 1, 0, 4), (GRAD, QKV, 0, 1), (PART, 0, 0, True), (PAIR, 0, False),
    (MEAN, DOWN, 0, 0, 5), (MEAN, QKV, 0, 1, 0), (PART, 0, 1, False), (SEND, 1), (MEAN, QKV, 0, 0, 1), (PART, 0, 1, True), (PAIR, 1, False),
    (MEAN, OUT, 1, 0, 5), (MEAN, OUT, 0, 0, 2), (MEAN, UP, 0, 1, 3), (MEAN, UP, 0, 0, 4), (MEAN, QKV, 0, 0, 2), (MEAN, OUT, 0, 0, 3),
    (MEAN, QKV, 0, 1, 1), (MEAN, UP, 0, 1, 4), (MEAN, QKV, 0, 1, 2), (MEAN, OUT, 0, 0, 4), (MEAN, QKV, 0, 0, 3), (MEAN, QKV, 0, 1, 3),
    (TOTAL, 0, True, True), (MEAN, UP, 0, 1, 5), (MEAN, QKV, 0, 0, 4), (TOTAL, 1, True, False), (MEAN, QKV, 0, 1, 4), (DONE, 1),
    (MEAN, OUT, 0, 0, 5), (DONE, 0), (MEAN, UP, 0, 0, 5), (MEAN, UP, 1, 0, 5), (FINISH,), (MEAN, QKV, 0, 0, 5), (MEAN, QKV, 1, 0, 5),
    (MEAN, DOWN, 0, 1, 5), (MEAN, QKV, 0, 1, 5),
)


def solution(mesh):
    replicas = mesh.shape["dpy"] * mesh.shape["dpx"]
    data_axes = ("dpy", "dpx")
    act_spec = P(None, data_axes, None, None)
    tok_spec = P(data_axes, None, None)
    qkv_spec = P(None, None, None, "tp", None)
    wout_spec = P(None, "tp", None, None)
    up_spec = P(None, None, "tp")
    down_spec = P(None, "tp", None)

    def device_backward(x_saved, y_saved, d_out, w_qkv, w_out, w_up, w_down):
        layers, width, _, heads, d = w_qkv.shape
        by_head = jnp.transpose(w_qkv, (0, 2, 3, 1, 4))
        d_in, *fins = backward(x_saved, y_saved, d_out, by_head, w_out, w_up, w_down, replicas)
        d_in, down, up, qkv, out = finish(d_in, fins, heads)
        g_qkv = jnp.transpose(qkv.reshape(layers, 3, heads, width, d), (0, 3, 1, 2, 4))
        return d_in, g_qkv, out.reshape(w_out.shape), up.reshape(w_up.shape), down.reshape(w_down.shape)

    return jax.shard_map(
        device_backward,
        mesh=mesh,
        in_specs=(act_spec, act_spec, tok_spec, qkv_spec, wout_spec, up_spec, down_spec),
        out_specs=(tok_spec, qkv_spec, wout_spec, up_spec, down_spec),
        check_vma=False,
    )
```
